256 devices in a mesh: ctx: 16 (over y, x), tp: 16 (over z, core).
Axes of the slice: x: 4, y: 4, z: 8, core: 2. Of those that a mesh axis runs over, the one named last changes fastest.
Arguments:
- query_proj: bfloat16 [6144, 4096], P('ctx', 'tp'), may hold values from -16 to 16
- key_proj: bfloat16 [6144, 4096], P('ctx', 'tp'), may hold values from -16 to 16
- value_proj: bfloat16 [6144, 4096], P('ctx', 'tp'), may hold values from -6 to 6
- query_gain: float32 [4096], P('tp'), may hold values from 0.1 to 1.9
- key_gain: float32 [4096], P('tp'), may hold values from 0.1 to 1.9
- stripe_of: int32 [32], replicated, may hold values from 0 to 31, as said below
- grad_out: bfloat16 [6144, 4096], P('ctx', 'tp'), may hold values from -6 to 6
Outputs:
- grad_query: bfloat16 [6144, 4096], P('ctx', 'tp')
- grad_key: bfloat16 [6144, 4096], P('ctx', 'tp')
- grad_value: bfloat16 [6144, 4096], P('ctx', 'tp')
- grad_query_gain: float32 [4096], P('tp')
- grad_key_gain: float32 [4096], P('tp')
The draws below stay inside these ranges and needn't reach their ends.
Inputs may be any that keep to these rules, and one draw needn't show every extreme that they name: `stripe_of`: each number of 0 to 31 appears once, and entries 2 d and 2 d + 1 sum to 31 for every d.
All inputs are finite; a program needn't handle non-finite values.
Results may differ from the reference program's by a relative error of at most 0.012.
The reference program's roundings to bfloat16 on the way count: a program that leaves them out, or rounds other values in their place, can miss the bound.
Values may be sent and summed in bfloat16 or wider, within the bound.
A program may use at most 128 MiB of HBM per device.

```python
import jax
import jax.numpy as jnp
from jax import lax

H = 32
HD = 128
D = 4096
TOK_DEV = 384
SEQ = 6144
STRIPE = 192


def stripe_table(base_key):
    group_count = SEQ // TOK_DEV
    table_key = jax.random.fold_in(base_key, 7)
    order_list = jax.random.permutation(jax.random.fold_in(table_key, 1), group_count)
    flip_bits = jax.random.randint(jax.random.fold_in(table_key, 2), (group_count,), 0, 2)
    first_stripe = jnp.where(flip_bits == 1, 2 * group_count - 1 - order_list, order_list)
    second_stripe = 2 * group_count - 1 - first_stripe
    return jnp.stack([first_stripe, second_stripe], axis=1).reshape(2 * group_count).astype(jnp.int32)


def shaped_field(base_key, salt_value):
    rough_field = jnp.clip(jax.random.normal(jax.random.fold_in(base_key, salt_value), (SEQ, D), jnp.float32), -5.0, 5.0)
    return rough_field


def draw_query_proj(key, part):
    return shaped_field(key, 101).astype(jnp.bfloat16)


def draw_key_proj(key, part):
    return shaped_field(key, 201).astype(jnp.bfloat16)


def draw_stripe_of(key, part):
    return stripe_table(key)


def block_levels(rng, shape, pieces, least, largest):
    def one(dim, blocks):
        heights = jax.random.uniform(jax.random.fold_in(jax.random.fold_in(rng, 6), dim), (blocks,), jnp.float32, least / len(pieces), largest / len(pieces))
        return jnp.repeat(jnp.exp(heights), shape[dim] // blocks).reshape((-1,) + (1,) * (len(shape) - dim - 1))

    factor_of = one(*pieces[0])
    for cut in pieces[1:]:
        factor_of = factor_of * one(*cut)
    return factor_of


def centred(stream_key, shape, spread, most, split=(), kind=jnp.bfloat16):
    array = spread * jax.random.normal(stream_key, shape, jnp.float32)
    if split:
        array = array * block_levels(stream_key, shape, split, -0.22, 0.18)
    return jnp.clip(array, -most, most).astype(kind)


def setup_inputs(seed: int = 0) -> dict:
    streams_of = jax.random.split(jax.random.key(seed), 8)
    query_proj = draw_query_proj(jax.random.fold_in(streams_of[7], 71), 0)
    key_proj = draw_key_proj(jax.random.fold_in(streams_of[7], 71), 0)
    value_proj = centred(streams_of[2], (SEQ, D), 1.0, 6.0, ((0, 16), (1, 16)))
    query_gain = jnp.clip(1.0 + 0.18 * jax.random.normal(streams_of[3], (D,), jnp.float32), 0.1, 1.9)
    key_gain = jnp.clip(1.0 + 0.18 * jax.random.normal(streams_of[4], (D,), jnp.float32), 0.1, 1.9)
    stripe_of = draw_stripe_of(jax.random.fold_in(streams_of[7], 71), 0)
    grad_out = centred(streams_of[6], (SEQ, D), 1.0, 6.0, ((0, 16), (1, 16)))
    return dict(query_proj=query_proj, key_proj=key_proj, value_proj=value_proj, query_gain=query_gain, key_gain=key_gain, stripe_of=stripe_of, grad_out=grad_out)


EPSILON = 1e-06

def normalize(raw_rows, gain_row):
    float_rows = raw_rows.astype(jnp.float32)
    inverse_norm = lax.rsqrt(lax.optimization_barrier(jnp.sum(float_rows * float_rows, axis=1, keepdims=True)) / D + EPSILON)
    unit_rows = float_rows * inverse_norm
    return (inverse_norm, unit_rows, (unit_rows * gain_row).astype(jnp.bfloat16))

def split_heads(matrix):
    return matrix.reshape(SEQ, H, HD).transpose(1, 0, 2)

def merge_heads(stacked):
    return stacked.transpose(1, 0, 2).reshape(SEQ, H * HD)

def finish_norm(inverse_norm, unit_rows, normed_grad, gain_row):
    unit_grad = normed_grad * gain_row
    centered = unit_grad - unit_rows * lax.optimization_barrier(jnp.mean(unit_grad * unit_rows, axis=1, keepdims=True))
    return (inverse_norm * centered).astype(jnp.bfloat16)

def reference(query_proj, key_proj, value_proj, query_gain, key_gain, stripe_of, grad_out):
    query_inverse, query_unit, query_normed = normalize(query_proj, query_gain)
    key_inverse, key_unit, key_normed = normalize(key_proj, key_gain)
    storage_rows = jnp.arange(SEQ, dtype=jnp.int32)
    positions = stripe_of[storage_rows // STRIPE] * STRIPE + storage_rows % STRIPE
    allowed = positions[None, :] <= positions[:, None]
    inverse_root = HD ** (-0.5)

    def one_head(operands):
        query_head, key_head, value_head, grad_head = operands
        scores = jnp.dot(query_head, key_head.T, preferred_element_type=jnp.float32) * inverse_root
        scores = jnp.where(allowed, scores, -jnp.inf)
        row_best = lax.optimization_barrier(jnp.max(scores, axis=1, keepdims=True))
        exponent = jnp.exp(scores - row_best)
        row_total = lax.optimization_barrier(jnp.sum(exponent, axis=1, keepdims=True))
        log_total = row_best + jnp.log(row_total)
        grad_probs = jnp.dot(grad_head, value_head.T, preferred_element_type=jnp.float32)
        probs = jnp.exp(scores - log_total)
        row_delta = lax.optimization_barrier(jnp.sum(probs * grad_probs, axis=1, keepdims=True))
        grad_scores = probs * (grad_probs - row_delta)
        probs_rounded = probs.astype(jnp.bfloat16)
        scores_rounded = grad_scores.astype(jnp.bfloat16)
        value_grad = jnp.dot(probs_rounded.T, grad_head, preferred_element_type=jnp.float32)
        query_grad = jnp.dot(scores_rounded, key_head, preferred_element_type=jnp.float32) * inverse_root
        key_grad = jnp.dot(scores_rounded.T, query_head, preferred_element_type=jnp.float32) * inverse_root
        return (query_grad, key_grad, value_grad)
    query_grads, key_grads, value_grads = lax.map(one_head, (split_heads(query_normed), split_heads(key_normed), split_heads(value_proj), split_heads(grad_out)))
    query_normed_grad = merge_heads(query_grads)
    key_normed_grad = merge_heads(key_grads)
    grad_value = merge_heads(value_grads).astype(jnp.bfloat16)
    grad_query_gain = lax.optimization_barrier(jnp.sum(query_normed_grad * query_unit, axis=0))
    grad_key_gain = lax.optimization_barrier(jnp.sum(key_normed_grad * key_unit, axis=0))
    grad_query = finish_norm(query_inverse, query_unit, query_normed_grad, query_gain)
    grad_key = finish_norm(key_inverse, key_unit, key_normed_grad, key_gain)
    return (grad_query, grad_key, grad_value, grad_query_gain, grad_key_gain)
```

```python
import jax
import jax.numpy as jnp
from jax import lax
from jax.experimental import pallas as pl
from jax.experimental.pallas import tpu as pltpu
from jax.sharding import Mesh
from jax.sharding import PartitionSpec as P

HD = 128
D = 4096
SEQ = 6144
TOK = 384
STRIPE = 192
QUAD = 768
OWN = 768
STEPS = 9
EPSILON = 1e-06
AXES = ("y", "x", "z", "core")
MESH = pl.DeviceIdType.MESH
ROOT = HD**-0.5
LOG2E = 1.4426950408889634
SCALE = ROOT * LOG2E
NEG = -1e30
F32 = jnp.float32
BF16 = jnp.bfloat16


def place():
    return tuple(lax.axis_index(a) for a in AXES)


def tp_peer(y, x, z, c, d):
    t = lax.rem(z * 2 + c + d, 16)
    return (y, x, t // 2, lax.rem(t, 2))


def dot_t(a, b):
    return lax.dot_general(a, b, (((1,), (1,)), ((), ())), preferred_element_type=F32)


def dot_n(a, b):
    return lax.dot_general(a, b, (((1,), (0,)), ((), ())), preferred_element_type=F32)


def rows_of(block):
    folded = block[:, :128] + block[:, 128:]
    return [
        jnp.sum(folded[b * 128 : (b + 1) * 128].T, axis=0, keepdims=True) for b in range(3)
    ]


def signal(device):
    pl.semaphore_signal(
        pltpu.get_barrier_semaphore(), inc=1, device_id=device, device_id_type=MESH
    )


def gather_kernel(
    q_ref, k_ref, v_ref, g_ref, qg_ref, kg_ref,
    q_all, k_all, v_all, g_all, tot_ref,
    qn, kn, sq, sqr, ssem, rsem, fssem, frsem, tssem, trsem,
):
    y, x, z, c = place()
    half = x // 2
    ctx = y * 4 + x
    tp = z * 2 + c
    mine = jnp.where(half == c, 1, 0)
    for d in range(1, 16):
        signal(tp_peer(y, x, z, c, d))
    for dy in range(4):
        for j in range(2):
            device = (lax.rem(y + dy, 4), 2 * c + j, z, half)
            if dy == 0:
                @pl.when(2 * c + j != x)
                def _():
                    signal(device)
            else:
                signal(device)
    pl.semaphore_wait(pltpu.get_barrier_semaphore(), 23 - mine)

    def remote(arr, dy, j, src, dst):
        return pltpu.make_async_remote_copy(
            src_ref=src.at[:, j * 128 : (j + 1) * 128],
            dst_ref=dst.at[pl.ds(ctx * TOK, TOK), :],
            send_sem=ssem.at[arr, dy * 2 + j],
            recv_sem=rsem.at[arr, y * 2 + lax.rem(x, 2)],
            device_id=(lax.rem(y + dy, 4), 2 * c + j, z, half),
            device_id_type=MESH,
        )

    def local(arr, j, src, dst):
        return pltpu.make_async_copy(
            src.at[:, j * 128 : (j + 1) * 128],
            dst.at[pl.ds(ctx * TOK, TOK), :],
            rsem.at[arr, y * 2 + lax.rem(x, 2)],
        )

    def send(arr, src, dst):
        for dy in (2, 1, 3, 0):
            for j in range(2):
                if dy == 0:
                    @pl.when(2 * c + j != x)
                    def _():
                        remote(arr, dy, j, src, dst).start()

                    @pl.when(2 * c + j == x)
                    def _():
                        local(arr, j, src, dst).start()
                else:
                    remote(arr, dy, j, src, dst).start()

    send(0, v_ref, v_all)
    rows = []
    for ref in (q_ref, k_ref):
        wide = ref[...].astype(F32)
        rows += rows_of(wide * wide)
    for i, row in enumerate(rows):
        sq[i : i + 1, :] = row
    sq[6:8, :] = jnp.zeros((2, 128), F32)

    def tp_copy(d):
        return pltpu.make_async_remote_copy(
            src_ref=sq,
            dst_ref=sqr.at[tp],
            send_sem=tssem.at[d],
            recv_sem=trsem.at[tp],
            device_id=tp_peer(y, x, z, c, d),
            device_id_type=MESH,
        )

    for d in range(1, 16):
        tp_copy(d).start()
    send(1, g_ref, g_all)
    sqr[pl.ds(tp, 1)] = sq[...][None]
    for d in range(1, 16):
        other = lax.rem(tp + d, 16)
        pltpu.make_async_remote_copy(
            src_ref=sq,
            dst_ref=sqr.at[other],
            send_sem=tssem.at[d],
            recv_sem=trsem.at[other],
            device_id=tp_peer(y, x, z, c, d),
            device_id_type=MESH,
        ).wait_recv()
    total = sqr[0]
    for i in range(1, 16):
        total = total + sqr[i]
    tot_ref[...] = total
    inverse = lax.rsqrt(total / D + EPSILON).T
    for which, (ref, gain, out) in enumerate(((k_ref, kg_ref, kn), (q_ref, qg_ref, qn))):
        base = 3 if which == 0 else 0
        for b in range(3):
            part = ref[b * 128 : (b + 1) * 128, :].astype(F32)
            unit = part * inverse[:, base + b : base + b + 1]
            out[b * 128 : (b + 1) * 128, :] = (unit * gain[...]).astype(BF16)
        if which == 0:
            send(2, kn, k_all)
    send(3, qn, q_all)

    arrays = (v_all, g_all, k_all, q_all)

    def forward(arr, dy, core, target):
        ys = lax.rem(y + dy, 4)
        part = arrays[arr].at[pl.ds((ys * 4 + core * 2) * TOK, 2 * TOK), :]
        return pltpu.make_async_remote_copy(
            src_ref=part,
            dst_ref=part,
            send_sem=fssem.at[arr, ys],
            recv_sem=frsem.at[arr, ys],
            device_id=(y, x, z, 1 - c),
            device_id_type=MESH,
        )

    for arr in range(4):
        for dy in (0, 1, 3, 2):
            ys = lax.rem(y + dy, 4)
            for j in range(2):
                part = arrays[arr].at[pl.ds((ys * 4 + 2 * c + j) * TOK, TOK), :]
                pltpu.make_async_remote_copy(
                    src_ref=part,
                    dst_ref=part,
                    send_sem=ssem.at[arr, 0],
                    recv_sem=rsem.at[arr, ys * 2 + j],
                    device_id=(y, x, z, 1 - c),
                    device_id_type=MESH,
                ).wait_recv()
            forward(arr, dy, c, 1 - c).start()
    for arr in range(4):
        for dy in (0, 1, 3, 2):
            forward(arr, dy, 1 - c, c).wait_recv()
    for arr in range(4):
        for dy in range(4):
            forward(arr, dy, c, 1 - c).wait_send()
    for arr, (src, dst) in enumerate(((v_ref, v_all), (g_ref, g_all), (kn, k_all), (qn, q_all))):
        for dy in range(4):
            for j in range(2):
                if dy == 0:
                    @pl.when(2 * c + j != x)
                    def _():
                        remote(arr, dy, j, src, dst).wait_send()
                else:
                    remote(arr, dy, j, src, dst).wait_send()
    for d in range(1, 16):
        tp_copy(d).wait_send()


def in_order(table, sources, targets):
    for s in range(32):
        first = pl.multiple_of(table[32 + s] * STRIPE, STRIPE)
        for source, target in zip(sources, targets):
            target[s * STRIPE : (s + 1) * STRIPE, :] = source[pl.ds(first, STRIPE), :]


def pair_of(table, own, p):
    first = table[own * 4 + 2 * p]
    later_first = first >= 16
    high = jnp.where(later_first, first, 31 - first)
    return later_first, high


def row_kernel(table, q_ref, g_ref, k_ref, v_ref, dq_ref, stat_ref, kp, vp, ps, dps, ms, ls, ws, dqs, tile):
    in_order(table, (k_ref, v_ref), (kp, vp))
    own = table[64]
    for p in range(2):
        later_first, high = pair_of(table, own, p)
        low = 31 - high
        high_slot = jnp.where(later_first, 2 * p, 2 * p + 1)
        low_slot = jnp.where(later_first, 2 * p + 1, 2 * p)
        count = (high + 4) // 4

        def scored(t):
            is_high = t < count
            slot = jnp.where(is_high, high_slot, low_slot)
            stripe = jnp.where(is_high, high, low)
            quad = jnp.where(is_high, t, t - count)
            return is_high, pl.multiple_of(slot * STRIPE, STRIPE), stripe, quad

        def first_pass(t, carry):
            is_high, row, stripe, quad = scored(t)
            keys = pl.ds(pl.multiple_of(quad * QUAD, QUAD), QUAD)
            s = dot_t(q_ref[pl.ds(row, STRIPE), :], kp[keys, :]) * SCALE
            gap = lax.broadcasted_iota(jnp.int32, (STRIPE, QUAD), 1) - lax.broadcasted_iota(
                jnp.int32, (STRIPE, QUAD), 0
            )
            s = jnp.where(gap <= stripe * STRIPE - quad * QUAD, s, NEG)
            dp = dot_t(g_ref[pl.ds(row, STRIPE), :], vp[keys, :])
            fresh = jnp.logical_or(t == 0, t == count)
            before = jnp.maximum(t - 1, 0)
            m_old = jnp.where(fresh, NEG, ms[before])
            m_new = jnp.maximum(m_old, jnp.max(s, axis=1, keepdims=True))
            decay = jnp.where(fresh, 0.0, jnp.exp2(m_old - m_new))
            e = jnp.exp2(s - m_new)
            ps[t] = e
            dps[t] = dp
            ms[t] = m_new
            l_old = jnp.where(fresh, 0.0, ls[before])
            w_old = jnp.where(fresh, 0.0, ws[before])
            ls[t] = l_old * decay + jnp.sum(e, axis=1, keepdims=True)
            ws[t] = w_old * decay + jnp.sum(e * dp, axis=1, keepdims=True)
            return carry

        ms[0] = jnp.full((STRIPE, 1), NEG, F32)
        ls[0] = jnp.zeros((STRIPE, 1), F32)
        ws[0] = jnp.zeros((STRIPE, 1), F32)
        lax.fori_loop(0, STEPS, first_pass, 0)
        ends = []
        for last in (count - 1, STEPS - 1):
            total = ls[last]
            ends.append((ms[last] + jnp.log2(total), ws[last] / total))

        def second_pass(t, carry):
            is_high, row, stripe, quad = scored(t)
            keys = pl.ds(pl.multiple_of(quad * QUAD, QUAD), QUAD)
            log_total = jnp.where(is_high, ends[0][0], ends[1][0])
            delta = jnp.where(is_high, ends[0][1], ends[1][1])
            factor = jnp.exp2(ms[t] - log_total)
            ds = (ps[t] * factor * (dps[t] - delta)).astype(BF16)
            dq = dot_n(ds, kp[keys, :])
            fresh = jnp.logical_or(t == 0, t == count)
            before = jnp.maximum(t - 1, 0)
            dqs[t] = jnp.where(fresh, 0.0, dqs[before]) + dq
            return carry

        dqs[0] = jnp.zeros((STRIPE, HD), F32)
        lax.fori_loop(0, STEPS, second_pass, 0)
        dq_high = dqs[count - 1] * ROOT
        dq_low = dqs[STEPS - 1] * ROOT
        for side in range(2):
            take_high = later_first if side == 0 else jnp.logical_not(later_first)
            slot = 2 * p + side
            dq_ref[slot * STRIPE : (slot + 1) * STRIPE, :] = jnp.where(take_high, dq_high, dq_low)
            lane = lax.broadcasted_iota(jnp.int32, (STRIPE, HD), 1)
            tile[0:STRIPE, :] = jnp.where(
                lane == 0,
                jnp.where(take_high, ends[0][0], ends[1][0]),
                jnp.where(take_high, ends[0][1], ends[1][1]),
            )
            tile[STRIPE:256, :] = jnp.zeros((256 - STRIPE, HD), F32)
            turned = tile[...].T
            stat_ref[slot : slot + 1, :] = turned[0:1, :]
            stat_ref[4 + slot : 5 + slot, :] = turned[1:2, :]


def stat_kernel(stat_ref, all_ref, ssem, rsem, lsem):
    y, x, z, c = place()
    own = y * 2 + c
    for d in range(1, 8):
        n = lax.rem(own + d, 8)
        signal((n // 2, x, z, lax.rem(n, 2)))
    pl.semaphore_wait(pltpu.get_barrier_semaphore(), 7)

    def copy(d):
        n = lax.rem(own + d, 8)
        return pltpu.make_async_remote_copy(
            src_ref=stat_ref,
            dst_ref=all_ref.at[own],
            send_sem=ssem.at[d],
            recv_sem=rsem.at[own],
            device_id=(n // 2, x, z, lax.rem(n, 2)),
            device_id_type=MESH,
        )

    for d in range(1, 8):
        copy(d).start()
    mine = pltpu.make_async_copy(stat_ref, all_ref.at[own], lsem)
    mine.start()
    for d in range(1, 8):
        n = lax.rem(own + d, 8)
        pltpu.make_async_remote_copy(
            src_ref=stat_ref,
            dst_ref=all_ref.at[n],
            send_sem=ssem.at[d],
            recv_sem=rsem.at[n],
            device_id=(n // 2, x, z, lax.rem(n, 2)),
            device_id_type=MESH,
        ).wait_recv()
    mine.wait()
    for d in range(1, 8):
        copy(d).wait_send()


def column_kernel(table, k_ref, v_ref, q_ref, g_ref, stat_ref, dk_ref, dv_ref, qp, gp, lse, dlt, dks, dvs):
    in_order(table, (q_ref, g_ref), (qp, gp))
    own = table[64]
    for quad in range(8):
        parts = [[], []]
        for i in range(4):
            slot = table[32 + quad * 4 + i]
            row = (slot // 4) * 8 + lax.rem(slot, 4)
            parts[0].append(stat_ref[pl.ds(row, 1), 0:STRIPE])
            parts[1].append(stat_ref[pl.ds(row + 4, 1), 0:STRIPE])
        lse[quad] = jnp.concatenate(parts[0], axis=1)
        dlt[quad] = jnp.concatenate(parts[1], axis=1)
    for p in range(2):
        later_first, high = pair_of(table, own, p)
        low = 31 - high
        high_slot = jnp.where(later_first, 2 * p, 2 * p + 1)
        low_slot = jnp.where(later_first, 2 * p + 1, 2 * p)
        count = 8 - low // 4

        def body(t, carry):
            is_low = t < count
            row = pl.multiple_of(jnp.where(is_low, low_slot, high_slot) * STRIPE, STRIPE)
            stripe = jnp.where(is_low, low, high)
            quad = jnp.where(is_low, low // 4 + t, high // 4 + t - count)
            queries = pl.ds(pl.multiple_of(quad * QUAD, QUAD), QUAD)
            qv = qp[queries, :]
            gv = gp[queries, :]
            s = dot_t(k_ref[pl.ds(row, STRIPE), :], qv) * SCALE - lse[quad]
            gap = lax.broadcasted_iota(jnp.int32, (STRIPE, QUAD), 0) - lax.broadcasted_iota(
                jnp.int32, (STRIPE, QUAD), 1
            )
            probs = jnp.where(gap <= quad * QUAD - stripe * STRIPE, jnp.exp2(s), 0.0)
            dp = dot_t(v_ref[pl.ds(row, STRIPE), :], gv)
            ds = (probs * (dp - dlt[quad])).astype(BF16)
            dv = dot_n(probs.astype(BF16), gv)
            dk = dot_n(ds, qv)
            fresh = jnp.logical_or(t == 0, t == count)
            before = jnp.maximum(t - 1, 0)
            dks[t] = jnp.where(fresh, 0.0, dks[before]) + dk
            dvs[t] = jnp.where(fresh, 0.0, dvs[before]) + dv
            return carry

        dks[0] = jnp.zeros((STRIPE, HD), F32)
        dvs[0] = jnp.zeros((STRIPE, HD), F32)
        lax.fori_loop(0, STEPS, body, 0)
        for side in range(2):
            take_high = later_first if side == 0 else jnp.logical_not(later_first)
            slot = 2 * p + side
            span = slice(slot * STRIPE, (slot + 1) * STRIPE)
            dk_ref[span, :] = jnp.where(take_high, dks[STEPS - 1], dks[count - 1]) * ROOT
            dv_ref[span, :] = jnp.where(take_high, dvs[STEPS - 1], dvs[count - 1]).astype(BF16)


def finish_kernel(
    dq_ref, dk_ref, dv_ref, q_ref, k_ref, qg_ref, kg_ref, tot_ref,
    oq_ref, ok_ref, ov_ref, gain_ref,
    rq, rk, rv, mt, mtr, gs, gsr, ssem, rsem, tssem, trsem, cssem, crsem,
):
    y, x, z, c = place()
    half = x // 2
    ctx = y * 4 + x
    tp = z * 2 + c
    mine = jnp.where(half == c, 1, 0)

    def ctx_peer(d):
        n = lax.rem(ctx + d, 16)
        return (n // 4, lax.rem(n, 4), z, c)

    for d in range(1, 16):
        signal(tp_peer(y, x, z, c, d))
        signal(ctx_peer(d))
    for j in range(2):
        @pl.when(2 * c + j != x)
        def _():
            signal((y, 2 * c + j, z, half))
    pl.semaphore_wait(pltpu.get_barrier_semaphore(), 32 - mine)
    sets = ((dq_ref, rq), (dk_ref, rk), (dv_ref, rv))

    def remote(arr, j):
        src, dst = sets[arr]
        return pltpu.make_async_remote_copy(
            src_ref=src.at[j * TOK : (j + 1) * TOK, :],
            dst_ref=dst.at[lax.rem(x, 2)],
            send_sem=ssem.at[arr, j],
            recv_sem=rsem.at[arr, lax.rem(x, 2)],
            device_id=(y, 2 * c + j, z, half),
            device_id_type=MESH,
        )

    def local(arr, j):
        src, dst = sets[arr]
        return pltpu.make_async_copy(
            src.at[j * TOK : (j + 1) * TOK, :],
            dst.at[lax.rem(x, 2)],
            rsem.at[arr, lax.rem(x, 2)],
        )

    for arr in range(3):
        for j in range(2):
            @pl.when(2 * c + j != x)
            def _():
                remote(arr, j).start()

            @pl.when(2 * c + j == x)
            def _():
                local(arr, j).start()

    inverse = lax.rsqrt(tot_ref[...] / D + EPSILON).T

    def wait(arr):
        src, dst = sets[arr]
        for j in range(2):
            pltpu.make_async_remote_copy(
                src_ref=dst.at[j],
                dst_ref=dst.at[j],
                send_sem=ssem.at[arr, j],
                recv_sem=rsem.at[arr, j],
                device_id=(y, x, z, 1 - c),
                device_id_type=MESH,
            ).wait_recv()

    streams = ((q_ref, qg_ref, rq, oq_ref), (k_ref, kg_ref, rk, ok_ref))

    def block(which, b):
        ref, gain, back, out = streams[which]
        span = slice(b * 128, (b + 1) * 128)
        scale = inverse[:, 3 * which + b : 3 * which + b + 1]
        unit = ref[span, :].astype(F32) * scale
        normed_grad = jnp.concatenate([back[0, span, :], back[1, span, :]], axis=1)
        return span, scale, unit, normed_grad

    gs[...] = jnp.zeros((8, 256), F32)
    mt[...] = jnp.zeros((8, 128), F32)
    for which in range(2):
        wait(which)
        gain_sum = jnp.zeros((1, 256), F32)
        for b in range(3):
            span, scale, unit, normed_grad = block(which, b)
            product = normed_grad * unit
            gain_sum = gain_sum + jnp.sum(product, axis=0, keepdims=True)
            weighted = product * streams[which][1][...]
            folded = weighted[:, :128] + weighted[:, 128:]
            mt[3 * which + b : 3 * which + b + 1, :] = jnp.sum(folded.T, axis=0, keepdims=True)
        gs[which : which + 1, :] = gain_sum

    def tp_copy(d, slot):
        return pltpu.make_async_remote_copy(
            src_ref=mt,
            dst_ref=mtr.at[slot],
            send_sem=tssem.at[d],
            recv_sem=trsem.at[slot],
            device_id=tp_peer(y, x, z, c, d),
            device_id_type=MESH,
        )

    def ctx_copy(d, slot):
        return pltpu.make_async_remote_copy(
            src_ref=gs,
            dst_ref=gsr.at[slot],
            send_sem=cssem.at[d],
            recv_sem=crsem.at[slot],
            device_id=ctx_peer(d),
            device_id_type=MESH,
        )

    for d in range(1, 16):
        tp_copy(d, tp).start()
    for d in range(1, 16):
        ctx_copy(d, ctx).start()
    mtr[pl.ds(tp, 1)] = mt[...][None]
    gsr[pl.ds(ctx, 1)] = gs[...][None]
    wait(2)
    ov_ref[:, 0:128] = rv[0]
    ov_ref[:, 128:256] = rv[1]
    for d in range(1, 16):
        tp_copy(d, lax.rem(tp + d, 16)).wait_recv()
    total = mtr[0]
    for i in range(1, 16):
        total = total + mtr[i]
    mean = (total / D).T
    for which in range(2):
        for b in range(3):
            span, scale, unit, normed_grad = block(which, b)
            unit_grad = normed_grad * streams[which][1][...]
            centred = unit_grad - unit * mean[:, 3 * which + b : 3 * which + b + 1]
            streams[which][3][span, :] = (scale * centred).astype(BF16)
    for d in range(1, 16):
        ctx_copy(d, lax.rem(ctx + d, 16)).wait_recv()
    gains = gsr[0]
    for i in range(1, 16):
        gains = gains + gsr[i]
    gain_ref[...] = gains
    for arr in range(3):
        for j in range(2):
            @pl.when(2 * c + j != x)
            def _():
                remote(arr, j).wait_send()
    for d in range(1, 16):
        tp_copy(d, tp).wait_send()
        ctx_copy(d, ctx).wait_send()


VM = pl.BlockSpec(memory_space=pltpu.VMEM)
DMA = pltpu.SemaphoreType.DMA
LIMIT = 60000 * 1024


def shape(dims, kind):
    return jax.ShapeDtypeStruct(dims, kind)


def per_device(query_proj, key_proj, value_proj, query_gain, key_gain, stripe_of, grad_out):
    y, x, z, c = place()
    own = y * 2 + c
    slots = jnp.arange(32, dtype=jnp.int32)
    slot_of = jnp.sum(
        jnp.where(stripe_of[None, :] == slots[:, None], slots[None, :], 0), axis=1
    ).astype(jnp.int32)
    table = jnp.concatenate([stripe_of, slot_of, jnp.broadcast_to(own, (8,)).astype(jnp.int32)])
    query_gain = query_gain[None, :]
    key_gain = key_gain[None, :]
    whole = shape((SEQ, HD), BF16)
    q_all, k_all, v_all, g_all, total = pl.pallas_call(
        gather_kernel,
        out_shape=(whole, whole, whole, whole, shape((8, 128), F32)),
        in_specs=[VM] * 6,
        out_specs=(VM,) * 5,
        scratch_shapes=[
            pltpu.VMEM((TOK, 256), BF16),
            pltpu.VMEM((TOK, 256), BF16),
            pltpu.VMEM((8, 128), F32),
            pltpu.VMEM((16, 8, 128), F32),
            DMA((4, 8)),
            DMA((4, 8)),
            DMA((4, 4)),
            DMA((4, 4)),
            DMA((16,)),
            DMA((16,)),
        ],
        compiler_params=pltpu.CompilerParams(
            collective_id=1, has_side_effects=True, vmem_limit_bytes=LIMIT
        ),
        name="gather",
    )(query_proj, key_proj, value_proj, grad_out, query_gain, key_gain)

    full = pl.BlockSpec((SEQ, HD), lambda i, tab: (0, 0))
    part = pl.BlockSpec((OWN, HD), lambda i, tab: (tab[64], 0))
    whole_out = lambda i, tab: (0, 0)
    dq, stat = pl.pallas_call(
        row_kernel,
        out_shape=(shape((OWN, HD), F32), shape((8, 256), F32)),
        grid_spec=pltpu.PrefetchScalarGridSpec(
            num_scalar_prefetch=1,
            grid=(1,),
            in_specs=[part, part, full, full],
            out_specs=(pl.BlockSpec((OWN, HD), whole_out), pl.BlockSpec((8, 256), whole_out)),
            scratch_shapes=[
                pltpu.VMEM((SEQ, HD), BF16),
                pltpu.VMEM((SEQ, HD), BF16),
                pltpu.VMEM((STEPS, STRIPE, QUAD), F32),
                pltpu.VMEM((STEPS, STRIPE, QUAD), F32),
                pltpu.VMEM((STEPS, STRIPE, 1), F32),
                pltpu.VMEM((STEPS, STRIPE, 1), F32),
                pltpu.VMEM((STEPS, STRIPE, 1), F32),
                pltpu.VMEM((STEPS, STRIPE, HD), F32),
                pltpu.VMEM((256, HD), F32),
            ],
        ),
        compiler_params=pltpu.CompilerParams(vmem_limit_bytes=LIMIT),
        name="rows",
    )(table, q_all, g_all, k_all, v_all)

    stats = pl.pallas_call(
        stat_kernel,
        out_shape=shape((8, 8, 256), F32),
        in_specs=[VM],
        out_specs=VM,
        scratch_shapes=[DMA((8,)), DMA((8,)), DMA(())],
        compiler_params=pltpu.CompilerParams(
            collective_id=2, has_side_effects=True, vmem_limit_bytes=LIMIT
        ),
        name="stats",
    )(stat).reshape(64, 256)

    dk, dv = pl.pallas_call(
        column_kernel,
        out_shape=(shape((OWN, HD), F32), shape((OWN, HD), BF16)),
        grid_spec=pltpu.PrefetchScalarGridSpec(
            num_scalar_prefetch=1,
            grid=(1,),
            in_specs=[part, part, full, full, pl.BlockSpec((64, 256), whole_out)],
            out_specs=(pl.BlockSpec((OWN, HD), whole_out), pl.BlockSpec((OWN, HD), whole_out)),
            scratch_shapes=[
                pltpu.VMEM((SEQ, HD), BF16),
                pltpu.VMEM((SEQ, HD), BF16),
                pltpu.VMEM((8, 1, QUAD), F32),
                pltpu.VMEM((8, 1, QUAD), F32),
                pltpu.VMEM((STEPS, STRIPE, HD), F32),
                pltpu.VMEM((STEPS, STRIPE, HD), F32),
            ],
        ),
        compiler_params=pltpu.CompilerParams(vmem_limit_bytes=LIMIT),
        name="columns",
    )(table, k_all, v_all, q_all, g_all, stats)

    out = shape((TOK, 256), BF16)
    grad_query, grad_key, grad_value, gains = pl.pallas_call(
        finish_kernel,
        out_shape=(out, out, out, shape((8, 256), F32)),
        in_specs=[VM] * 8,
        out_specs=(VM,) * 4,
        scratch_shapes=[
            pltpu.VMEM((2, TOK, HD), F32),
            pltpu.VMEM((2, TOK, HD), F32),
            pltpu.VMEM((2, TOK, HD), BF16),
            pltpu.VMEM((8, 128), F32),
            pltpu.VMEM((16, 8, 128), F32),
            pltpu.VMEM((8, 256), F32),
            pltpu.VMEM((16, 8, 256), F32),
            DMA((3, 2)),
            DMA((3, 2)),
            DMA((16,)),
            DMA((16,)),
            DMA((16,)),
            DMA((16,)),
        ],
        compiler_params=pltpu.CompilerParams(
            collective_id=3, has_side_effects=True, vmem_limit_bytes=LIMIT
        ),
        name="finish",
    )(dq, dk, dv, query_proj, key_proj, query_gain, key_gain, total)
    return (grad_query, grad_key, grad_value, gains[0], gains[1])


def solution(mesh):
    torus = Mesh(mesh.devices.reshape(4, 4, 8, 2), AXES)
    wide = P(("y", "x"), ("z", "core"))
    thin = P(("z", "core"))
    return jax.shard_map(
        per_device,
        mesh=torus,
        in_specs=(wide, wide, wide, thin, thin, P(), wide),
        out_specs=(wide, wide, wide, thin, thin),
        check_vma=False,
    )
```

```python
import jax
import jax.numpy as jnp
from jax import lax
from jax.experimental import pallas as pl
from jax.experimental.pallas import tpu as pltpu
from jax.sharding import Mesh
from jax.sharding import PartitionSpec as P

HD = 128
D = 4096
SEQ = 6144
TOK = 384
STRIPE = 192
QUAD = 768
OWN = 768
STEPS = 9
UNROLL = 3
EPSILON = 1e-06
AXES = ("y", "x", "z", "core")
MESH = pl.DeviceIdType.MESH
ROOT = HD**-0.5
LOG2E = 1.4426950408889634
SCALE = ROOT * LOG2E
NEG = -1e30
F32 = jnp.float32
BF16 = jnp.bfloat16


def place():
    return tuple(lax.axis_index(a) for a in AXES)


def tp_peer(y, x, z, c, d):
    t = lax.rem(z * 2 + c + d, 16)
    return (y, x, t // 2, lax.rem(t, 2))


def dot_t(a, b):
    return lax.dot_general(a, b, (((1,), (1,)), ((), ())), preferred_element_type=F32)


def dot_n(a, b):
    return lax.dot_general(a, b, (((1,), (0,)), ((), ())), preferred_element_type=F32)


def rows_of(block):
    folded = block[:, :128] + block[:, 128:]
    return [
        jnp.sum(folded[b * 128 : (b + 1) * 128].T, axis=0, keepdims=True) for b in range(3)
    ]


def signal(device):
    pl.semaphore_signal(
        pltpu.get_barrier_semaphore(), inc=1, device_id=device, device_id_type=MESH
    )


def remote(src, dst, send_sem, recv_sem, device):
    return pltpu.make_async_remote_copy(
        src_ref=src,
        dst_ref=dst,
        send_sem=send_sem,
        recv_sem=recv_sem,
        device_id=device,
        device_id_type=MESH,
    )


def in_order(table, source, target):
    for s in range(32):
        target[s // 4, s % 4 * STRIPE : (s % 4 + 1) * STRIPE, :] = source[table[32 + s]]


def steps(body):
    def some(i, carry):
        for u in range(UNROLL):
            body(i * UNROLL + u)
        return carry

    lax.fori_loop(0, STEPS // UNROLL, some, 0)


class Pair:
    def __init__(self, table, own, p):
        first = table[own * 4 + 2 * p]
        self.p = p
        self.later_first = first >= 16
        self.high = jnp.where(self.later_first, first, 31 - first)
        self.low = 31 - self.high
        self.high_slot = jnp.where(self.later_first, 2 * p, 2 * p + 1)
        self.low_slot = jnp.where(self.later_first, 2 * p + 1, 2 * p)
        self.count = (self.high + 4) // 4
        self.column_count = 8 - self.low // 4

    def row_step(self, t):
        is_high = t < self.count
        side = jnp.where(is_high, 0, 1)
        slot = jnp.where(is_high, self.high_slot, self.low_slot)
        stripe = jnp.where(is_high, self.high, self.low)
        quad = jnp.where(is_high, t, t - self.count)
        fresh = jnp.logical_or(t == 0, t == self.count)
        return side, slot, stripe, quad, fresh

    def column_step(self, t):
        is_low = t < self.column_count
        slot = jnp.where(is_low, self.low_slot, self.high_slot)
        stripe = jnp.where(is_low, self.low, self.high)
        quad = jnp.where(is_low, self.low // 4 + t, self.high // 4 + t - self.column_count)
        fresh = jnp.logical_or(t == 0, t == self.column_count)
        return slot, stripe, quad, fresh


def chunk(i):
    return slice(i * 128, (i + 1) * 128)


def previous(t):
    return jnp.maximum(t - 1, 0)


def main_kernel(
    table, q_ref, k_ref, v_ref, g_ref, qg_ref, kg_ref,
    rq, rk, rv, tot_ref, mean_ref, gain_ref,
    qn, kn, own_v, own_k, own_g, own_q, all_v, all_k, all_g, all_q, vp, kp, gp, qp,
    sq, sqr, ss, dps, ms, mm, ls, ws, lz, dl, dqs, dks, tile, st_own, st_all, lse, dlt,
    dq_out, dk_out, dv_out, mt, mtr, gs, gsr,
    row_s, row_r, col_s, col_r, rel_s, sib_s, sib_r, tp_s, tp_r, st_s, st_r,
    ret_s, ret_r, mt_s, mt_r, cx_s, cx_r,
):
    y, x, z, c = place()
    half = x // 2
    parity = lax.rem(x, 2)
    ctx = y * 4 + x
    tp = z * 2 + c
    own = y * 2 + c
    up, down, far = lax.rem(y + 1, 4), lax.rem(y + 3, 4), lax.rem(y + 2, 4)
    sibling = (y, x, z, 1 - c)

    for d in range(1, 32):
        n = lax.rem(ctx * 2 + c + d, 32)
        signal((n // 8, lax.rem(n // 2, 4), z, lax.rem(n, 2)))
    for d in range(1, 8):
        for core in range(2):
            signal((y, x, lax.rem(z + d, 8), core))
    pl.semaphore_wait(pltpu.get_barrier_semaphore(), 45)

    V, K, G, Q = range(4)
    sources = (v_ref, kn, g_ref, qn)
    owns = (own_v, own_k, own_g, own_q)
    alls = (all_v, all_k, all_g, all_q)

    def row_copy(a, j):
        return remote(
            sources[a].at[:, :, chunk(j)],
            owns[a].at[pl.ds(parity * 2, 2)],
            row_s.at[a, j],
            row_r.at[a, parity],
            (y, 2 * c + j, z, half),
        )

    def row_start(a):
        for j in range(2):
            @pl.when(2 * c + j != x)
            def _():
                row_copy(a, j).start()

            @pl.when(2 * c + j == x)
            def _():
                pltpu.make_async_copy(
                    sources[a].at[:, :, chunk(j)],
                    owns[a].at[pl.ds(parity * 2, 2)],
                    row_r.at[a, parity],
                ).start()

    def row_wait(a):
        for j in range(2):
            part = owns[a].at[pl.ds(j * 2, 2)]
            remote(part, part, row_s.at[a, j], row_r.at[a, j], sibling).wait_recv()

    def rows_at(yy, core, j):
        return pl.ds((yy * 4 + 2 * core + j) * 2, 2)

    def block_at(yy, core):
        return pl.ds((yy * 4 + 2 * core) * 2, 4)

    def own_copy(a, direction, j):
        target = up if direction == 0 else down
        return remote(
            owns[a].at[pl.ds(j * 2, 2)],
            alls[a].at[rows_at(y, c, j)],
            col_s.at[a, direction * 2 + j],
            col_r.at[a, direction * 2 + j],
            (target, x, z, c),
        )

    def relay_copy(a, direction):
        origin, target = (down, up) if direction == 0 else (up, down)
        part = alls[a].at[rows_at(origin, c, direction)]
        return remote(
            part, part, rel_s.at[a, direction], col_r.at[a, 4 + direction], (target, x, z, c)
        )

    def sib_copy(a, which, core):
        yy = (y, down, up, far)[which]
        place_of = alls[a].at[block_at(yy, core)]
        start = owns[a] if which == 0 else place_of
        return remote(start, place_of, sib_s.at[a, which], sib_r.at[a, which], sibling)

    def col_wait(a, index):
        origin = (down, down, up, up, far, far)[index]
        part = alls[a].at[rows_at(origin, c, index % 2)]
        remote(part, part, rel_s.at[a, 0], col_r.at[a, index], sibling).wait_recv()

    def own_send(a):
        own_copy(a, 0, 0).start()
        own_copy(a, 1, 1).start()
        own_copy(a, 0, 1).start()
        own_copy(a, 1, 0).start()
        sib_copy(a, 0, c).start()

    def relay(a):
        col_wait(a, 0)
        relay_copy(a, 0).start()
        col_wait(a, 3)
        relay_copy(a, 1).start()

    def near(a):
        col_wait(a, 1)
        sib_copy(a, 1, c).start()
        col_wait(a, 2)
        sib_copy(a, 2, c).start()

    def away(a):
        col_wait(a, 4)
        col_wait(a, 5)
        sib_copy(a, 3, c).start()

    def settle(a, target):
        alls[a][block_at(y, c)] = owns[a][...]
        for which in range(4):
            sib_copy(a, which, 1 - c).wait_recv()
        in_order(table, alls[a], target)

    row_start(V)
    rows = []
    for ref in (q_ref, k_ref):
        wide = ref[...].astype(F32).reshape(TOK, 256)
        rows += rows_of(wide * wide)
    for i, row in enumerate(rows):
        sq[i : i + 1, :] = row
    sq[6:8, :] = jnp.zeros((2, 128), F32)

    def tp_copy(src, dst, send, recv, d, slot):
        return remote(src, dst.at[slot], send.at[d], recv.at[slot], tp_peer(y, x, z, c, d))

    for d in range(1, 16):
        tp_copy(sq, sqr, tp_s, tp_r, d, tp).start()
    row_start(G)
    sqr[pl.ds(tp, 1)] = sq[...][None]
    row_wait(V)
    own_send(V)
    for d in range(1, 16):
        tp_copy(sq, sqr, tp_s, tp_r, d, lax.rem(tp + d, 16)).wait_recv()
    total = sqr[0]
    for i in range(1, 16):
        total = total + sqr[i]
    tot_ref[...] = total
    inverse = lax.rsqrt(total / D + EPSILON).T
    for ref, gain, out, base, a in ((k_ref, kg_ref, kn, 3, K), (q_ref, qg_ref, qn, 0, Q)):
        wide = ref[...].astype(F32).reshape(TOK, 256)
        parts = []
        for b in range(3):
            unit = wide[chunk(b)] * inverse[:, base + b : base + b + 1]
            parts.append(unit * gain[...])
        out[...] = jnp.concatenate(parts, axis=0).reshape(2, STRIPE, 256).astype(BF16)
        row_start(a)

    pairs = [Pair(table, own, p) for p in range(2)]

    def grad_probs(pair):
        def body(t):
            side, slot, stripe, quad, fresh = pair.row_step(t)
            dps[pair.p, t] = dot_t(own_g[slot], vp[quad])

        steps(body)

    def score(pair):
        p = pair.p
        ms[0] = jnp.full((STRIPE, 128), NEG, F32)

        def body(t):
            side, slot, stripe, quad, fresh = pair.row_step(t)
            s = dot_t(own_q[slot], kp[quad]) * SCALE
            gap = lax.broadcasted_iota(jnp.int32, (STRIPE, QUAD), 1) - lax.broadcasted_iota(
                jnp.int32, (STRIPE, QUAD), 0
            )
            s = jnp.where(gap <= stripe * STRIPE - quad * QUAD, s, NEG)
            ss[p, t] = s
            most = jnp.where(fresh, NEG, ms[previous(t)])
            for i in range(6):
                most = jnp.maximum(most, s[:, chunk(i)])
            ms[t] = most

        steps(body)
        for side, last in enumerate((pair.count - 1, STEPS - 1)):
            mm[p, side] = jnp.broadcast_to(
                jnp.max(ms[last], axis=1, keepdims=True), (STRIPE, 128)
            )

    def sums(pair):
        p = pair.p
        ls[0] = jnp.zeros((STRIPE, 128), F32)
        ws[0] = jnp.zeros((STRIPE, 128), F32)

        def body(t):
            side, slot, stripe, quad, fresh = pair.row_step(t)
            most = mm[p, side]
            l = jnp.where(fresh, 0.0, ls[previous(t)])
            w = jnp.where(fresh, 0.0, ws[previous(t)])
            for i in range(6):
                e = jnp.exp2(ss[p, t, :, chunk(i)] - most)
                l = l + e
                w = w + e * dps[p, t, :, chunk(i)]
            ls[t] = l
            ws[t] = w

        steps(body)
        ends = []
        for side, last in enumerate((pair.count - 1, STEPS - 1)):
            l = jnp.sum(ls[last], axis=1, keepdims=True)
            w = jnp.sum(ws[last], axis=1, keepdims=True)
            log_total = mm[p, side] + jnp.log2(l)
            delta = jnp.broadcast_to(w / l, (STRIPE, 128))
            lz[p, side] = log_total
            dl[p, side] = delta
            ends.append((log_total, delta))
        lane = lax.broadcasted_iota(jnp.int32, (STRIPE, HD), 1)
        for side in range(2):
            take_high = pair.later_first if side == 0 else jnp.logical_not(pair.later_first)
            slot = 2 * p + side
            tile[0:STRIPE, :] = jnp.where(
                lane == 0,
                jnp.where(take_high, ends[0][0], ends[1][0]),
                jnp.where(take_high, ends[0][1], ends[1][1]),
            )
            tile[STRIPE:256, :] = jnp.zeros((256 - STRIPE, HD), F32)
            turned = tile[...].T
            st_own[slot : slot + 1, :] = turned[0:1, :]
            st_own[4 + slot : 5 + slot, :] = turned[1:2, :]

    def query_grad(pair):
        p = pair.p
        dqs[0] = jnp.zeros((STRIPE, HD), F32)

        def body(t):
            side, slot, stripe, quad, fresh = pair.row_step(t)
            log_total = lz[p, side]
            delta = dl[p, side]
            parts = []
            for i in range(6):
                probs = jnp.exp2(ss[p, t, :, chunk(i)] - log_total)
                parts.append((probs * (dps[p, t, :, chunk(i)] - delta)).astype(BF16))
            dq = dot_n(jnp.concatenate(parts, axis=1), kp[quad])
            dqs[t] = jnp.where(fresh, 0.0, dqs[previous(t)]) + dq

        steps(body)
        high, low = dqs[pair.count - 1] * ROOT, dqs[STEPS - 1] * ROOT
        for side in range(2):
            take_high = pair.later_first if side == 0 else jnp.logical_not(pair.later_first)
            slot = 2 * p + side
            dq_out[slot * STRIPE : (slot + 1) * STRIPE, :] = jnp.where(take_high, high, low)

    def key_grads(pair):
        p = pair.p
        dqs[0] = jnp.zeros((STRIPE, HD), F32)
        dks[0] = jnp.zeros((STRIPE, HD), F32)

        def body(t):
            slot, stripe, quad, fresh = pair.column_step(t)
            qv = qp[quad]
            gv = gp[quad]
            s = dot_t(own_k[slot], qv) * SCALE - lse[quad]
            gap = lax.broadcasted_iota(jnp.int32, (STRIPE, QUAD), 0) - lax.broadcasted_iota(
                jnp.int32, (STRIPE, QUAD), 1
            )
            probs = jnp.where(gap <= quad * QUAD - stripe * STRIPE, jnp.exp2(s), 0.0)
            dp = dot_t(own_v[slot], gv)
            ds = (probs * (dp - dlt[quad])).astype(BF16)
            dv = dot_n(probs.astype(BF16), gv)
            dk = dot_n(ds, qv)
            dks[t] = jnp.where(fresh, 0.0, dks[previous(t)]) + dk
            dqs[t] = jnp.where(fresh, 0.0, dqs[previous(t)]) + dv

        steps(body)
        for side in range(2):
            take_high = pair.later_first if side == 0 else jnp.logical_not(pair.later_first)
            slot = 2 * p + side
            span = slice(slot * STRIPE, (slot + 1) * STRIPE)
            last = pair.column_count - 1
            dk_out[span, :] = jnp.where(take_high, dks[STEPS - 1], dks[last]) * ROOT
            dv_out[span, :] = jnp.where(take_high, dqs[STEPS - 1], dqs[last]).astype(BF16)

    relay(V)
    row_wait(K)
    own_send(K)
    near(V)
    away(V)
    settle(V, vp)
    row_wait(G)
    grad_probs(pairs[0])
    relay(K)
    grad_probs(pairs[1])
    near(K)
    own_send(G)
    away(K)
    settle(K, kp)
    row_wait(Q)
    own_send(Q)
    relay(G)
    score(pairs[0])
    near(G)
    relay(Q)
    score(pairs[1])
    away(G)
    near(Q)
    sums(pairs[0])
    away(Q)
    sums(pairs[1])

    def stat_copy(d, slot):
        n = lax.rem(own + d, 8)
        return remote(
            st_own,
            st_all.at[pl.ds(slot * 8, 8), :],
            st_s.at[d],
            st_r.at[slot],
            (n // 2, x, z, lax.rem(n, 2)),
        )

    for d in range(1, 8):
        stat_copy(d, own).start()
    st_all[pl.ds(own * 8, 8), :] = st_own[...]
    returns = ((dq_out, rq), (dk_out, rk), (dv_out, rv))

    def return_copy(a, j):
        out, back = returns[a]
        return remote(
            out.at[j * TOK : (j + 1) * TOK, :],
            back.at[parity],
            ret_s.at[a, j],
            ret_r.at[a, parity],
            (y, 2 * c + j, z, half),
        )

    def return_start(a, j):
        out, back = returns[a]

        @pl.when(2 * c + j != x)
        def _():
            return_copy(a, j).start()

        @pl.when(2 * c + j == x)
        def _():
            pltpu.make_async_copy(
                out.at[j * TOK : (j + 1) * TOK, :], back.at[parity], ret_r.at[a, parity]
            ).start()

    def return_wait(a):
        back = returns[a][1]
        for j in range(2):
            remote(
                back.at[j], back.at[j], ret_s.at[a, j], ret_r.at[a, j], sibling
            ).wait_recv()

    for p in range(2):
        query_grad(pairs[p])
        return_start(0, p)
    settle(G, gp)
    settle(Q, qp)
    for d in range(1, 8):
        stat_copy(d, lax.rem(own + d, 8)).wait_recv()
    for quad in range(8):
        parts = [[], []]
        for i in range(4):
            slot = table[32 + quad * 4 + i]
            row = (slot // 4) * 8 + lax.rem(slot, 4)
            parts[0].append(st_all[pl.ds(row, 1), 0:STRIPE])
            parts[1].append(st_all[pl.ds(row + 4, 1), 0:STRIPE])
        lse[quad] = jnp.concatenate(parts[0], axis=1)
        dlt[quad] = jnp.concatenate(parts[1], axis=1)
    for p in range(2):
        key_grads(pairs[p])
        return_start(1, p)
        return_start(2, p)

    streams = ((q_ref, qg_ref, rq), (k_ref, kg_ref, rk))
    gs[...] = jnp.zeros((8, 256), F32)
    mt[...] = jnp.zeros((8, 128), F32)
    for which, (ref, gain, back) in enumerate(streams):
        return_wait(which)
        gain_sum = jnp.zeros((1, 256), F32)
        wide = ref[...].astype(F32).reshape(TOK, 256)
        for b in range(3):
            scale = inverse[:, 3 * which + b : 3 * which + b + 1]
            unit = wide[chunk(b)] * scale
            normed_grad = jnp.concatenate([back[0, chunk(b), :], back[1, chunk(b), :]], axis=1)
            product = normed_grad * unit
            gain_sum = gain_sum + jnp.sum(product, axis=0, keepdims=True)
            weighted = product * gain[...]
            folded = weighted[:, :128] + weighted[:, 128:]
            mt[3 * which + b : 3 * which + b + 1, :] = jnp.sum(folded.T, axis=0, keepdims=True)
        gs[which : which + 1, :] = gain_sum

    def ctx_copy(d, slot):
        n = lax.rem(ctx + d, 16)
        return remote(
            gs, gsr.at[slot], cx_s.at[d], cx_r.at[slot], (n // 4, lax.rem(n, 4), z, c)
        )

    for d in range(1, 16):
        tp_copy(mt, mtr, mt_s, mt_r, d, tp).start()
    for d in range(1, 16):
        ctx_copy(d, ctx).start()
    mtr[pl.ds(tp, 1)] = mt[...][None]
    gsr[pl.ds(ctx, 1)] = gs[...][None]
    return_wait(2)
    for a in range(4):
        for j in range(2):
            @pl.when(2 * c + j != x)
            def _():
                row_copy(a, j).wait_send()
        for direction in range(2):
            for j in range(2):
                own_copy(a, direction, j).wait_send()
            relay_copy(a, direction).wait_send()
        for which in range(4):
            sib_copy(a, which, c).wait_send()
    for d in range(1, 8):
        stat_copy(d, own).wait_send()
    for a in range(3):
        for j in range(2):
            @pl.when(2 * c + j != x)
            def _():
                return_copy(a, j).wait_send()
    for d in range(1, 16):
        tp_copy(sq, sqr, tp_s, tp_r, d, tp).wait_send()
    for d in range(1, 16):
        tp_copy(mt, mtr, mt_s, mt_r, d, lax.rem(tp + d, 16)).wait_recv()
    total = mtr[0]
    for i in range(1, 16):
        total = total + mtr[i]
    mean_ref[...] = total
    for d in range(1, 16):
        ctx_copy(d, lax.rem(ctx + d, 16)).wait_recv()
    gains = gsr[0]
    for i in range(1, 16):
        gains = gains + gsr[i]
    gain_ref[...] = gains
    for d in range(1, 16):
        tp_copy(mt, mtr, mt_s, mt_r, d, tp).wait_send()
        ctx_copy(d, ctx).wait_send()


def finish_kernel(
    rq, rk, rv, tot_ref, mean_ref, gain_ref, q_ref, k_ref, qg_ref, kg_ref,
    oq_ref, ok_ref, ov_ref, ogq_ref, ogk_ref,
):
    inverse = lax.rsqrt(tot_ref[...] / D + EPSILON).T
    mean = (mean_ref[...] / D).T
    streams = ((q_ref, qg_ref, rq, oq_ref), (k_ref, kg_ref, rk, ok_ref))
    for which, (ref, gain, back, out) in enumerate(streams):
        for b in range(3):
            column = slice(3 * which + b, 3 * which + b + 1)
            unit = ref[chunk(b), :].astype(F32) * inverse[:, column]
            normed_grad = jnp.concatenate([back[0, chunk(b), :], back[1, chunk(b), :]], axis=1)
            centred = normed_grad * gain[...] - unit * mean[:, column]
            out[chunk(b), :] = (inverse[:, column] * centred).astype(BF16)
    ov_ref[:, 0:128] = rv[0]
    ov_ref[:, 128:256] = rv[1]
    ogq_ref[...] = gain_ref[0:1, :]
    ogk_ref[...] = gain_ref[1:2, :]


VM = pl.BlockSpec(memory_space=pltpu.VMEM)
DMA = pltpu.SemaphoreType.DMA
LIMIT = 60000 * 1024


def shape(dims, kind):
    return jax.ShapeDtypeStruct(dims, kind)


def vmem(kind, *dims):
    return pltpu.VMEM(dims, kind)


def per_device(query_proj, key_proj, value_proj, query_gain, key_gain, stripe_of, grad_out):
    slots = jnp.arange(32, dtype=jnp.int32)
    slot_of = jnp.sum(
        jnp.where(stripe_of[None, :] == slots[:, None], slots[None, :], 0), axis=1
    ).astype(jnp.int32)
    table = jnp.concatenate([stripe_of, slot_of])
    query_gain = query_gain[None, :]
    key_gain = key_gain[None, :]
    back = shape((2, TOK, HD), F32)
    small = shape((8, 128), F32)
    rq, rk, rv, total, mean, gains = pl.pallas_call(
        main_kernel,
        out_shape=(back, back, shape((2, TOK, HD), BF16), small, small, shape((8, 256), F32)),
        in_specs=[pl.BlockSpec(memory_space=pltpu.SMEM)] + [VM] * 6,
        out_specs=(VM,) * 6,
        scratch_shapes=[vmem(BF16, 2, STRIPE, 256)] * 2
        + [vmem(BF16, 4, STRIPE, HD)] * 4
        + [vmem(BF16, 32, STRIPE, HD)] * 4
        + [vmem(BF16, 8, QUAD, HD)] * 4
        + [
            vmem(F32, 8, 128),
            vmem(F32, 16, 8, 128),
            vmem(F32, 2, STEPS, STRIPE, QUAD),
            vmem(F32, 2, STEPS, STRIPE, QUAD),
            vmem(F32, STEPS, STRIPE, 128),
            vmem(F32, 2, 2, STRIPE, 128),
            vmem(F32, STEPS, STRIPE, 128),
            vmem(F32, STEPS, STRIPE, 128),
            vmem(F32, 2, 2, STRIPE, 128),
            vmem(F32, 2, 2, STRIPE, 128),
            vmem(F32, STEPS, STRIPE, HD),
            vmem(F32, STEPS, STRIPE, HD),
            vmem(F32, 256, HD),
            vmem(F32, 8, 256),
            vmem(F32, 64, 256),
            vmem(F32, 8, 1, QUAD),
            vmem(F32, 8, 1, QUAD),
            vmem(F32, OWN, HD),
            vmem(F32, OWN, HD),
            vmem(BF16, OWN, HD),
            vmem(F32, 8, 128),
            vmem(F32, 16, 8, 128),
            vmem(F32, 8, 256),
            vmem(F32, 16, 8, 256),
            DMA((4, 2)),
            DMA((4, 2)),
            DMA((4, 4)),
            DMA((4, 6)),
            DMA((4, 2)),
            DMA((4, 4)),
            DMA((4, 4)),
            DMA((16,)),
            DMA((16,)),
            DMA((8,)),
            DMA((8,)),
            DMA((3, 2)),
            DMA((3, 2)),
            DMA((16,)),
            DMA((16,)),
            DMA((16,)),
            DMA((16,)),
        ],
        compiler_params=pltpu.CompilerParams(
            collective_id=1, has_side_effects=True, vmem_limit_bytes=LIMIT
        ),
        name="main",
    )(
        table,
        *(a.reshape(2, STRIPE, 256) for a in (query_proj, key_proj, value_proj, grad_out)),
        query_gain,
        key_gain,
    )

    out = shape((TOK, 256), BF16)
    gain_out = shape((1, 256), F32)
    grad_query, grad_key, grad_value, gain_q, gain_k = pl.pallas_call(
        finish_kernel,
        out_shape=(out, out, out, gain_out, gain_out),
        in_specs=[VM] * 10,
        out_specs=(VM,) * 5,
        name="finish",
    )(rq, rk, rv, total, mean, gains, query_proj, key_proj, query_gain, key_gain)
    return (grad_query, grad_key, grad_value, gain_q[0], gain_k[0])


def solution(mesh):
    torus = Mesh(mesh.devices.reshape(4, 4, 8, 2), AXES)
    wide = P(("y", "x"), ("z", "core"))
    thin = P(("z", "core"))
    return jax.shard_map(
        per_device,
        mesh=torus,
        in_specs=(wide, wide, wide, thin, thin, P(), wide),
        out_specs=(wide, wide, wide, thin, thin),
        check_vma=False,
    )
```

```python
import jax
import jax.numpy as jnp
from jax import lax
from jax.experimental import pallas as pl
from jax.experimental.pallas import tpu as pltpu
from jax.sharding import Mesh
from jax.sharding import PartitionSpec as P

HD = 128
D = 4096
SEQ = 6144
TOK = 384
STRIPE = 192
QUAD = 768
OWN = 768
STEPS = 5
QS, QIDX, QST, KS, KIDX, KST, QCOUNT, KCOUNT = 0, 16, 32, 48, 64, 80, 96, 100
EPSILON = 1e-06
AXES = ("y", "x", "z", "core")
MESH = pl.DeviceIdType.MESH
ROOT = HD**-0.5
LOG2E = 1.4426950408889634
SCALE = ROOT * LOG2E
NEG = -1e30
F32 = jnp.float32
BF16 = jnp.bfloat16


def place():
    return tuple(lax.axis_index(a) for a in AXES)


def tp_peer(y, x, z, c, d):
    t = lax.rem(z * 2 + c + d, 16)
    return (y, x, t // 2, lax.rem(t, 2))


def dot_t(a, b):
    return lax.dot_general(a, b, (((1,), (1,)), ((), ())), preferred_element_type=F32)


def dot_n(a, b):
    return lax.dot_general(a, b, (((1,), (0,)), ((), ())), preferred_element_type=F32)


def rows_of(block):
    folded = block[:, :128] + block[:, 128:]
    return [
        jnp.sum(folded[b * 128 : (b + 1) * 128].T, axis=0, keepdims=True) for b in range(3)
    ]


def signal(device):
    pl.semaphore_signal(
        pltpu.get_barrier_semaphore(), inc=1, device_id=device, device_id_type=MESH
    )


def remote(src, dst, send_sem, recv_sem, device):
    return pltpu.make_async_remote_copy(
        src_ref=src,
        dst_ref=dst,
        send_sem=send_sem,
        recv_sem=recv_sem,
        device_id=device,
        device_id_type=MESH,
    )


def chunk(i):
    return slice(i * 128, (i + 1) * 128)


def main_kernel(
    table, q_ref, k_ref, v_ref, g_ref, qg_ref, kg_ref,
    rq, rk, rv, tot_ref, mean_ref, gain_ref,
    qn, kn, all_v, all_k, all_g, all_q, vp, kp, gp, qp,
    sq, sqr, ss, dps, ms, mm, ls, ws, lz, dl, acc, acc2, tile, st_all, fin_l, fin_d,
    lse, dlt, kpos, qpos, dq_all, dk_all, dv_all, dq_send, dk_send, dv_send,
    dq_got, dk_got, dv_got, dq_ret, dk_ret, dv_ret, mt, mtr, gs, gsr,
    row_s, row_r, y_s, y_r, sib_s, sib_r, tp_s, tp_r, st_s, st_r, red_s, red_r,
    ret_s, ret_r, mt_s, mt_r, cx_s, cx_r,
):
    y, x, z, c = place()
    half = x // 2
    parity = lax.rem(x, 2)
    ctx = y * 4 + x
    tp = z * 2 + c
    sibling = (y, x, z, 1 - c)
    y_query = y + 1 - 2 * lax.rem(y, 2)
    y_key = 3 - y

    for d in range(1, 32):
        n = lax.rem(ctx * 2 + c + d, 32)
        signal((n // 8, lax.rem(n // 2, 4), z, lax.rem(n, 2)))
    for d in range(1, 8):
        for core in range(2):
            signal((y, x, lax.rem(z + d, 8), core))
    pl.semaphore_wait(pltpu.get_barrier_semaphore(), 45)

    V, K, G, Q = range(4)
    sources = (v_ref, kn, g_ref, qn)
    alls = (all_v, all_k, all_g, all_q)
    partners = ((y_key, x, z, c), (y_key, x, z, c), (y_query, x, z, c), (y_query, x, z, c))

    def row_copy(a, j):
        return remote(
            sources[a].at[:, :, chunk(j)],
            alls[a].at[pl.ds(half * 4 + parity * 2, 2)],
            row_s.at[a, j],
            row_r.at[a, parity],
            (y, 2 * c + j, z, half),
        )

    def row_start(a):
        for j in range(2):
            @pl.when(2 * c + j != x)
            def _():
                row_copy(a, j).start()

            @pl.when(2 * c + j == x)
            def _():
                pltpu.make_async_copy(
                    sources[a].at[:, :, chunk(j)],
                    alls[a].at[pl.ds(half * 4 + parity * 2, 2)],
                    row_r.at[a, parity],
                ).start()

    def y_copy(a, j):
        return remote(
            alls[a].at[pl.ds(c * 4 + j * 2, 2)],
            alls[a].at[pl.ds(8 + c * 4 + j * 2, 2)],
            y_s.at[a, j],
            y_r.at[a, j],
            partners[a],
        )

    def sib_copy(a, which, core):
        part = alls[a].at[pl.ds(which * 8 + core * 4, 4)]
        return remote(part, part, sib_s.at[a, which], sib_r.at[a, which], sibling)

    def spread(a):
        for j in range(2):
            part = alls[a].at[pl.ds(c * 4 + j * 2, 2)]
            remote(part, part, row_s.at[a, j], row_r.at[a, j], sibling).wait_recv()
            y_copy(a, j).start()
        sib_copy(a, 0, c).start()

    def arrive(a):
        for j in range(2):
            part = alls[a].at[pl.ds(8 + c * 4 + j * 2, 2)]
            remote(part, part, y_s.at[a, j], y_r.at[a, j], sibling).wait_recv()
        sib_copy(a, 1, c).start()

    def settle(a, order, target):
        for which in range(2):
            sib_copy(a, which, 1 - c).wait_recv()
        for s in range(16):
            target[s // 4, s % 4 * STRIPE : (s % 4 + 1) * STRIPE, :] = alls[a][table[order + s]]

    row_start(V)
    rows = []
    for ref in (q_ref, k_ref):
        wide = ref[...].astype(F32).reshape(TOK, 256)
        rows += rows_of(wide * wide)
    for i, row in enumerate(rows):
        sq[i : i + 1, :] = row
    sq[6:8, :] = jnp.zeros((2, 128), F32)

    def tp_copy(src, dst, send, recv, d, slot):
        return remote(src, dst.at[slot], send.at[d], recv.at[slot], tp_peer(y, x, z, c, d))

    for d in range(1, 16):
        tp_copy(sq, sqr, tp_s, tp_r, d, tp).start()
    row_start(G)
    sqr[pl.ds(tp, 1)] = sq[...][None]
    lane = lax.broadcasted_iota(jnp.int32, (1, QUAD), 1)
    for sorted_at, out in ((KST, kpos), (QST, qpos)):
        for quad in range(4):
            base = [(table[sorted_at + quad * 4 + i] - i) * STRIPE for i in range(4)]
            shift = jnp.where(
                lane < 2 * STRIPE,
                jnp.where(lane < STRIPE, base[0], base[1]),
                jnp.where(lane < 3 * STRIPE, base[2], base[3]),
            )
            out[quad] = lane + shift
    spread(V)
    for d in range(1, 16):
        tp_copy(sq, sqr, tp_s, tp_r, d, lax.rem(tp + d, 16)).wait_recv()
    total = sqr[0]
    for i in range(1, 16):
        total = total + sqr[i]
    tot_ref[...] = total
    inverse = lax.rsqrt(total / D + EPSILON).T
    for ref, gain, out, base, a in ((k_ref, kg_ref, kn, 3, K), (q_ref, qg_ref, qn, 0, Q)):
        wide = ref[...].astype(F32).reshape(TOK, 256)
        parts = []
        for b in range(3):
            unit = wide[chunk(b)] * inverse[:, base + b : base + b + 1]
            parts.append(unit * gain[...])
        out[...] = jnp.concatenate(parts, axis=0).reshape(2, STRIPE, 256).astype(BF16)
        row_start(a)

    def pair_of(set_at, count_at, p):
        base = c * 4 + 2 * lax.rem(p, 2) + 8 * (1 - p // 2)
        first = table[set_at + base]
        first_high = first >= 16
        high = jnp.where(first_high, first, 31 - first)
        high_at = jnp.where(first_high, 0, 1)
        return base, first_high, high, high_at, table[count_at + p]

    def row_step(p, t):
        base, first_high, high, high_at, count = pair_of(QS, QCOUNT, p)
        is_high = t < count
        side = jnp.where(is_high, high_at, 1 - high_at)
        stripe = jnp.where(is_high, high, 31 - high)
        quad = jnp.where(is_high, t, t - count)
        return base + side, side, stripe, jnp.clip(quad, 0, 3)

    def column_step(p, t):
        base, first_high, high, high_at, count = pair_of(KS, KCOUNT, p)
        is_low = t < count
        side = jnp.where(is_low, 1 - high_at, high_at)
        stripe = jnp.where(is_low, 31 - high, high)
        quad = jnp.where(is_low, 4 - count + t, t - 1)
        return base + side, stripe, jnp.clip(quad, 0, 3)

    def split(ref, count, start, join):
        two, three = 2 < count, 3 < count
        first = join(ref[0], ref[1])
        first = join(first, jnp.where(two, ref[2], start))
        first = join(first, jnp.where(three, ref[3], start))
        second = join(ref[4], jnp.where(two, start, ref[2]))
        second = join(second, jnp.where(three, start, ref[3]))
        return first, second

    def loop(lower, upper, body):
        def one(p, carry):
            body(p)
            return carry

        lax.fori_loop(lower, upper, one, 0)

    def grad_probs(p):
        for t in range(STEPS):
            slot, side, stripe, quad = row_step(p, t)
            dps[p, t] = dot_t(all_g[slot], vp[quad])

    def score(p):
        base, first_high, high, high_at, count = pair_of(QS, QCOUNT, p)
        row = lax.broadcasted_iota(jnp.int32, (STRIPE, QUAD), 0)
        for t in range(STEPS):
            slot, side, stripe, quad = row_step(p, t)
            s = dot_t(all_q[slot], kp[quad]) * SCALE
            s = jnp.where(kpos[quad] - stripe * STRIPE <= row, s, NEG)
            ss[p, t] = s
            most = s[:, chunk(0)]
            for i in range(1, 6):
                most = jnp.maximum(most, s[:, chunk(i)])
            ms[t] = most
        for side, most in enumerate(split(ms, count, NEG, jnp.maximum)):
            at = high_at if side == 0 else 1 - high_at
            wide = jnp.broadcast_to(jnp.max(most, axis=1, keepdims=True), (STRIPE, 128))
            mm[p, 0] = jnp.where(at == 0, wide, mm[p, 0])
            mm[p, 1] = jnp.where(at == 1, wide, mm[p, 1])

    def sums(p):
        base, first_high, high, high_at, count = pair_of(QS, QCOUNT, p)
        for t in range(STEPS):
            slot, side, stripe, quad = row_step(p, t)
            most = mm[p, side]
            l = jnp.zeros((STRIPE, 128), F32)
            w = jnp.zeros((STRIPE, 128), F32)
            for i in range(6):
                e = jnp.exp2(ss[p, t, :, chunk(i)] - most)
                l = l + e
                w = w + e * dps[p, t, :, chunk(i)]
            ls[t] = l
            ws[t] = w
        l_ends = [jnp.sum(v, axis=1, keepdims=True) for v in split(ls, count, 0.0, jnp.add)]
        w_ends = [jnp.sum(v, axis=1, keepdims=True) for v in split(ws, count, 0.0, jnp.add)]
        lane = lax.broadcasted_iota(jnp.int32, (STRIPE, HD), 1)
        for side in range(2):
            take_first = first_high if side == 0 else jnp.logical_not(first_high)
            l = jnp.where(take_first, l_ends[0], l_ends[1])
            w = jnp.where(take_first, w_ends[0], w_ends[1])
            tile[0:STRIPE, :] = jnp.where(
                lane == 0, mm[p, side], jnp.where(lane == 1, l, w)
            )
            turned = tile[...].T
            for i in range(3):
                st_all[0, pl.ds(i * 8 + p * 2 + side, 1), :] = turned[i : i + 1, :]

    def query_grad(p):
        base, first_high, high, high_at, count = pair_of(QS, QCOUNT, p)
        for t in range(STEPS):
            slot, side, stripe, quad = row_step(p, t)
            log_total = lz[p * 2 + side]
            delta = dl[p * 2 + side]
            parts = []
            for i in range(6):
                probs = jnp.exp2(ss[p, t, :, chunk(i)] - log_total)
                parts.append((probs * (dps[p, t, :, chunk(i)] - delta)).astype(BF16))
            acc[t] = dot_n(jnp.concatenate(parts, axis=1), kp[quad])
        ends = split(acc, count, 0.0, jnp.add)
        for side in range(2):
            take_first = first_high if side == 0 else jnp.logical_not(first_high)
            value = jnp.where(take_first, ends[0], ends[1]) * ROOT
            dq_all[p * 2 + side] = value
            dq_send[p * 2 + side] = value.astype(BF16)

    def key_grads(p):
        base, first_high, high, high_at, count = pair_of(KS, KCOUNT, p)
        row = lax.broadcasted_iota(jnp.int32, (STRIPE, QUAD), 0)
        for t in range(STEPS):
            slot, stripe, quad = column_step(p, t)
            qv = qp[quad]
            gv = gp[quad]
            s = dot_t(all_k[slot], qv) * SCALE - lse[quad]
            probs = jnp.where(row <= qpos[quad] - stripe * STRIPE, jnp.exp2(s), 0.0)
            dp = dot_t(all_v[slot], gv)
            ds = (probs * (dp - dlt[quad])).astype(BF16)
            acc[t] = dot_n(probs.astype(BF16), gv)
            acc2[t] = dot_n(ds, qv)
        for source, scale, out, send in ((acc, None, dv_all, dv_send), (acc2, ROOT, dk_all, dk_send)):
            ends = split(source, count, 0.0, jnp.add)
            for side in range(2):
                take_low = jnp.logical_not(first_high) if side == 0 else first_high
                value = jnp.where(take_low, ends[0], ends[1])
                value = value if scale is None else value * scale
                out[p * 2 + side] = value
                send[p * 2 + side] = value.astype(BF16)

    tile[STRIPE:256, :] = jnp.zeros((256 - STRIPE, HD), F32)
    for p in range(4):
        for side in range(2):
            mm[p, side] = jnp.zeros((STRIPE, 128), F32)
    spread(G)
    arrive(V)
    arrive(G)
    spread(K)
    settle(V, KIDX, vp)
    settle(G, QIDX, gp)
    loop(0, 2, grad_probs)
    spread(Q)
    loop(2, 4, grad_probs)
    arrive(K)
    arrive(Q)
    settle(K, KIDX, kp)
    settle(Q, QIDX, qp)
    loop(0, 4, score)
    loop(0, 4, sums)

    stat_peers = (None, (y_query, x, z, c), sibling, (y_query, x, z, 1 - c))

    def stat_copy(i):
        return remote(st_all.at[0], st_all.at[i], st_s.at[i], st_r.at[i], stat_peers[i])

    for i in range(1, 4):
        stat_copy(i).start()
    for i in range(1, 4):
        stat_copy(i).wait_recv()
    for which in range(2):
        mine, other = st_all[2 * which], st_all[2 * which + 1]
        other = jnp.concatenate(
            [other[i * 8 + r : i * 8 + r + 4] for i in range(3) for r in (4, 0)], axis=0
        )
        most = jnp.maximum(mine[0:8], other[0:8])
        left, right = jnp.exp2(mine[0:8] - most), jnp.exp2(other[0:8] - most)
        l = mine[8:16] * left + other[8:16] * right
        w = mine[16:24] * left + other[16:24] * right
        log_total = most + jnp.log2(l)
        delta = w / l
        core = c if which == 0 else 1 - c
        fin_l[core] = log_total
        fin_d[core] = delta
        if which == 0:
            turned_l, turned_d = log_total.T, delta.T
            for i in range(8):
                lz[i] = jnp.broadcast_to(turned_l[0:STRIPE, i : i + 1], (STRIPE, 128))
                dl[i] = jnp.broadcast_to(turned_d[0:STRIPE, i : i + 1], (STRIPE, 128))

    reduces = (
        (dq_send, dq_got, (y_query, x, z, c)),
        (dk_send, dk_got, (y_key, x, z, c)),
        (dv_send, dv_got, (y_key, x, z, c)),
    )

    def reduce_copy(a):
        send, got, device = reduces[a]
        return remote(send.at[pl.ds(0, 4)], got, red_s.at[a], red_r.at[a], device)

    returns = ((dq_ret, rq), (dk_ret, rk), (dv_ret, rv))

    def return_copy(a, j):
        out, back = returns[a]
        return remote(
            out.at[pl.ds(j * 2, 2)],
            back.at[parity],
            ret_s.at[a, j],
            ret_r.at[a, parity],
            (y, 2 * c + j, z, half),
        )

    def return_start(a):
        out, back = returns[a]
        for j in range(2):
            @pl.when(2 * c + j != x)
            def _():
                return_copy(a, j).start()

            @pl.when(2 * c + j == x)
            def _():
                pltpu.make_async_copy(
                    out.at[pl.ds(j * 2, 2)], back.at[parity], ret_r.at[a, parity]
                ).start()

    def return_wait(a):
        back = returns[a][1]
        for j in range(2):
            remote(
                back.at[j], back.at[j], ret_s.at[a, j], ret_r.at[a, j], sibling
            ).wait_recv()

    def join(a, mine):
        reduce_copy(a).wait_recv()
        for i in range(4):
            returns[a][0][i] = (mine[4 + i] + reduces[a][1][i].astype(F32)).astype(BF16)
        return_start(a)

    loop(0, 2, query_grad)
    reduce_copy(0).start()
    loop(2, 4, query_grad)
    for quad in range(4):
        parts = [[], []]
        for i in range(4):
            at = table[QIDX + quad * 4 + i]
            core = lax.rem(at // 4, 2)
            row = lax.rem(at, 4) + 4 * (1 - at // 8)
            parts[0].append(fin_l[core, pl.ds(row, 1), 0:STRIPE])
            parts[1].append(fin_d[core, pl.ds(row, 1), 0:STRIPE])
        lse[quad] = jnp.concatenate(parts[0], axis=1)
        dlt[quad] = jnp.concatenate(parts[1], axis=1)
    loop(0, 2, key_grads)
    reduce_copy(2).start()
    reduce_copy(1).start()
    join(0, dq_all)
    loop(2, 4, key_grads)
    join(2, dv_all)
    join(1, dk_all)

    streams = ((q_ref, qg_ref, rq), (k_ref, kg_ref, rk))
    gs[...] = jnp.zeros((8, 256), F32)
    mt[...] = jnp.zeros((8, 128), F32)
    for which, (ref, gain, back) in enumerate(streams):
        return_wait(which)
        gain_sum = jnp.zeros((1, 256), F32)
        wide = ref[...].astype(F32).reshape(TOK, 256)
        grads = [back[j].reshape(TOK, HD) for j in range(2)]
        for b in range(3):
            scale = inverse[:, 3 * which + b : 3 * which + b + 1]
            unit = wide[chunk(b)] * scale
            normed_grad = jnp.concatenate([g[chunk(b)] for g in grads], axis=1).astype(F32)
            product = normed_grad * unit
            gain_sum = gain_sum + jnp.sum(product, axis=0, keepdims=True)
            weighted = product * gain[...]
            folded = weighted[:, :128] + weighted[:, 128:]
            mt[3 * which + b : 3 * which + b + 1, :] = jnp.sum(folded.T, axis=0, keepdims=True)
        gs[which : which + 1, :] = gain_sum

    def ctx_copy(d, slot):
        n = lax.rem(ctx + d, 16)
        return remote(
            gs, gsr.at[slot], cx_s.at[d], cx_r.at[slot], (n // 4, lax.rem(n, 4), z, c)
        )

    for d in range(1, 16):
        tp_copy(mt, mtr, mt_s, mt_r, d, tp).start()
    for d in range(1, 16):
        ctx_copy(d, ctx).start()
    mtr[pl.ds(tp, 1)] = mt[...][None]
    gsr[pl.ds(ctx, 1)] = gs[...][None]
    return_wait(2)
    for a in range(4):
        for j in range(2):
            @pl.when(2 * c + j != x)
            def _():
                row_copy(a, j).wait_send()
            y_copy(a, j).wait_send()
            sib_copy(a, j, c).wait_send()
    for i in range(1, 4):
        stat_copy(i).wait_send()
    for a in range(3):
        reduce_copy(a).wait_send()
        for j in range(2):
            @pl.when(2 * c + j != x)
            def _():
                return_copy(a, j).wait_send()
    for d in range(1, 16):
        tp_copy(sq, sqr, tp_s, tp_r, d, tp).wait_send()
    for d in range(1, 16):
        tp_copy(mt, mtr, mt_s, mt_r, d, lax.rem(tp + d, 16)).wait_recv()
    total = mtr[0]
    for i in range(1, 16):
        total = total + mtr[i]
    mean_ref[...] = total
    for d in range(1, 16):
        ctx_copy(d, lax.rem(ctx + d, 16)).wait_recv()
    gains = gsr[0]
    for i in range(1, 16):
        gains = gains + gsr[i]
    gain_ref[...] = gains
    for d in range(1, 16):
        tp_copy(mt, mtr, mt_s, mt_r, d, tp).wait_send()
        ctx_copy(d, ctx).wait_send()


def finish_kernel(
    rq, rk, rv, tot_ref, mean_ref, gain_ref, q_ref, k_ref, qg_ref, kg_ref,
    oq_ref, ok_ref, ov_ref, ogq_ref, ogk_ref,
):
    inverse = lax.rsqrt(tot_ref[...] / D + EPSILON).T
    mean = (mean_ref[...] / D).T
    streams = ((q_ref, qg_ref, rq, oq_ref), (k_ref, kg_ref, rk, ok_ref))
    for which, (ref, gain, back, out) in enumerate(streams):
        grads = [back[j].reshape(TOK, HD) for j in range(2)]
        for b in range(3):
            column = slice(3 * which + b, 3 * which + b + 1)
            unit = ref[chunk(b), :].astype(F32) * inverse[:, column]
            normed_grad = jnp.concatenate([g[chunk(b)] for g in grads], axis=1).astype(F32)
            centred = normed_grad * gain[...] - unit * mean[:, column]
            out[chunk(b), :] = (inverse[:, column] * centred).astype(BF16)
    for j in range(2):
        ov_ref[:, chunk(j)] = rv[j].reshape(TOK, HD)
    ogq_ref[...] = gain_ref[0:1, :]
    ogk_ref[...] = gain_ref[1:2, :]


VM = pl.BlockSpec(memory_space=pltpu.VMEM)
DMA = pltpu.SemaphoreType.DMA
LIMIT = 60000 * 1024


def shape(dims, kind):
    return jax.ShapeDtypeStruct(dims, kind)


def vmem(kind, *dims):
    return pltpu.VMEM(dims, kind)


def per_device(query_proj, key_proj, value_proj, query_gain, key_gain, stripe_of, grad_out):
    y, c = lax.axis_index("y"), lax.axis_index("core")
    by_row = stripe_of.reshape(4, 8)
    entries = []
    counts = []
    sets = []
    for other in (y + 1 - 2 * lax.rem(y, 2), 3 - y):
        mine = lax.dynamic_index_in_dim(by_row, y, 0, False)
        theirs = lax.dynamic_index_in_dim(by_row, other, 0, False)
        sets.append(jnp.concatenate([mine, theirs]))
    seats = jnp.arange(16, dtype=jnp.int32)
    for here, across in ((0, 1), (1, 0)):
        members = sets[here]
        rank = jnp.sum(jnp.where(members[None, :] < members[:, None], 1, 0), axis=1)
        hit = rank[None, :] == seats[:, None]
        entries += [
            members,
            jnp.sum(jnp.where(hit, seats[None, :], 0), axis=1),
            jnp.sum(jnp.where(hit, members[None, :], 0), axis=1),
        ]
        lows = jnp.minimum(members, 31 - members).reshape(2, 2, 2, 2)[:, :, :, 0]
        lows = lax.dynamic_index_in_dim(lows, c, 1, False)[::-1].reshape(4)
        seen = jnp.where(
            jnp.logical_and(sets[across] < 16, sets[across] >= lows[:, None]), 1, 0
        )
        counts.append(2 + (jnp.sum(seen, axis=1) + 3) // 4)
    table = jnp.concatenate(entries + counts).astype(jnp.int32)
    query_gain = query_gain[None, :]
    key_gain = key_gain[None, :]
    back = shape((2, 2, STRIPE, HD), BF16)
    small = shape((8, 128), F32)
    rq, rk, rv, total, mean, gains = pl.pallas_call(
        main_kernel,
        out_shape=(back, back, back, small, small, shape((8, 256), F32)),
        in_specs=[pl.BlockSpec(memory_space=pltpu.SMEM)] + [VM] * 6,
        out_specs=(VM,) * 6,
        scratch_shapes=[vmem(BF16, 2, STRIPE, 256)] * 2
        + [vmem(BF16, 16, STRIPE, HD)] * 4
        + [vmem(BF16, 4, QUAD, HD)] * 4
        + [
            vmem(F32, 8, 128),
            vmem(F32, 16, 8, 128),
            vmem(F32, 4, STEPS, STRIPE, QUAD),
            vmem(F32, 4, STEPS, STRIPE, QUAD),
            vmem(F32, STEPS, STRIPE, 128),
            vmem(F32, 4, 2, STRIPE, 128),
            vmem(F32, STEPS, STRIPE, 128),
            vmem(F32, STEPS, STRIPE, 128),
            vmem(F32, 8, STRIPE, 128),
            vmem(F32, 8, STRIPE, 128),
            vmem(F32, STEPS, STRIPE, HD),
            vmem(F32, STEPS, STRIPE, HD),
            vmem(F32, 256, HD),
            vmem(F32, 4, 24, 256),
            vmem(F32, 2, 8, 256),
            vmem(F32, 2, 8, 256),
            vmem(F32, 4, 1, QUAD),
            vmem(F32, 4, 1, QUAD),
            vmem(jnp.int32, 4, 1, QUAD),
            vmem(jnp.int32, 4, 1, QUAD),
        ]
        + [vmem(F32, 8, STRIPE, HD)] * 3
        + [vmem(BF16, 8, STRIPE, HD)] * 3
        + [vmem(BF16, 4, STRIPE, HD)] * 6
        + [
            vmem(F32, 8, 128),
            vmem(F32, 16, 8, 128),
            vmem(F32, 8, 256),
            vmem(F32, 16, 8, 256),
            DMA((4, 2)),
            DMA((4, 2)),
            DMA((4, 2)),
            DMA((4, 2)),
            DMA((4, 2)),
            DMA((4, 2)),
            DMA((16,)),
            DMA((16,)),
            DMA((4,)),
            DMA((4,)),
            DMA((3,)),
            DMA((3,)),
            DMA((3, 2)),
            DMA((3, 2)),
            DMA((16,)),
            DMA((16,)),
            DMA((16,)),
            DMA((16,)),
        ],
        compiler_params=pltpu.CompilerParams(
            collective_id=1, has_side_effects=True, vmem_limit_bytes=LIMIT
        ),
        name="main",
    )(
        table,
        *(a.reshape(2, STRIPE, 256) for a in (query_proj, key_proj, value_proj, grad_out)),
        query_gain,
        key_gain,
    )

    out = shape((TOK, 256), BF16)
    gain_out = shape((1, 256), F32)
    grad_query, grad_key, grad_value, gain_q, gain_k = pl.pallas_call(
        finish_kernel,
        out_shape=(out, out, out, gain_out, gain_out),
        in_specs=[VM] * 10,
        out_specs=(VM,) * 5,
        name="finish",
    )(rq, rk, rv, total, mean, gains, query_proj, key_proj, query_gain, key_gain)
    return (grad_query, grad_key, grad_value, gain_q[0], gain_k[0])


def solution(mesh):
    torus = Mesh(mesh.devices.reshape(4, 4, 8, 2), AXES)
    wide = P(("y", "x"), ("z", "core"))
    thin = P(("z", "core"))
    return jax.shard_map(
        per_device,
        mesh=torus,
        in_specs=(wide, wide, wide, thin, thin, P(), wide),
        out_specs=(wide, wide, wide, thin, thin),
        check_vma=False,
    )
```

```python
import jax
import jax.numpy as jnp
from jax import lax
from jax.experimental import pallas as pl
from jax.experimental.pallas import tpu as pltpu
from jax.sharding import Mesh
from jax.sharding import PartitionSpec as P

HD = 128
D = 4096
SEQ = 6144
TOK = 384
STRIPE = 192
QUAD = 768
OWN = 768
STEPS = 5
QS, QIDX, QST, KS, KIDX, KST, QCOUNT, KCOUNT = 0, 16, 32, 48, 64, 80, 96, 100
EPSILON = 1e-06
AXES = ("y", "x", "z", "core")
MESH = pl.DeviceIdType.MESH
ROOT = HD**-0.5
LOG2E = 1.4426950408889634
SCALE = ROOT * LOG2E
NEG = -1e30
F32 = jnp.float32
BF16 = jnp.bfloat16


def place():
    return tuple(lax.axis_index(a) for a in AXES)


def tp_peer(y, x, z, c, d):
    t = lax.rem(z * 2 + c + d, 16)
    return (y, x, t // 2, lax.rem(t, 2))


def dot_t(a, b):
    return lax.dot_general(a, b, (((1,), (1,)), ((), ())), preferred_element_type=F32)


def dot_n(a, b):
    return lax.dot_general(a, b, (((1,), (0,)), ((), ())), preferred_element_type=F32)


def rows_of(block):
    folded = block[:, :128] + block[:, 128:]
    return [
        jnp.sum(folded[b * 128 : (b + 1) * 128].T, axis=0, keepdims=True) for b in range(3)
    ]


def signal(device):
    pl.semaphore_signal(
        pltpu.get_barrier_semaphore(), inc=1, device_id=device, device_id_type=MESH
    )


def remote(src, dst, send_sem, recv_sem, device):
    return pltpu.make_async_remote_copy(
        src_ref=src,
        dst_ref=dst,
        send_sem=send_sem,
        recv_sem=recv_sem,
        device_id=device,
        device_id_type=MESH,
    )


def sort_keys(keys):
    keys = list(keys)
    n, p = len(keys), 1
    while p < n:
        k = p
        while k >= 1:
            for j in range(k % p, n - k, 2 * k):
                for i in range(min(k, n - j - k)):
                    if (i + j) // (2 * p) == (i + j + k) // (2 * p):
                        a, b = keys[i + j], keys[i + j + k]
                        keys[i + j], keys[i + j + k] = jnp.minimum(a, b), jnp.maximum(a, b)
            k //= 2
        p *= 2
    return keys


def chunk(i):
    return slice(i * 128, (i + 1) * 128)


def main_kernel(
    stripes, q_ref, k_ref, v_ref, g_ref, qg_ref, kg_ref,
    rq, rk, rv, tot_ref, mean_ref, gain_ref,
    qn, kn, all_v, all_k, all_g, all_q, vp, kp, gp, qp,
    sq, sqr, ss, dps, ms, mm, ls, ws, lz, dl, acc, acc2, tile, st_all, fin_l, fin_d,
    lse, dlt, kpos, qpos, dq_all, dk_all, dv_all, dq_send, dk_send, dv_send,
    dq_got, dk_got, dv_got, dq_ret, dk_ret, dv_ret, mt, mtr, gs, gsr,
    row_s, row_r, y_s, y_r, sib_s, sib_r, tp_s, tp_r, st_s, st_r, red_s, red_r,
    ret_s, ret_r, mt_s, mt_r, cx_s, cx_r, cy_s, cy_r, gy, gyr, table,
):
    y, x, z, c = place()
    half = x // 2
    parity = lax.rem(x, 2)
    tp = z * 2 + c
    sibling = (y, x, z, 1 - c)
    y_query = y + 1 - 2 * lax.rem(y, 2)
    y_key = 3 - y

    def x_peer(d):
        return (y, lax.rem(x + d, 4), z, c)

    def y_peer(d):
        return (lax.rem(y + d, 4), x, z, c)

    for j in range(2):
        @pl.when(2 * c + j != x)
        def _():
            signal((y, 2 * c + j, z, half))
    for d in range(1, 4):
        signal(x_peer(d))
        signal(y_peer(d))
    signal((y_query, x, z, 1 - c))
    for d in range(1, 16):
        signal(tp_peer(y, x, z, c, d))

    ordered = []
    for at, other in ((QS, y_query), (KS, y_key)):
        members = [stripes[y * 8 + i] for i in range(8)]
        members += [stripes[other * 8 + i] for i in range(8)]
        keys = sort_keys([m * 16 + i for i, m in enumerate(members)])
        for i in range(16):
            table[at + i] = members[i]
            table[at + 16 + i] = keys[i] & 15
            table[at + 32 + i] = keys[i] >> 4
        ordered.append([k >> 4 for k in keys[:8]])
    for at, count_at, across in ((QS, QCOUNT, ordered[1]), (KS, KCOUNT, ordered[0])):
        for p in range(4):
            first = table[at + c * 4 + 2 * (p % 2) + 8 * (1 - p // 2)]
            low = jnp.minimum(first, 31 - first)
            seen = 3
            for other in across:
                seen = seen + jnp.where(other >= low, 1, 0)
            table[count_at + p] = 2 + (seen >> 2)

    rows = []
    for ref in (q_ref, k_ref):
        wide = ref[...].astype(F32).reshape(TOK, 256)
        rows += rows_of(wide * wide)
    for i, row in enumerate(rows):
        sq[i : i + 1, :] = row
    sq[6:8, :] = jnp.zeros((2, 128), F32)
    sqr[pl.ds(tp, 1)] = sq[...][None]
    lane = lax.broadcasted_iota(jnp.int32, (1, QUAD), 1)
    for sorted_at, out in ((KST, kpos), (QST, qpos)):
        for quad in range(4):
            base = [(table[sorted_at + quad * 4 + i] - i) * STRIPE for i in range(4)]
            shift = jnp.where(
                lane < 2 * STRIPE,
                jnp.where(lane < STRIPE, base[0], base[1]),
                jnp.where(lane < 3 * STRIPE, base[2], base[3]),
            )
            out[quad] = lane + shift
    tile[STRIPE:256, :] = jnp.zeros((256 - STRIPE, HD), F32)
    for p in range(4):
        for side in range(2):
            mm[p, side] = jnp.zeros((STRIPE, 128), F32)
    mine = jnp.where(half == c, 1, 0)
    pl.semaphore_wait(pltpu.get_barrier_semaphore(), 24 - mine)

    V, K, G, Q = range(4)
    sources = (v_ref, kn, g_ref, qn)
    alls = (all_v, all_k, all_g, all_q)
    partners = ((y_key, x, z, c), (y_key, x, z, c), (y_query, x, z, c), (y_query, x, z, c))

    def row_copy(a, j):
        return remote(
            sources[a].at[:, :, chunk(j)],
            alls[a].at[pl.ds(half * 4 + parity * 2, 2)],
            row_s.at[a, j],
            row_r.at[a, parity],
            (y, 2 * c + j, z, half),
        )

    def row_start(a):
        for j in range(2):
            @pl.when(2 * c + j != x)
            def _():
                row_copy(a, j).start()

            @pl.when(2 * c + j == x)
            def _():
                pltpu.make_async_copy(
                    sources[a].at[:, :, chunk(j)],
                    alls[a].at[pl.ds(half * 4 + parity * 2, 2)],
                    row_r.at[a, parity],
                ).start()

    def y_copy(a, j):
        return remote(
            alls[a].at[pl.ds(c * 4 + j * 2, 2)],
            alls[a].at[pl.ds(8 + c * 4 + j * 2, 2)],
            y_s.at[a, j],
            y_r.at[a, j],
            partners[a],
        )

    def sib_copy(a, which, core):
        part = alls[a].at[pl.ds(which * 8 + core * 4, 4)]
        return remote(part, part, sib_s.at[a, which], sib_r.at[a, which], sibling)

    def spread(a):
        for j in range(2):
            part = alls[a].at[pl.ds(c * 4 + j * 2, 2)]
            remote(part, part, row_s.at[a, j], row_r.at[a, j], sibling).wait_recv()
            y_copy(a, j).start()
        sib_copy(a, 0, c).start()

    def arrive(a):
        for j in range(2):
            part = alls[a].at[pl.ds(8 + c * 4 + j * 2, 2)]
            remote(part, part, y_s.at[a, j], y_r.at[a, j], sibling).wait_recv()
        sib_copy(a, 1, c).start()

    def settle(a, order, target):
        for which in range(2):
            sib_copy(a, which, 1 - c).wait_recv()
        for s in range(16):
            target[s // 4, s % 4 * STRIPE : (s % 4 + 1) * STRIPE, :] = alls[a][table[order + s]]

    row_start(V)

    def tp_copy(src, dst, send, recv, d, slot):
        return remote(src, dst.at[slot], send.at[d], recv.at[slot], tp_peer(y, x, z, c, d))

    for d in range(1, 16):
        tp_copy(sq, sqr, tp_s, tp_r, d, tp).start()
    row_start(G)
    spread(V)
    for d in range(1, 16):
        tp_copy(sq, sqr, tp_s, tp_r, d, lax.rem(tp + d, 16)).wait_recv()
    total = sqr[0]
    for i in range(1, 16):
        total = total + sqr[i]
    tot_ref[...] = total
    inverse = lax.rsqrt(total / D + EPSILON).T
    for ref, gain, out, base, a in ((k_ref, kg_ref, kn, 3, K), (q_ref, qg_ref, qn, 0, Q)):
        wide = ref[...].astype(F32).reshape(TOK, 256)
        parts = []
        for b in range(3):
            unit = wide[chunk(b)] * inverse[:, base + b : base + b + 1]
            parts.append(unit * gain[...])
        out[...] = jnp.concatenate(parts, axis=0).reshape(2, STRIPE, 256).astype(BF16)
        row_start(a)

    def pair_of(set_at, count_at, p):
        base = c * 4 + 2 * lax.rem(p, 2) + 8 * (1 - p // 2)
        first = table[set_at + base]
        first_high = first >= 16
        high = jnp.where(first_high, first, 31 - first)
        high_at = jnp.where(first_high, 0, 1)
        return base, first_high, high, high_at, table[count_at + p]

    def row_step(p, t):
        base, first_high, high, high_at, count = pair_of(QS, QCOUNT, p)
        is_high = t < count
        side = jnp.where(is_high, high_at, 1 - high_at)
        stripe = jnp.where(is_high, high, 31 - high)
        quad = jnp.where(is_high, t, t - count)
        return base + side, side, stripe, jnp.clip(quad, 0, 3)

    def column_step(p, t):
        base, first_high, high, high_at, count = pair_of(KS, KCOUNT, p)
        is_low = t < count
        side = jnp.where(is_low, 1 - high_at, high_at)
        stripe = jnp.where(is_low, 31 - high, high)
        quad = jnp.where(is_low, 4 - count + t, t - 1)
        return base + side, stripe, jnp.clip(quad, 0, 3)

    def split(ref, count, start, join):
        two, three = 2 < count, 3 < count
        first = join(ref[0], ref[1])
        first = join(first, jnp.where(two, ref[2], start))
        first = join(first, jnp.where(three, ref[3], start))
        second = join(ref[4], jnp.where(two, start, ref[2]))
        second = join(second, jnp.where(three, start, ref[3]))
        return first, second

    def loop(lower, upper, body):
        def one(p, carry):
            body(p)
            return carry

        lax.fori_loop(lower, upper, one, 0)

    def grad_probs(p):
        for t in range(STEPS):
            slot, side, stripe, quad = row_step(p, t)
            dps[p, t] = dot_t(all_g[slot], vp[quad])

    def score(p):
        base, first_high, high, high_at, count = pair_of(QS, QCOUNT, p)
        row = lax.broadcasted_iota(jnp.int32, (STRIPE, QUAD), 0)
        for t in range(STEPS):
            slot, side, stripe, quad = row_step(p, t)
            s = dot_t(all_q[slot], kp[quad]) * SCALE
            s = jnp.where(kpos[quad] - stripe * STRIPE <= row, s, NEG)
            ss[p, t] = s
            most = s[:, chunk(0)]
            for i in range(1, 6):
                most = jnp.maximum(most, s[:, chunk(i)])
            ms[t] = most
        for side, most in enumerate(split(ms, count, NEG, jnp.maximum)):
            at = high_at if side == 0 else 1 - high_at
            wide = jnp.broadcast_to(jnp.max(most, axis=1, keepdims=True), (STRIPE, 128))
            mm[p, 0] = jnp.where(at == 0, wide, mm[p, 0])
            mm[p, 1] = jnp.where(at == 1, wide, mm[p, 1])

    def sums(p):
        base, first_high, high, high_at, count = pair_of(QS, QCOUNT, p)
        for t in range(STEPS):
            slot, side, stripe, quad = row_step(p, t)
            most = mm[p, side]
            l = jnp.zeros((STRIPE, 128), F32)
            w = jnp.zeros((STRIPE, 128), F32)
            for i in range(6):
                e = jnp.exp2(ss[p, t, :, chunk(i)] - most)
                l = l + e
                w = w + e * dps[p, t, :, chunk(i)]
            ls[t] = l
            ws[t] = w
        l_ends = [jnp.sum(v, axis=1, keepdims=True) for v in split(ls, count, 0.0, jnp.add)]
        w_ends = [jnp.sum(v, axis=1, keepdims=True) for v in split(ws, count, 0.0, jnp.add)]
        lane = lax.broadcasted_iota(jnp.int32, (STRIPE, HD), 1)
        for side in range(2):
            take_first = first_high if side == 0 else jnp.logical_not(first_high)
            l = jnp.where(take_first, l_ends[0], l_ends[1])
            w = jnp.where(take_first, w_ends[0], w_ends[1])
            tile[0:STRIPE, :] = jnp.where(
                lane == 0, mm[p, side], jnp.where(lane == 1, l, w)
            )
            turned = tile[...].T
            for i in range(3):
                st_all[0, pl.ds(i * 8 + p * 2 + side, 1), :] = turned[i : i + 1, :]

    def query_grad(p):
        base, first_high, high, high_at, count = pair_of(QS, QCOUNT, p)
        for t in range(STEPS):
            slot, side, stripe, quad = row_step(p, t)
            log_total = lz[p * 2 + side]
            delta = dl[p * 2 + side]
            parts = []
            for i in range(6):
                probs = jnp.exp2(ss[p, t, :, chunk(i)] - log_total)
                parts.append((probs * (dps[p, t, :, chunk(i)] - delta)).astype(BF16))
            acc[t] = dot_n(jnp.concatenate(parts, axis=1), kp[quad])
        ends = split(acc, count, 0.0, jnp.add)
        for side in range(2):
            take_first = first_high if side == 0 else jnp.logical_not(first_high)
            value = jnp.where(take_first, ends[0], ends[1]) * ROOT
            dq_all[p * 2 + side] = value
            dq_send[p * 2 + side] = value.astype(BF16)

    def key_grads(p):
        base, first_high, high, high_at, count = pair_of(KS, KCOUNT, p)
        row = lax.broadcasted_iota(jnp.int32, (STRIPE, QUAD), 0)
        for t in range(STEPS):
            slot, stripe, quad = column_step(p, t)
            qv = qp[quad]
            gv = gp[quad]
            s = dot_t(all_k[slot], qv) * SCALE - lse[quad]
            probs = jnp.where(row <= qpos[quad] - stripe * STRIPE, jnp.exp2(s), 0.0)
            dp = dot_t(all_v[slot], gv)
            ds = (probs * (dp - dlt[quad])).astype(BF16)
            acc[t] = dot_n(probs.astype(BF16), gv)
            acc2[t] = dot_n(ds, qv)
        for source, scale, out, send in ((acc, None, dv_all, dv_send), (acc2, ROOT, dk_all, dk_send)):
            ends = split(source, count, 0.0, jnp.add)
            for side in range(2):
                take_low = jnp.logical_not(first_high) if side == 0 else first_high
                value = jnp.where(take_low, ends[0], ends[1])
                value = value if scale is None else value * scale
                out[p * 2 + side] = value
                send[p * 2 + side] = value.astype(BF16)

    spread(G)
    arrive(V)
    arrive(G)
    spread(K)
    settle(V, KIDX, vp)
    settle(G, QIDX, gp)
    loop(0, 2, grad_probs)
    spread(Q)
    loop(2, 4, grad_probs)
    arrive(K)
    arrive(Q)
    settle(K, KIDX, kp)
    settle(Q, QIDX, qp)
    loop(0, 4, score)
    loop(0, 4, sums)

    stat_peers = (None, (y_query, x, z, c), sibling, (y_query, x, z, 1 - c))

    def stat_copy(i):
        return remote(st_all.at[0], st_all.at[i], st_s.at[i], st_r.at[i], stat_peers[i])

    for i in range(1, 4):
        stat_copy(i).start()
    for i in range(1, 4):
        stat_copy(i).wait_recv()
    for which in range(2):
        mine, other = st_all[2 * which], st_all[2 * which + 1]
        other = jnp.concatenate(
            [other[i * 8 + r : i * 8 + r + 4] for i in range(3) for r in (4, 0)], axis=0
        )
        most = jnp.maximum(mine[0:8], other[0:8])
        left, right = jnp.exp2(mine[0:8] - most), jnp.exp2(other[0:8] - most)
        l = mine[8:16] * left + other[8:16] * right
        w = mine[16:24] * left + other[16:24] * right
        log_total = most + jnp.log2(l)
        delta = w / l
        core = c if which == 0 else 1 - c
        fin_l[core] = log_total
        fin_d[core] = delta
        if which == 0:
            turned_l, turned_d = log_total.T, delta.T
            for i in range(8):
                lz[i] = jnp.broadcast_to(turned_l[0:STRIPE, i : i + 1], (STRIPE, 128))
                dl[i] = jnp.broadcast_to(turned_d[0:STRIPE, i : i + 1], (STRIPE, 128))

    reduces = (
        (dq_send, dq_got, (y_query, x, z, c)),
        (dk_send, dk_got, (y_key, x, z, c)),
        (dv_send, dv_got, (y_key, x, z, c)),
    )

    def reduce_copy(a, p):
        send, got, device = reduces[a]
        part = pl.ds(2 * p, 2)
        return remote(send.at[part], got.at[part], red_s.at[a, p], red_r.at[a, p], device)

    returns = ((dq_ret, rq), (dk_ret, rk), (dv_ret, rv))

    def return_copy(a, j):
        out, back = returns[a]
        return remote(
            out.at[pl.ds(j * 2, 2)],
            back.at[parity],
            ret_s.at[a, j],
            ret_r.at[a, parity],
            (y, 2 * c + j, z, half),
        )

    def return_start(a, j):
        out, back = returns[a]

        @pl.when(2 * c + j != x)
        def _():
            return_copy(a, j).start()

        @pl.when(2 * c + j == x)
        def _():
            pltpu.make_async_copy(
                out.at[pl.ds(j * 2, 2)], back.at[parity], ret_r.at[a, parity]
            ).start()

    def return_wait(a):
        back = returns[a][1]
        for j in range(2):
            remote(
                back.at[j], back.at[j], ret_s.at[a, j], ret_r.at[a, j], sibling
            ).wait_recv()

    def join(a, mine, p):
        reduce_copy(a, p).wait_recv()
        for i in (2 * p, 2 * p + 1):
            returns[a][0][i] = (mine[4 + i] + reduces[a][1][i].astype(F32)).astype(BF16)
        return_start(a, p)

    for quad in range(4):
        parts = [[], []]
        for i in range(4):
            at = table[QIDX + quad * 4 + i]
            core = lax.rem(at // 4, 2)
            row = lax.rem(at, 4) + 4 * (1 - at // 8)
            parts[0].append(fin_l[core, pl.ds(row, 1), 0:STRIPE])
            parts[1].append(fin_d[core, pl.ds(row, 1), 0:STRIPE])
        lse[quad] = jnp.concatenate(parts[0], axis=1)
        dlt[quad] = jnp.concatenate(parts[1], axis=1)
    for p in range(2):
        key_grads(p)
        reduce_copy(2, p).start()
        reduce_copy(1, p).start()
    loop(0, 2, query_grad)
    for p in range(2):
        reduce_copy(0, p).start()
    loop(2, 4, query_grad)
    for p in range(2):
        join(0, dq_all, p)
    for p in range(2):
        key_grads(2 + p)
        join(1, dk_all, p)
        join(2, dv_all, p)

    streams = ((q_ref, qg_ref, rq), (k_ref, kg_ref, rk))
    gs[...] = jnp.zeros((8, 256), F32)
    mt[...] = jnp.zeros((8, 128), F32)
    for which, (ref, gain, back) in enumerate(streams):
        return_wait(which)
        gain_sum = jnp.zeros((1, 256), F32)
        wide = ref[...].astype(F32).reshape(TOK, 256)
        grads = [back[j].reshape(TOK, HD) for j in range(2)]
        for b in range(3):
            scale = inverse[:, 3 * which + b : 3 * which + b + 1]
            unit = wide[chunk(b)] * scale
            normed_grad = jnp.concatenate([g[chunk(b)] for g in grads], axis=1).astype(F32)
            product = normed_grad * unit
            gain_sum = gain_sum + jnp.sum(product, axis=0, keepdims=True)
            weighted = product * gain[...]
            folded = weighted[:, :128] + weighted[:, 128:]
            mt[3 * which + b : 3 * which + b + 1, :] = jnp.sum(folded.T, axis=0, keepdims=True)
        gs[which : which + 1, :] = gain_sum

    def x_copy(d, slot):
        return remote(gs, gsr.at[slot], cx_s.at[d], cx_r.at[slot], x_peer(d))

    def gain_copy(d, slot):
        return remote(gy, gyr.at[slot], cy_s.at[d], cy_r.at[slot], y_peer(d))

    for d in range(1, 16):
        tp_copy(mt, mtr, mt_s, mt_r, d, tp).start()
    for d in range(1, 4):
        x_copy(d, x).start()
    mtr[pl.ds(tp, 1)] = mt[...][None]
    gsr[pl.ds(x, 1)] = gs[...][None]
    for d in range(1, 4):
        x_copy(d, lax.rem(x + d, 4)).wait_recv()
    gains = (gsr[0] + gsr[1]) + (gsr[2] + gsr[3])
    gy[...] = gains
    gyr[pl.ds(y, 1)] = gains[None]
    for d in range(1, 4):
        gain_copy(d, y).start()
    return_wait(2)
    for a in range(4):
        for j in range(2):
            @pl.when(2 * c + j != x)
            def _():
                row_copy(a, j).wait_send()
            y_copy(a, j).wait_send()
            sib_copy(a, j, c).wait_send()
    for i in range(1, 4):
        stat_copy(i).wait_send()
    for a in range(3):
        for j in range(2):
            reduce_copy(a, j).wait_send()

            @pl.when(2 * c + j != x)
            def _():
                return_copy(a, j).wait_send()
    for d in range(1, 16):
        tp_copy(sq, sqr, tp_s, tp_r, d, tp).wait_send()
    for d in range(1, 16):
        tp_copy(mt, mtr, mt_s, mt_r, d, lax.rem(tp + d, 16)).wait_recv()
    total = mtr[0]
    for i in range(1, 16):
        total = total + mtr[i]
    mean_ref[...] = total
    for d in range(1, 4):
        gain_copy(d, lax.rem(y + d, 4)).wait_recv()
    gain_ref[...] = (gyr[0] + gyr[1]) + (gyr[2] + gyr[3])
    for d in range(1, 16):
        tp_copy(mt, mtr, mt_s, mt_r, d, tp).wait_send()
    for d in range(1, 4):
        x_copy(d, x).wait_send()
        gain_copy(d, y).wait_send()


def finish_kernel(
    rq, rk, rv, tot_ref, mean_ref, gain_ref, q_ref, k_ref, qg_ref, kg_ref,
    oq_ref, ok_ref, ov_ref, ogq_ref, ogk_ref,
):
    inverse = lax.rsqrt(tot_ref[...] / D + EPSILON).T
    mean = (mean_ref[...] / D).T
    streams = ((q_ref, qg_ref, rq, oq_ref), (k_ref, kg_ref, rk, ok_ref))
    for which, (ref, gain, back, out) in enumerate(streams):
        grads = [back[j].reshape(TOK, HD) for j in range(2)]
        for b in range(3):
            column = slice(3 * which + b, 3 * which + b + 1)
            unit = ref[chunk(b), :].astype(F32) * inverse[:, column]
            normed_grad = jnp.concatenate([g[chunk(b)] for g in grads], axis=1).astype(F32)
            centred = normed_grad * gain[...] - unit * mean[:, column]
            out[chunk(b), :] = (inverse[:, column] * centred).astype(BF16)
    for j in range(2):
        ov_ref[:, chunk(j)] = rv[j].reshape(TOK, HD)
    ogq_ref[...] = gain_ref[0:1, :]
    ogk_ref[...] = gain_ref[1:2, :]


VM = pl.BlockSpec(memory_space=pltpu.VMEM)
DMA = pltpu.SemaphoreType.DMA
LIMIT = 60000 * 1024


def shape(dims, kind):
    return jax.ShapeDtypeStruct(dims, kind)


def vmem(kind, *dims):
    return pltpu.VMEM(dims, kind)


def per_device(query_proj, key_proj, value_proj, query_gain, key_gain, stripe_of, grad_out):
    query_gain = query_gain[None, :]
    key_gain = key_gain[None, :]
    back = shape((2, 2, STRIPE, HD), BF16)
    small = shape((8, 128), F32)
    rq, rk, rv, total, mean, gains = pl.pallas_call(
        main_kernel,
        out_shape=(back, back, back, small, small, shape((8, 256), F32)),
        in_specs=[pl.BlockSpec(memory_space=pltpu.SMEM)] + [VM] * 6,
        out_specs=(VM,) * 6,
        scratch_shapes=[vmem(BF16, 2, STRIPE, 256)] * 2
        + [vmem(BF16, 16, STRIPE, HD)] * 4
        + [vmem(BF16, 4, QUAD, HD)] * 4
        + [
            vmem(F32, 8, 128),
            vmem(F32, 16, 8, 128),
            vmem(F32, 4, STEPS, STRIPE, QUAD),
            vmem(F32, 4, STEPS, STRIPE, QUAD),
            vmem(F32, STEPS, STRIPE, 128),
            vmem(F32, 4, 2, STRIPE, 128),
            vmem(F32, STEPS, STRIPE, 128),
            vmem(F32, STEPS, STRIPE, 128),
            vmem(F32, 8, STRIPE, 128),
            vmem(F32, 8, STRIPE, 128),
            vmem(F32, STEPS, STRIPE, HD),
            vmem(F32, STEPS, STRIPE, HD),
            vmem(F32, 256, HD),
            vmem(F32, 4, 24, 256),
            vmem(F32, 2, 8, 256),
            vmem(F32, 2, 8, 256),
            vmem(F32, 4, 1, QUAD),
            vmem(F32, 4, 1, QUAD),
            vmem(jnp.int32, 4, 1, QUAD),
            vmem(jnp.int32, 4, 1, QUAD),
        ]
        + [vmem(F32, 8, STRIPE, HD)] * 3
        + [vmem(BF16, 8, STRIPE, HD)] * 3
        + [vmem(BF16, 4, STRIPE, HD)] * 6
        + [
            vmem(F32, 8, 128),
            vmem(F32, 16, 8, 128),
            vmem(F32, 8, 256),
            vmem(F32, 4, 8, 256),
            DMA((4, 2)),
            DMA((4, 2)),
            DMA((4, 2)),
            DMA((4, 2)),
            DMA((4, 2)),
            DMA((4, 2)),
            DMA((16,)),
            DMA((16,)),
            DMA((4,)),
            DMA((4,)),
            DMA((3, 2)),
            DMA((3, 2)),
            DMA((3, 2)),
            DMA((3, 2)),
            DMA((16,)),
            DMA((16,)),
            DMA((4,)),
            DMA((4,)),
            DMA((4,)),
            DMA((4,)),
            vmem(F32, 8, 256),
            vmem(F32, 4, 8, 256),
            pltpu.SMEM((104,), jnp.int32),
        ],
        compiler_params=pltpu.CompilerParams(
            collective_id=1, has_side_effects=True, vmem_limit_bytes=LIMIT
        ),
        name="main",
    )(
        stripe_of,
        *(a.reshape(2, STRIPE, 256) for a in (query_proj, key_proj, value_proj, grad_out)),
        query_gain,
        key_gain,
    )

    out = shape((TOK, 256), BF16)
    gain_out = shape((1, 256), F32)
    grad_query, grad_key, grad_value, gain_q, gain_k = pl.pallas_call(
        finish_kernel,
        out_shape=(out, out, out, gain_out, gain_out),
        in_specs=[VM] * 10,
        out_specs=(VM,) * 5,
        name="finish",
    )(rq, rk, rv, total, mean, gains, query_proj, key_proj, query_gain, key_gain)
    return (grad_query, grad_key, grad_value, gain_q[0], gain_k[0])


def solution(mesh):
    torus = Mesh(mesh.devices.reshape(4, 4, 8, 2), AXES)
    wide = P(("y", "x"), ("z", "core"))
    thin = P(("z", "core"))
    return jax.shard_map(
        per_device,
        mesh=torus,
        in_specs=(wide, wide, wide, thin, thin, P(), wide),
        out_specs=(wide, wide, wide, thin, thin),
        check_vma=False,
    )
```

```python
import jax
import jax.numpy as jnp
from jax import lax
from jax.experimental import pallas as pl
from jax.experimental.pallas import tpu as pltpu
from jax.sharding import Mesh
from jax.sharding import PartitionSpec as P

HD = 128
D = 4096
SEQ = 6144
TOK = 384
STRIPE = 192
QUAD = 768
OWN = 768
STEPS = 5
QS, QIDX, QST, KS, KIDX, KST, QCOUNT, KCOUNT = 0, 16, 32, 48, 64, 80, 96, 100
EPSILON = 1e-06
AXES = ("y", "x", "z", "core")
MESH = pl.DeviceIdType.MESH
ROOT = HD**-0.5
LOG2E = 1.4426950408889634
SCALE = ROOT * LOG2E
NEG = -1e30
F32 = jnp.float32
BF16 = jnp.bfloat16


def place():
    return tuple(lax.axis_index(a) for a in AXES)


def tp_peer(y, x, z, c, d):
    t = lax.rem(z * 2 + c + d, 16)
    return (y, x, t // 2, lax.rem(t, 2))


def dot_t(a, b):
    return lax.dot_general(a, b, (((1,), (1,)), ((), ())), preferred_element_type=F32)


def dot_n(a, b):
    return lax.dot_general(a, b, (((1,), (0,)), ((), ())), preferred_element_type=F32)


def rows_of(block):
    folded = block[:, :128] + block[:, 128:]
    return [
        jnp.sum(folded[b * 128 : (b + 1) * 128].T, axis=0, keepdims=True) for b in range(3)
    ]


def signal(device):
    pl.semaphore_signal(
        pltpu.get_barrier_semaphore(), inc=1, device_id=device, device_id_type=MESH
    )


def remote(src, dst, send_sem, recv_sem, device):
    return pltpu.make_async_remote_copy(
        src_ref=src,
        dst_ref=dst,
        send_sem=send_sem,
        recv_sem=recv_sem,
        device_id=device,
        device_id_type=MESH,
    )


def sort_keys(keys):
    keys = list(keys)
    n, p = len(keys), 1
    while p < n:
        k = p
        while k >= 1:
            for j in range(k % p, n - k, 2 * k):
                for i in range(min(k, n - j - k)):
                    if (i + j) // (2 * p) == (i + j + k) // (2 * p):
                        a, b = keys[i + j], keys[i + j + k]
                        keys[i + j], keys[i + j + k] = jnp.minimum(a, b), jnp.maximum(a, b)
            k //= 2
        p *= 2
    return keys


def chunk(i):
    return slice(i * 128, (i + 1) * 128)


def main_kernel(
    stripes, q_ref, k_ref, v_ref, g_ref, qg_ref, kg_ref,
    rq, rk, rv, tot_ref, mean_ref, gain_ref,
    qn, kn, all_v, all_k, all_g, all_q, mine_g, mine_q, vp, kp, gp, qp,
    sq, sqr, ss, dps, ms, mm, ls, ws, lz, dl, acc, acc2, tile, st_all, fin_l, fin_d,
    lse, dlt, kpos, qpos, dq_all, dk_all, dv_all, dq_send, dk_send, dv_send,
    dq_got, dk_got, dv_got, dq_ret, dk_ret, dv_ret, mt, mtr, gs, gsr,
    row_s, row_r, y_s, y_r, sib_s, sib_r, tp_s, tp_r, st_s, st_r, red_s, red_r,
    ret_s, ret_r, mt_s, mt_r, cx_s, cx_r, cy_s, cy_r, gy, gyr, table,
):
    y, x, z, c = place()
    half = x // 2
    parity = lax.rem(x, 2)
    tp = z * 2 + c
    sibling = (y, x, z, 1 - c)
    y_query = y + 1 - 2 * lax.rem(y, 2)
    y_key = 3 - y

    def x_peer(d):
        return (y, lax.rem(x + d, 4), z, c)

    def y_peer(d):
        return (lax.rem(y + d, 4), x, z, c)

    for j in range(2):
        @pl.when(2 * c + j != x)
        def _():
            signal((y, 2 * c + j, z, half))
    for d in range(1, 4):
        signal(x_peer(d))
        signal(y_peer(d))
    signal((y_query, x, z, 1 - c))
    for d in range(1, 16):
        signal(tp_peer(y, x, z, c, d))

    ordered = []
    for at, other in ((QS, y_query), (KS, y_key)):
        members = [stripes[y * 8 + i] for i in range(8)]
        members += [stripes[other * 8 + i] for i in range(8)]
        keys = sort_keys([m * 16 + i for i, m in enumerate(members)])
        for i in range(16):
            table[at + i] = members[i]
            table[at + 16 + i] = keys[i] & 15
            table[at + 32 + i] = keys[i] >> 4
        ordered.append([k >> 4 for k in keys[:8]])
    for at, count_at, across in ((QS, QCOUNT, ordered[1]), (KS, KCOUNT, ordered[0])):
        for p in range(4):
            first = table[at + c * 4 + 2 * (p % 2) + 8 * (1 - p // 2)]
            low = jnp.minimum(first, 31 - first)
            seen = 3
            for other in across:
                seen = seen + jnp.where(other >= low, 1, 0)
            table[count_at + p] = 2 + (seen >> 2)

    rows = []
    for ref in (q_ref, k_ref):
        wide = ref[...].astype(F32).reshape(TOK, 256)
        rows += rows_of(wide * wide)
    for i, row in enumerate(rows):
        sq[i : i + 1, :] = row
    sq[6:8, :] = jnp.zeros((2, 128), F32)
    sqr[pl.ds(tp, 1)] = sq[...][None]
    lane = lax.broadcasted_iota(jnp.int32, (1, QUAD), 1)
    for sorted_at, out in ((KST, kpos), (QST, qpos)):
        for quad in range(4):
            base = [(table[sorted_at + quad * 4 + i] - i) * STRIPE for i in range(4)]
            shift = jnp.where(
                lane < 2 * STRIPE,
                jnp.where(lane < STRIPE, base[0], base[1]),
                jnp.where(lane < 3 * STRIPE, base[2], base[3]),
            )
            out[quad] = lane + shift
    tile[STRIPE:256, :] = jnp.zeros((256 - STRIPE, HD), F32)
    for p in range(4):
        for side in range(2):
            mm[p, side] = jnp.zeros((STRIPE, 128), F32)
    mine = jnp.where(half == c, 1, 0)
    pl.semaphore_wait(pltpu.get_barrier_semaphore(), 24 - mine)

    V, K, G, Q = range(4)
    sources = (v_ref, kn, g_ref, qn)
    alls = (all_v, all_k, all_g, all_q)
    held = (all_v, all_k, mine_g, mine_q)
    partners = ((y_key, x, z, c), (y_key, x, z, c), (y_query, x, z, c), (y_query, x, z, c))

    def seat(a, block, core, start, size):
        if a < 2:
            return held[a].at[pl.ds(block * 8 + core * 4 + start, size)]
        return held[a].at[pl.ds(block * 4 + start, size)]

    def row_copy(a, j):
        return remote(
            sources[a].at[:, :, chunk(j)],
            seat(a, 0, half, parity * 2, 2),
            row_s.at[a, j],
            row_r.at[a, parity],
            (y, 2 * c + j, z, half),
        )

    def row_start(a):
        for j in range(2):
            @pl.when(2 * c + j != x)
            def _():
                row_copy(a, j).start()

            @pl.when(2 * c + j == x)
            def _():
                pltpu.make_async_copy(
                    sources[a].at[:, :, chunk(j)],
                    seat(a, 0, half, parity * 2, 2),
                    row_r.at[a, parity],
                ).start()

    def y_copy(a, j):
        return remote(
            seat(a, 0, c, j * 2, 2),
            seat(a, 1, c, j * 2, 2),
            y_s.at[a, j],
            y_r.at[a, j],
            partners[a],
        )

    def sib_copy(a, which, core):
        part = alls[a].at[pl.ds(which * 8 + core * 4, 4)]
        return remote(seat(a, which, core, 0, 4), part, sib_s.at[a, which], sib_r.at[a, which], sibling)

    def spread(a):
        for j in range(2):
            part = seat(a, 0, c, j * 2, 2)
            remote(part, part, row_s.at[a, j], row_r.at[a, j], sibling).wait_recv()
            y_copy(a, j).start()
        sib_copy(a, 0, c).start()

    def arrive(a):
        for j in range(2):
            part = seat(a, 1, c, j * 2, 2)
            remote(part, part, y_s.at[a, j], y_r.at[a, j], sibling).wait_recv()
        sib_copy(a, 1, c).start()

    def settle(a, order, target):
        for which in range(2):
            sib_copy(a, which, 1 - c).wait_recv()
            if a >= 2:
                alls[a][pl.ds(which * 8 + c * 4, 4)] = held[a][which * 4 : which * 4 + 4]
        for s in range(16):
            target[s // 4, s % 4 * STRIPE : (s % 4 + 1) * STRIPE, :] = alls[a][table[order + s]]

    row_start(V)

    def tp_copy(src, dst, send, recv, d, slot):
        return remote(src, dst.at[slot], send.at[d], recv.at[slot], tp_peer(y, x, z, c, d))

    for d in range(1, 16):
        tp_copy(sq, sqr, tp_s, tp_r, d, tp).start()
    row_start(G)
    spread(V)
    for d in range(1, 16):
        tp_copy(sq, sqr, tp_s, tp_r, d, lax.rem(tp + d, 16)).wait_recv()
    total = sqr[0]
    for i in range(1, 16):
        total = total + sqr[i]
    tot_ref[...] = total
    inverse = lax.rsqrt(total / D + EPSILON).T
    for ref, gain, out, base, a in ((k_ref, kg_ref, kn, 3, K), (q_ref, qg_ref, qn, 0, Q)):
        wide = ref[...].astype(F32).reshape(TOK, 256)
        parts = []
        for b in range(3):
            unit = wide[chunk(b)] * inverse[:, base + b : base + b + 1]
            parts.append(unit * gain[...])
        out[...] = jnp.concatenate(parts, axis=0).reshape(2, STRIPE, 256).astype(BF16)
        row_start(a)

    def pair_of(set_at, count_at, p):
        base = c * 4 + 2 * lax.rem(p, 2) + 8 * (1 - p // 2)
        first = table[set_at + base]
        first_high = first >= 16
        high = jnp.where(first_high, first, 31 - first)
        high_at = jnp.where(first_high, 0, 1)
        return base, first_high, high, high_at, table[count_at + p]

    def row_step(p, t):
        base, first_high, high, high_at, count = pair_of(QS, QCOUNT, p)
        is_high = t < count
        side = jnp.where(is_high, high_at, 1 - high_at)
        stripe = jnp.where(is_high, high, 31 - high)
        quad = jnp.where(is_high, t, t - count)
        local = 2 * lax.rem(p, 2) + 4 * (1 - p // 2)
        return local + side, side, stripe, jnp.clip(quad, 0, 3)

    def column_step(p, t):
        base, first_high, high, high_at, count = pair_of(KS, KCOUNT, p)
        is_low = t < count
        side = jnp.where(is_low, 1 - high_at, high_at)
        stripe = jnp.where(is_low, 31 - high, high)
        quad = jnp.where(is_low, 4 - count + t, t - 1)
        return base + side, stripe, jnp.clip(quad, 0, 3)

    def split(ref, count, start, join):
        two, three = 2 < count, 3 < count
        first = join(ref[0], ref[1])
        first = join(first, jnp.where(two, ref[2], start))
        first = join(first, jnp.where(three, ref[3], start))
        second = join(ref[4], jnp.where(two, start, ref[2]))
        second = join(second, jnp.where(three, start, ref[3]))
        return first, second

    def loop(lower, upper, body):
        def one(p, carry):
            body(p)
            return carry

        lax.fori_loop(lower, upper, one, 0)

    def grad_probs(p):
        for t in range(STEPS):
            slot, side, stripe, quad = row_step(p, t)
            dps[p, t] = dot_t(mine_g[slot], vp[quad])

    def score(p):
        base, first_high, high, high_at, count = pair_of(QS, QCOUNT, p)
        row = lax.broadcasted_iota(jnp.int32, (STRIPE, QUAD), 0)
        for t in range(STEPS):
            slot, side, stripe, quad = row_step(p, t)
            s = dot_t(mine_q[slot], kp[quad]) * SCALE
            s = jnp.where(kpos[quad] - stripe * STRIPE <= row, s, NEG)
            ss[p, t] = s
            most = s[:, chunk(0)]
            for i in range(1, 6):
                most = jnp.maximum(most, s[:, chunk(i)])
            ms[t] = most
        for side, most in enumerate(split(ms, count, NEG, jnp.maximum)):
            at = high_at if side == 0 else 1 - high_at
            wide = jnp.broadcast_to(jnp.max(most, axis=1, keepdims=True), (STRIPE, 128))
            mm[p, 0] = jnp.where(at == 0, wide, mm[p, 0])
            mm[p, 1] = jnp.where(at == 1, wide, mm[p, 1])

    def sums(p):
        base, first_high, high, high_at, count = pair_of(QS, QCOUNT, p)
        for t in range(STEPS):
            slot, side, stripe, quad = row_step(p, t)
            most = mm[p, side]
            l = jnp.zeros((STRIPE, 128), F32)
            w = jnp.zeros((STRIPE, 128), F32)
            for i in range(6):
                e = jnp.exp2(ss[p, t, :, chunk(i)] - most)
                l = l + e
                w = w + e * dps[p, t, :, chunk(i)]
            ls[t] = l
            ws[t] = w
        l_ends = [jnp.sum(v, axis=1, keepdims=True) for v in split(ls, count, 0.0, jnp.add)]
        w_ends = [jnp.sum(v, axis=1, keepdims=True) for v in split(ws, count, 0.0, jnp.add)]
        lane = lax.broadcasted_iota(jnp.int32, (STRIPE, HD), 1)
        for side in range(2):
            take_first = first_high if side == 0 else jnp.logical_not(first_high)
            l = jnp.where(take_first, l_ends[0], l_ends[1])
            w = jnp.where(take_first, w_ends[0], w_ends[1])
            tile[0:STRIPE, :] = jnp.where(
                lane == 0, mm[p, side], jnp.where(lane == 1, l, w)
            )
            turned = tile[...].T
            for i in range(3):
                st_all[0, pl.ds(i * 8 + p * 2 + side, 1), :] = turned[i : i + 1, :]

    def query_grad(p):
        base, first_high, high, high_at, count = pair_of(QS, QCOUNT, p)
        for t in range(STEPS):
            slot, side, stripe, quad = row_step(p, t)
            log_total = lz[p * 2 + side]
            delta = dl[p * 2 + side]
            parts = []
            for i in range(6):
                probs = jnp.exp2(ss[p, t, :, chunk(i)] - log_total)
                parts.append((probs * (dps[p, t, :, chunk(i)] - delta)).astype(BF16))
            acc[t] = dot_n(jnp.concatenate(parts, axis=1), kp[quad])
        ends = split(acc, count, 0.0, jnp.add)
        for side in range(2):
            take_first = first_high if side == 0 else jnp.logical_not(first_high)
            value = jnp.where(take_first, ends[0], ends[1]) * ROOT
            dq_all[p * 2 + side] = value
            dq_send[p * 2 + side] = value.astype(BF16)

    def key_grads(p):
        base, first_high, high, high_at, count = pair_of(KS, KCOUNT, p)
        row = lax.broadcasted_iota(jnp.int32, (STRIPE, QUAD), 0)
        for t in range(STEPS):
            slot, stripe, quad = column_step(p, t)
            qv = qp[quad]
            gv = gp[quad]
            s = dot_t(all_k[slot], qv) * SCALE - lse[quad]
            probs = jnp.where(row <= qpos[quad] - stripe * STRIPE, jnp.exp2(s), 0.0)
            dp = dot_t(all_v[slot], gv)
            ds = (probs * (dp - dlt[quad])).astype(BF16)
            acc[t] = dot_n(probs.astype(BF16), gv)
            acc2[t] = dot_n(ds, qv)
        for source, scale, out, send in ((acc, None, dv_all, dv_send), (acc2, ROOT, dk_all, dk_send)):
            ends = split(source, count, 0.0, jnp.add)
            for side in range(2):
                take_low = jnp.logical_not(first_high) if side == 0 else first_high
                value = jnp.where(take_low, ends[0], ends[1])
                value = value if scale is None else value * scale
                out[p * 2 + side] = value
                send[p * 2 + side] = value.astype(BF16)

    spread(G)
    arrive(V)
    arrive(G)
    spread(K)
    settle(V, KIDX, vp)
    loop(0, 2, grad_probs)
    spread(Q)
    loop(2, 4, grad_probs)
    arrive(K)
    arrive(Q)
    settle(K, KIDX, kp)
    score(0)
    for p in range(1, 4):
        score(p)
        sums(p - 1)
    sums(3)

    stat_peers = (None, (y_query, x, z, c), sibling, (y_query, x, z, 1 - c))

    def stat_copy(i):
        return remote(st_all.at[0], st_all.at[i], st_s.at[i], st_r.at[i], stat_peers[i])

    for i in range(1, 4):
        stat_copy(i).start()
    settle(G, QIDX, gp)
    settle(Q, QIDX, qp)
    for i in range(1, 4):
        stat_copy(i).wait_recv()
    for which in range(2):
        mine, other = st_all[2 * which], st_all[2 * which + 1]
        other = jnp.concatenate(
            [other[i * 8 + r : i * 8 + r + 4] for i in range(3) for r in (4, 0)], axis=0
        )
        most = jnp.maximum(mine[0:8], other[0:8])
        left, right = jnp.exp2(mine[0:8] - most), jnp.exp2(other[0:8] - most)
        l = mine[8:16] * left + other[8:16] * right
        w = mine[16:24] * left + other[16:24] * right
        log_total = most + jnp.log2(l)
        delta = w / l
        core = c if which == 0 else 1 - c
        fin_l[core] = log_total
        fin_d[core] = delta
        if which == 0:
            turned_l, turned_d = log_total.T, delta.T
            for i in range(8):
                lz[i] = jnp.broadcast_to(turned_l[0:STRIPE, i : i + 1], (STRIPE, 128))
                dl[i] = jnp.broadcast_to(turned_d[0:STRIPE, i : i + 1], (STRIPE, 128))

    reduces = (
        (dq_send, dq_got, (y_query, x, z, c)),
        (dk_send, dk_got, (y_key, x, z, c)),
        (dv_send, dv_got, (y_key, x, z, c)),
    )

    def reduce_copy(a, p):
        send, got, device = reduces[a]
        part = pl.ds(2 * p, 2)
        return remote(send.at[part], got.at[part], red_s.at[a, p], red_r.at[a, p], device)

    returns = ((dq_ret, rq), (dk_ret, rk), (dv_ret, rv))

    def return_copy(a, j):
        out, back = returns[a]
        return remote(
            out.at[pl.ds(j * 2, 2)],
            back.at[parity],
            ret_s.at[a, j],
            ret_r.at[a, parity],
            (y, 2 * c + j, z, half),
        )

    def return_start(a, j):
        out, back = returns[a]

        @pl.when(2 * c + j != x)
        def _():
            return_copy(a, j).start()

        @pl.when(2 * c + j == x)
        def _():
            pltpu.make_async_copy(
                out.at[pl.ds(j * 2, 2)], back.at[parity], ret_r.at[a, parity]
            ).start()

    def return_wait(a):
        back = returns[a][1]
        for j in range(2):
            remote(
                back.at[j], back.at[j], ret_s.at[a, j], ret_r.at[a, j], sibling
            ).wait_recv()

    def join(a, mine, p):
        reduce_copy(a, p).wait_recv()
        for i in (2 * p, 2 * p + 1):
            returns[a][0][i] = (mine[4 + i] + reduces[a][1][i].astype(F32)).astype(BF16)
        return_start(a, p)

    for quad in range(4):
        parts = [[], []]
        for i in range(4):
            at = table[QIDX + quad * 4 + i]
            core = lax.rem(at // 4, 2)
            row = lax.rem(at, 4) + 4 * (1 - at // 8)
            parts[0].append(fin_l[core, pl.ds(row, 1), 0:STRIPE])
            parts[1].append(fin_d[core, pl.ds(row, 1), 0:STRIPE])
        lse[quad] = jnp.concatenate(parts[0], axis=1)
        dlt[quad] = jnp.concatenate(parts[1], axis=1)
    for p in range(2):
        key_grads(p)
        reduce_copy(2, p).start()
        reduce_copy(1, p).start()
    loop(0, 2, query_grad)
    for p in range(2):
        reduce_copy(0, p).start()
    loop(2, 4, query_grad)
    for p in range(2):
        join(0, dq_all, p)
    for p in range(2):
        key_grads(2 + p)
        join(1, dk_all, p)
        join(2, dv_all, p)

    streams = ((q_ref, qg_ref, rq), (k_ref, kg_ref, rk))
    gs[...] = jnp.zeros((8, 256), F32)
    mt[...] = jnp.zeros((8, 128), F32)
    for which, (ref, gain, back) in enumerate(streams):
        return_wait(which)
        gain_sum = jnp.zeros((1, 256), F32)
        wide = ref[...].astype(F32).reshape(TOK, 256)
        grads = [back[j].reshape(TOK, HD) for j in range(2)]
        for b in range(3):
            scale = inverse[:, 3 * which + b : 3 * which + b + 1]
            unit = wide[chunk(b)] * scale
            normed_grad = jnp.concatenate([g[chunk(b)] for g in grads], axis=1).astype(F32)
            product = normed_grad * unit
            gain_sum = gain_sum + jnp.sum(product, axis=0, keepdims=True)
            weighted = product * gain[...]
            folded = weighted[:, :128] + weighted[:, 128:]
            mt[3 * which + b : 3 * which + b + 1, :] = jnp.sum(folded.T, axis=0, keepdims=True)
        gs[which : which + 1, :] = gain_sum

    def x_copy(d, slot):
        return remote(gs, gsr.at[slot], cx_s.at[d], cx_r.at[slot], x_peer(d))

    def gain_copy(d, slot):
        return remote(gy, gyr.at[slot], cy_s.at[d], cy_r.at[slot], y_peer(d))

    for d in range(1, 16):
        tp_copy(mt, mtr, mt_s, mt_r, d, tp).start()
    for d in range(1, 4):
        x_copy(d, x).start()
    mtr[pl.ds(tp, 1)] = mt[...][None]
    gsr[pl.ds(x, 1)] = gs[...][None]
    for d in range(1, 4):
        x_copy(d, lax.rem(x + d, 4)).wait_recv()
    gains = (gsr[0] + gsr[1]) + (gsr[2] + gsr[3])
    gy[...] = gains
    gyr[pl.ds(y, 1)] = gains[None]
    for d in range(1, 4):
        gain_copy(d, y).start()
    return_wait(2)
    for a in range(4):
        for j in range(2):
            @pl.when(2 * c + j != x)
            def _():
                row_copy(a, j).wait_send()
            y_copy(a, j).wait_send()
            sib_copy(a, j, c).wait_send()
    for i in range(1, 4):
        stat_copy(i).wait_send()
    for a in range(3):
        for j in range(2):
            reduce_copy(a, j).wait_send()

            @pl.when(2 * c + j != x)
            def _():
                return_copy(a, j).wait_send()
    for d in range(1, 16):
        tp_copy(sq, sqr, tp_s, tp_r, d, tp).wait_send()
    for d in range(1, 16):
        tp_copy(mt, mtr, mt_s, mt_r, d, lax.rem(tp + d, 16)).wait_recv()
    total = mtr[0]
    for i in range(1, 16):
        total = total + mtr[i]
    mean_ref[...] = total
    for d in range(1, 4):
        gain_copy(d, lax.rem(y + d, 4)).wait_recv()
    gain_ref[...] = (gyr[0] + gyr[1]) + (gyr[2] + gyr[3])
    for d in range(1, 16):
        tp_copy(mt, mtr, mt_s, mt_r, d, tp).wait_send()
    for d in range(1, 4):
        x_copy(d, x).wait_send()
        gain_copy(d, y).wait_send()


def finish_kernel(
    rq, rk, rv, tot_ref, mean_ref, gain_ref, q_ref, k_ref, qg_ref, kg_ref,
    oq_ref, ok_ref, ov_ref, ogq_ref, ogk_ref,
):
    inverse = lax.rsqrt(tot_ref[...] / D + EPSILON).T
    mean = (mean_ref[...] / D).T
    streams = ((q_ref, qg_ref, rq, oq_ref), (k_ref, kg_ref, rk, ok_ref))
    for which, (ref, gain, back, out) in enumerate(streams):
        grads = [back[j].reshape(TOK, HD) for j in range(2)]
        for b in range(3):
            column = slice(3 * which + b, 3 * which + b + 1)
            unit = ref[chunk(b), :].astype(F32) * inverse[:, column]
            normed_grad = jnp.concatenate([g[chunk(b)] for g in grads], axis=1).astype(F32)
            centred = normed_grad * gain[...] - unit * mean[:, column]
            out[chunk(b), :] = (inverse[:, column] * centred).astype(BF16)
    for j in range(2):
        ov_ref[:, chunk(j)] = rv[j].reshape(TOK, HD)
    ogq_ref[...] = gain_ref[0:1, :]
    ogk_ref[...] = gain_ref[1:2, :]


VM = pl.BlockSpec(memory_space=pltpu.VMEM)
DMA = pltpu.SemaphoreType.DMA
LIMIT = 60000 * 1024


def shape(dims, kind):
    return jax.ShapeDtypeStruct(dims, kind)


def vmem(kind, *dims):
    return pltpu.VMEM(dims, kind)


def per_device(query_proj, key_proj, value_proj, query_gain, key_gain, stripe_of, grad_out):
    query_gain = query_gain[None, :]
    key_gain = key_gain[None, :]
    back = shape((2, 2, STRIPE, HD), BF16)
    small = shape((8, 128), F32)
    rq, rk, rv, total, mean, gains = pl.pallas_call(
        main_kernel,
        out_shape=(back, back, back, small, small, shape((8, 256), F32)),
        in_specs=[pl.BlockSpec(memory_space=pltpu.SMEM)] + [VM] * 6,
        out_specs=(VM,) * 6,
        scratch_shapes=[vmem(BF16, 2, STRIPE, 256)] * 2
        + [vmem(BF16, 16, STRIPE, HD)] * 4
        + [vmem(BF16, 8, STRIPE, HD)] * 2
        + [vmem(BF16, 4, QUAD, HD)] * 4
        + [
            vmem(F32, 8, 128),
            vmem(F32, 16, 8, 128),
            vmem(F32, 4, STEPS, STRIPE, QUAD),
            vmem(F32, 4, STEPS, STRIPE, QUAD),
            vmem(F32, STEPS, STRIPE, 128),
            vmem(F32, 4, 2, STRIPE, 128),
            vmem(F32, STEPS, STRIPE, 128),
            vmem(F32, STEPS, STRIPE, 128),
            vmem(F32, 8, STRIPE, 128),
            vmem(F32, 8, STRIPE, 128),
            vmem(F32, STEPS, STRIPE, HD),
            vmem(F32, STEPS, STRIPE, HD),
            vmem(F32, 256, HD),
            vmem(F32, 4, 24, 256),
            vmem(F32, 2, 8, 256),
            vmem(F32, 2, 8, 256),
            vmem(F32, 4, 1, QUAD),
            vmem(F32, 4, 1, QUAD),
            vmem(jnp.int32, 4, 1, QUAD),
            vmem(jnp.int32, 4, 1, QUAD),
        ]
        + [vmem(F32, 8, STRIPE, HD)] * 3
        + [vmem(BF16, 8, STRIPE, HD)] * 3
        + [vmem(BF16, 4, STRIPE, HD)] * 6
        + [
            vmem(F32, 8, 128),
            vmem(F32, 16, 8, 128),
            vmem(F32, 8, 256),
            vmem(F32, 4, 8, 256),
            DMA((4, 2)),
            DMA((4, 2)),
            DMA((4, 2)),
            DMA((4, 2)),
            DMA((4, 2)),
            DMA((4, 2)),
            DMA((16,)),
            DMA((16,)),
            DMA((4,)),
            DMA((4,)),
            DMA((3, 2)),
            DMA((3, 2)),
            DMA((3, 2)),
            DMA((3, 2)),
            DMA((16,)),
            DMA((16,)),
            DMA((4,)),
            DMA((4,)),
            DMA((4,)),
            DMA((4,)),
            vmem(F32, 8, 256),
            vmem(F32, 4, 8, 256),
            pltpu.SMEM((104,), jnp.int32),
        ],
        compiler_params=pltpu.CompilerParams(
            collective_id=1, has_side_effects=True, vmem_limit_bytes=LIMIT
        ),
        name="main",
    )(
        stripe_of,
        *(a.reshape(2, STRIPE, 256) for a in (query_proj, key_proj, value_proj, grad_out)),
        query_gain,
        key_gain,
    )

    out = shape((TOK, 256), BF16)
    gain_out = shape((1, 256), F32)
    grad_query, grad_key, grad_value, gain_q, gain_k = pl.pallas_call(
        finish_kernel,
        out_shape=(out, out, out, gain_out, gain_out),
        in_specs=[VM] * 10,
        out_specs=(VM,) * 5,
        name="finish",
    )(rq, rk, rv, total, mean, gains, query_proj, key_proj, query_gain, key_gain)
    return (grad_query, grad_key, grad_value, gain_q[0], gain_k[0])


def solution(mesh):
    torus = Mesh(mesh.devices.reshape(4, 4, 8, 2), AXES)
    wide = P(("y", "x"), ("z", "core"))
    thin = P(("z", "core"))
    return jax.shard_map(
        per_device,
        mesh=torus,
        in_specs=(wide, wide, wide, thin, thin, P(), wide),
        out_specs=(wide, wide, wide, thin, thin),
        check_vma=False,
    )
```

```python
import jax
import jax.numpy as jnp
from jax import lax
from jax.experimental import pallas as pl
from jax.experimental.pallas import tpu as pltpu
from jax.sharding import Mesh
from jax.sharding import PartitionSpec as P

HD = 128
D = 4096
SEQ = 6144
TOK = 384
STRIPE = 192
QUAD = 768
OWN = 768
STEPS = 5
QS, QIDX, QST, KS, KIDX, KST, QCOUNT, KCOUNT = 0, 16, 32, 48, 64, 80, 96, 100
EPSILON = 1e-06
AXES = ("y", "x", "z", "core")
MESH = pl.DeviceIdType.MESH
ROOT = HD**-0.5
LOG2E = 1.4426950408889634
SCALE = ROOT * LOG2E
NEG = -1e30
F32 = jnp.float32
BF16 = jnp.bfloat16


def place():
    return tuple(lax.axis_index(a) for a in AXES)


def tp_peer(y, x, z, c, d):
    t = lax.rem(z * 2 + c + d, 16)
    return (y, x, t // 2, lax.rem(t, 2))


def dot_t(a, b):
    return lax.dot_general(a, b, (((1,), (1,)), ((), ())), preferred_element_type=F32)


def dot_n(a, b):
    return lax.dot_general(a, b, (((1,), (0,)), ((), ())), preferred_element_type=F32)


def rows_of(block):
    folded = block[:, :128] + block[:, 128:]
    return [
        jnp.sum(folded[b * 128 : (b + 1) * 128].T, axis=0, keepdims=True) for b in range(3)
    ]


def signal(device):
    pl.semaphore_signal(
        pltpu.get_barrier_semaphore(), inc=1, device_id=device, device_id_type=MESH
    )


def remote(src, dst, send_sem, recv_sem, device):
    return pltpu.make_async_remote_copy(
        src_ref=src,
        dst_ref=dst,
        send_sem=send_sem,
        recv_sem=recv_sem,
        device_id=device,
        device_id_type=MESH,
    )


def sort_keys(keys):
    keys = list(keys)
    n, p = len(keys), 1
    while p < n:
        k = p
        while k >= 1:
            for j in range(k % p, n - k, 2 * k):
                for i in range(min(k, n - j - k)):
                    if (i + j) // (2 * p) == (i + j + k) // (2 * p):
                        a, b = keys[i + j], keys[i + j + k]
                        keys[i + j], keys[i + j + k] = jnp.minimum(a, b), jnp.maximum(a, b)
            k //= 2
        p *= 2
    return keys


def chunk(i):
    return slice(i * 128, (i + 1) * 128)


def main_kernel(
    stripes, q_ref, k_ref, v_ref, g_ref, qg_ref, kg_ref,
    rq, rk, rv, tot_ref, mean_ref, gain_ref,
    qn, kn, all_v, all_k, all_g, all_q, mine_g, mine_q, vp, kp, gp, qp,
    sq, sqr, ss, dps, ms, mm, ls, ws, lz, dl, acc, acc2, tile, st_all, fin_l, fin_d,
    lse, dlt, kpos, qpos, dq_all, dk_all, dv_all, dq_send, dk_send, dv_send,
    dq_got, dk_got, dv_got, dq_ret, dk_ret, dv_ret, mt, mtr, gs, gsr,
    row_s, row_r, y_s, y_r, sib_s, sib_r, tp_s, tp_r, st_s, st_r, red_s, red_r,
    ret_s, ret_r, mt_s, mt_r, cx_s, cx_r, cy_s, cy_r, gy, gyr, table,
):
    y, x, z, c = place()
    half = x // 2
    parity = lax.rem(x, 2)
    tp = z * 2 + c
    sibling = (y, x, z, 1 - c)
    y_query = y + 1 - 2 * lax.rem(y, 2)
    y_key = 3 - y

    def x_peer(d):
        return (y, lax.rem(x + d, 4), z, c)

    def y_peer(d):
        return (lax.rem(y + d, 4), x, z, c)

    for j in range(2):
        @pl.when(2 * c + j != x)
        def _():
            signal((y, 2 * c + j, z, half))
    for d in range(1, 4):
        signal(x_peer(d))
        signal(y_peer(d))
    signal((y_query, x, z, 1 - c))
    for d in range(1, 16):
        signal(tp_peer(y, x, z, c, d))

    ordered = []
    for at, other in ((QS, y_query), (KS, y_key)):
        members = [stripes[y * 8 + i] for i in range(8)]
        members += [stripes[other * 8 + i] for i in range(8)]
        keys = sort_keys([m * 16 + i for i, m in enumerate(members)])
        for i in range(16):
            table[at + i] = members[i]
            table[at + 16 + i] = keys[i] & 15
            table[at + 32 + i] = keys[i] >> 4
        ordered.append([k >> 4 for k in keys[:8]])
    for at, count_at, across in ((QS, QCOUNT, ordered[1]), (KS, KCOUNT, ordered[0])):
        for p in range(4):
            first = table[at + c * 4 + 2 * (p % 2) + 8 * (1 - p // 2)]
            low = jnp.minimum(first, 31 - first)
            seen = 3
            for other in across:
                seen = seen + jnp.where(other >= low, 1, 0)
            table[count_at + p] = 2 + (seen >> 2)

    rows = []
    for ref in (q_ref, k_ref):
        wide = ref[...].astype(F32).reshape(TOK, 256)
        rows += rows_of(wide * wide)
    for i, row in enumerate(rows):
        sq[i : i + 1, :] = row
    sq[6:8, :] = jnp.zeros((2, 128), F32)
    sqr[pl.ds(tp, 1)] = sq[...][None]
    lane = lax.broadcasted_iota(jnp.int32, (1, QUAD), 1)
    for sorted_at, out in ((KST, kpos), (QST, qpos)):
        for quad in range(4):
            base = [(table[sorted_at + quad * 4 + i] - i) * STRIPE for i in range(4)]
            shift = jnp.where(
                lane < 2 * STRIPE,
                jnp.where(lane < STRIPE, base[0], base[1]),
                jnp.where(lane < 3 * STRIPE, base[2], base[3]),
            )
            out[quad] = lane + shift
    tile[STRIPE:256, :] = jnp.zeros((256 - STRIPE, HD), F32)
    for p in range(4):
        for side in range(2):
            mm[p, side] = jnp.zeros((STRIPE, 128), F32)
    mine = jnp.where(half == c, 1, 0)
    pl.semaphore_wait(pltpu.get_barrier_semaphore(), 24 - mine)

    V, K, G, Q = range(4)
    sources = (v_ref, kn, g_ref, qn)
    alls = (all_v, all_k, all_g, all_q)
    held = (all_v, all_k, mine_g, mine_q)
    partners = ((y_key, x, z, c), (y_key, x, z, c), (y_query, x, z, c), (y_query, x, z, c))

    def seat(a, block, core, start, size):
        if a < 2:
            return held[a].at[pl.ds(block * 8 + core * 4 + start, size)]
        return held[a].at[pl.ds(block * 4 + start, size)]

    def row_copy(a, j):
        return remote(
            sources[a].at[:, :, chunk(j)],
            seat(a, 0, half, parity * 2, 2),
            row_s.at[a, j],
            row_r.at[a, parity],
            (y, 2 * c + j, z, half),
        )

    def row_start(a):
        for j in range(2):
            @pl.when(2 * c + j != x)
            def _():
                row_copy(a, j).start()

            @pl.when(2 * c + j == x)
            def _():
                pltpu.make_async_copy(
                    sources[a].at[:, :, chunk(j)],
                    seat(a, 0, half, parity * 2, 2),
                    row_r.at[a, parity],
                ).start()

    def y_copy(a, j):
        return remote(
            seat(a, 0, c, j * 2, 2),
            seat(a, 1, c, j * 2, 2),
            y_s.at[a, j],
            y_r.at[a, j],
            partners[a],
        )

    def sib_copy(a, which, core):
        part = alls[a].at[pl.ds(which * 8 + core * 4, 4)]
        return remote(seat(a, which, core, 0, 4), part, sib_s.at[a, which], sib_r.at[a, which], sibling)

    def spread(a):
        for j in range(2):
            part = seat(a, 0, c, j * 2, 2)
            remote(part, part, row_s.at[a, j], row_r.at[a, j], sibling).wait_recv()
            y_copy(a, j).start()
        sib_copy(a, 0, c).start()

    def arrive(a):
        for j in range(2):
            part = seat(a, 1, c, j * 2, 2)
            remote(part, part, y_s.at[a, j], y_r.at[a, j], sibling).wait_recv()
        sib_copy(a, 1, c).start()

    def settle(a, order, target):
        for which in range(2):
            sib_copy(a, which, 1 - c).wait_recv()
            if a >= 2:
                alls[a][pl.ds(which * 8 + c * 4, 4)] = held[a][which * 4 : which * 4 + 4]
        for s in range(16):
            target[s // 4, s % 4 * STRIPE : (s % 4 + 1) * STRIPE, :] = alls[a][table[order + s]]

    row_start(V)

    def tp_copy(src, dst, send, recv, d, slot):
        return remote(src, dst.at[slot], send.at[d], recv.at[slot], tp_peer(y, x, z, c, d))

    for d in range(1, 16):
        tp_copy(sq, sqr, tp_s, tp_r, d, tp).start()
    row_start(G)
    spread(V)
    for d in range(1, 16):
        tp_copy(sq, sqr, tp_s, tp_r, d, lax.rem(tp + d, 16)).wait_recv()
    total = sqr[0]
    for i in range(1, 16):
        total = total + sqr[i]
    tot_ref[...] = total
    inverse = lax.rsqrt(total / D + EPSILON).T
    for ref, gain, out, base, a in ((k_ref, kg_ref, kn, 3, K), (q_ref, qg_ref, qn, 0, Q)):
        wide = ref[...].astype(F32).reshape(TOK, 256)
        parts = []
        for b in range(3):
            unit = wide[chunk(b)] * inverse[:, base + b : base + b + 1]
            parts.append(unit * gain[...])
        out[...] = jnp.concatenate(parts, axis=0).reshape(2, STRIPE, 256).astype(BF16)
        row_start(a)

    def pair_of(set_at, count_at, p):
        base = c * 4 + 2 * lax.rem(p, 2) + 8 * (1 - p // 2)
        first = table[set_at + base]
        first_high = first >= 16
        high = jnp.where(first_high, first, 31 - first)
        high_at = jnp.where(first_high, 0, 1)
        return base, first_high, high, high_at, table[count_at + p]

    def row_step(p, t):
        base, first_high, high, high_at, count = pair_of(QS, QCOUNT, p)
        is_high = t < count
        side = jnp.where(is_high, high_at, 1 - high_at)
        stripe = jnp.where(is_high, high, 31 - high)
        quad = jnp.where(is_high, t, t - count)
        local = 2 * lax.rem(p, 2) + 4 * (1 - p // 2)
        return local + side, side, stripe, jnp.clip(quad, 0, 3)

    def column_step(p, t):
        base, first_high, high, high_at, count = pair_of(KS, KCOUNT, p)
        is_low = t < count
        side = jnp.where(is_low, 1 - high_at, high_at)
        stripe = jnp.where(is_low, 31 - high, high)
        quad = jnp.where(is_low, 4 - count + t, t - 1)
        return base + side, stripe, jnp.clip(quad, 0, 3)

    def split(ref, count, start, join):
        two, three = 2 < count, 3 < count
        first = join(ref[0], ref[1])
        first = join(first, jnp.where(two, ref[2], start))
        first = join(first, jnp.where(three, ref[3], start))
        second = join(ref[4], jnp.where(two, start, ref[2]))
        second = join(second, jnp.where(three, start, ref[3]))
        return first, second

    def loop(lower, upper, body):
        def one(p, carry):
            body(p)
            return carry

        lax.fori_loop(lower, upper, one, 0)

    def grad_probs(p):
        for t in range(STEPS):
            slot, side, stripe, quad = row_step(p, t)
            dps[p, t] = dot_t(mine_g[slot], vp[quad])

    def score(p):
        base, first_high, high, high_at, count = pair_of(QS, QCOUNT, p)
        row = lax.broadcasted_iota(jnp.int32, (STRIPE, QUAD), 0)
        for t in range(STEPS):
            slot, side, stripe, quad = row_step(p, t)
            s = dot_t(mine_q[slot], kp[quad]) * SCALE
            s = jnp.where(kpos[quad] - stripe * STRIPE <= row, s, NEG)
            ss[p, t] = s
            most = s[:, chunk(0)]
            for i in range(1, 6):
                most = jnp.maximum(most, s[:, chunk(i)])
            ms[t] = most
        for side, most in enumerate(split(ms, count, NEG, jnp.maximum)):
            at = high_at if side == 0 else 1 - high_at
            wide = jnp.broadcast_to(jnp.max(most, axis=1, keepdims=True), (STRIPE, 128))
            mm[p, 0] = jnp.where(at == 0, wide, mm[p, 0])
            mm[p, 1] = jnp.where(at == 1, wide, mm[p, 1])

    def sums(p):
        base, first_high, high, high_at, count = pair_of(QS, QCOUNT, p)
        for t in range(STEPS):
            slot, side, stripe, quad = row_step(p, t)
            most = mm[p, side]
            l = jnp.zeros((STRIPE, 128), F32)
            w = jnp.zeros((STRIPE, 128), F32)
            for i in range(6):
                e = jnp.exp2(ss[p, t, :, chunk(i)] - most)
                l = l + e
                w = w + e * dps[p, t, :, chunk(i)]
            ls[t] = l
            ws[t] = w
        l_ends = [jnp.sum(v, axis=1, keepdims=True) for v in split(ls, count, 0.0, jnp.add)]
        w_ends = [jnp.sum(v, axis=1, keepdims=True) for v in split(ws, count, 0.0, jnp.add)]
        lane = lax.broadcasted_iota(jnp.int32, (STRIPE, HD), 1)
        for side in range(2):
            take_first = first_high if side == 0 else jnp.logical_not(first_high)
            l = jnp.where(take_first, l_ends[0], l_ends[1])
            w = jnp.where(take_first, w_ends[0], w_ends[1])
            tile[0:STRIPE, :] = jnp.where(
                lane == 0, mm[p, side], jnp.where(lane == 1, l, w)
            )
            turned = tile[...].T
            for i in range(3):
                st_all[0, pl.ds(i * 8 + p * 2 + side, 1), :] = turned[i : i + 1, :]

    def query_grad(p):
        base, first_high, high, high_at, count = pair_of(QS, QCOUNT, p)
        for t in range(STEPS):
            slot, side, stripe, quad = row_step(p, t)
            log_total = lz[p * 2 + side]
            delta = dl[p * 2 + side]
            parts = []
            for i in range(6):
                probs = jnp.exp2(ss[p, t, :, chunk(i)] - log_total)
                parts.append((probs * (dps[p, t, :, chunk(i)] - delta)).astype(BF16))
            acc[t] = dot_n(jnp.concatenate(parts, axis=1), kp[quad])
        ends = split(acc, count, 0.0, jnp.add)
        for side in range(2):
            take_first = first_high if side == 0 else jnp.logical_not(first_high)
            value = jnp.where(take_first, ends[0], ends[1]) * ROOT
            dq_all[p * 2 + side] = value
            dq_send[p * 2 + side] = value.astype(BF16)

    def key_grads(p):
        base, first_high, high, high_at, count = pair_of(KS, KCOUNT, p)
        row = lax.broadcasted_iota(jnp.int32, (STRIPE, QUAD), 0)
        for t in range(STEPS):
            slot, stripe, quad = column_step(p, t)
            qv = qp[quad]
            gv = gp[quad]
            s = dot_t(all_k[slot], qv) * SCALE - lse[quad]
            probs = jnp.where(row <= qpos[quad] - stripe * STRIPE, jnp.exp2(s), 0.0)
            dp = dot_t(all_v[slot], gv)
            ds = (probs * (dp - dlt[quad])).astype(BF16)
            acc[t] = dot_n(probs.astype(BF16), gv)
            acc2[t] = dot_n(ds, qv)
        for source, scale, out, send in ((acc, None, dv_all, dv_send), (acc2, ROOT, dk_all, dk_send)):
            ends = split(source, count, 0.0, jnp.add)
            for side in range(2):
                take_low = jnp.logical_not(first_high) if side == 0 else first_high
                value = jnp.where(take_low, ends[0], ends[1])
                value = value if scale is None else value * scale
                out[p * 2 + side] = value
                send[p * 2 + side] = value.astype(BF16)

    spread(G)
    arrive(V)
    arrive(G)
    spread(K)
    settle(V, KIDX, vp)
    loop(0, 2, grad_probs)
    spread(Q)
    loop(2, 4, grad_probs)
    arrive(K)
    arrive(Q)
    settle(K, KIDX, kp)
    score(0)
    for p in range(1, 4):
        score(p)
        sums(p - 1)
    sums(3)

    stat_peers = (None, (y_query, x, z, c), sibling, (y_query, x, z, 1 - c))

    def stat_copy(i):
        return remote(st_all.at[0], st_all.at[i], st_s.at[i], st_r.at[i], stat_peers[i])

    for i in range(1, 4):
        stat_copy(i).start()
    settle(G, QIDX, gp)
    settle(Q, QIDX, qp)
    for i in range(1, 4):
        stat_copy(i).wait_recv()
    for which in range(2):
        mine, other = st_all[2 * which], st_all[2 * which + 1]
        other = jnp.concatenate(
            [other[i * 8 + r : i * 8 + r + 4] for i in range(3) for r in (4, 0)], axis=0
        )
        most = jnp.maximum(mine[0:8], other[0:8])
        left, right = jnp.exp2(mine[0:8] - most), jnp.exp2(other[0:8] - most)
        l = mine[8:16] * left + other[8:16] * right
        w = mine[16:24] * left + other[16:24] * right
        log_total = most + jnp.log2(l)
        delta = w / l
        core = c if which == 0 else 1 - c
        fin_l[core] = log_total
        fin_d[core] = delta
        if which == 0:
            turned_l, turned_d = log_total.T, delta.T
            for i in range(8):
                lz[i] = jnp.broadcast_to(turned_l[0:STRIPE, i : i + 1], (STRIPE, 128))
                dl[i] = jnp.broadcast_to(turned_d[0:STRIPE, i : i + 1], (STRIPE, 128))

    reduces = (
        (dq_send, dq_got, (y_query, x, z, c)),
        (dk_send, dk_got, (y_key, x, z, c)),
        (dv_send, dv_got, (y_key, x, z, c)),
    )

    def reduce_copy(a, p):
        send, got, device = reduces[a]
        part = pl.ds(2 * p, 2)
        return remote(send.at[part], got.at[part], red_s.at[a, p], red_r.at[a, p], device)

    returns = ((dq_ret, rq), (dk_ret, rk), (dv_ret, rv))

    def return_copy(a, j):
        out, back = returns[a]
        return remote(
            out.at[pl.ds(j * 2, 2)],
            back.at[parity],
            ret_s.at[a, j],
            ret_r.at[a, parity],
            (y, 2 * c + j, z, half),
        )

    def return_start(a, j):
        out, back = returns[a]

        @pl.when(2 * c + j != x)
        def _():
            return_copy(a, j).start()

        @pl.when(2 * c + j == x)
        def _():
            pltpu.make_async_copy(
                out.at[pl.ds(j * 2, 2)], back.at[parity], ret_r.at[a, parity]
            ).start()

    def return_wait(a):
        back = returns[a][1]
        for j in range(2):
            remote(
                back.at[j], back.at[j], ret_s.at[a, j], ret_r.at[a, j], sibling
            ).wait_recv()

    def join(a, mine, p):
        reduce_copy(a, p).wait_recv()
        for i in (2 * p, 2 * p + 1):
            returns[a][0][i] = (mine[4 + i] + reduces[a][1][i].astype(F32)).astype(BF16)
        return_start(a, p)

    for quad in range(4):
        parts = [[], []]
        for i in range(4):
            at = table[QIDX + quad * 4 + i]
            core = lax.rem(at // 4, 2)
            row = lax.rem(at, 4) + 4 * (1 - at // 8)
            parts[0].append(fin_l[core, pl.ds(row, 1), 0:STRIPE])
            parts[1].append(fin_d[core, pl.ds(row, 1), 0:STRIPE])
        lse[quad] = jnp.concatenate(parts[0], axis=1)
        dlt[quad] = jnp.concatenate(parts[1], axis=1)
    for p in range(2):
        key_grads(p)
        reduce_copy(1, p).start()
        reduce_copy(2, p).start()
        if p == 0:
            loop(0, 2, query_grad)
            for other in range(2):
                reduce_copy(0, other).start()
    loop(2, 4, query_grad)
    for p in range(2):
        join(0, dq_all, p)
    for p in range(2):
        key_grads(2 + p)
        join(1, dk_all, p)
        join(2, dv_all, p)

    streams = ((q_ref, qg_ref, rq), (k_ref, kg_ref, rk))
    gs[...] = jnp.zeros((8, 256), F32)
    mt[...] = jnp.zeros((8, 128), F32)
    for which, (ref, gain, back) in enumerate(streams):
        return_wait(which)
        gain_sum = jnp.zeros((1, 256), F32)
        wide = ref[...].astype(F32).reshape(TOK, 256)
        grads = [back[j].reshape(TOK, HD) for j in range(2)]
        for b in range(3):
            scale = inverse[:, 3 * which + b : 3 * which + b + 1]
            unit = wide[chunk(b)] * scale
            normed_grad = jnp.concatenate([g[chunk(b)] for g in grads], axis=1).astype(F32)
            product = normed_grad * unit
            gain_sum = gain_sum + jnp.sum(product, axis=0, keepdims=True)
            weighted = product * gain[...]
            folded = weighted[:, :128] + weighted[:, 128:]
            mt[3 * which + b : 3 * which + b + 1, :] = jnp.sum(folded.T, axis=0, keepdims=True)
        gs[which : which + 1, :] = gain_sum

    def x_copy(d, slot):
        return remote(gs, gsr.at[slot], cx_s.at[d], cx_r.at[slot], x_peer(d))

    def gain_copy(d, slot):
        return remote(gy, gyr.at[slot], cy_s.at[d], cy_r.at[slot], y_peer(d))

    for d in range(1, 16):
        tp_copy(mt, mtr, mt_s, mt_r, d, tp).start()
    for d in range(1, 4):
        x_copy(d, x).start()
    mtr[pl.ds(tp, 1)] = mt[...][None]
    gsr[pl.ds(x, 1)] = gs[...][None]
    for d in range(1, 4):
        x_copy(d, lax.rem(x + d, 4)).wait_recv()
    gains = (gsr[0] + gsr[1]) + (gsr[2] + gsr[3])
    gy[...] = gains
    gyr[pl.ds(y, 1)] = gains[None]
    for d in range(1, 4):
        gain_copy(d, y).start()
    return_wait(2)
    for a in range(4):
        for j in range(2):
            @pl.when(2 * c + j != x)
            def _():
                row_copy(a, j).wait_send()
            y_copy(a, j).wait_send()
            sib_copy(a, j, c).wait_send()
    for i in range(1, 4):
        stat_copy(i).wait_send()
    for a in range(3):
        for j in range(2):
            reduce_copy(a, j).wait_send()

            @pl.when(2 * c + j != x)
            def _():
                return_copy(a, j).wait_send()
    for d in range(1, 16):
        tp_copy(sq, sqr, tp_s, tp_r, d, tp).wait_send()
    for d in range(1, 16):
        tp_copy(mt, mtr, mt_s, mt_r, d, lax.rem(tp + d, 16)).wait_recv()
    total = mtr[0]
    for i in range(1, 16):
        total = total + mtr[i]
    mean_ref[...] = total
    for d in range(1, 4):
        gain_copy(d, lax.rem(y + d, 4)).wait_recv()
    gain_ref[...] = (gyr[0] + gyr[1]) + (gyr[2] + gyr[3])
    for d in range(1, 16):
        tp_copy(mt, mtr, mt_s, mt_r, d, tp).wait_send()
    for d in range(1, 4):
        x_copy(d, x).wait_send()
        gain_copy(d, y).wait_send()


def finish_kernel(
    rq, rk, rv, tot_ref, mean_ref, gain_ref, q_ref, k_ref, qg_ref, kg_ref,
    oq_ref, ok_ref, ov_ref, ogq_ref, ogk_ref,
):
    inverse = lax.rsqrt(tot_ref[...] / D + EPSILON).T
    mean = (mean_ref[...] / D).T
    streams = ((q_ref, qg_ref, rq, oq_ref), (k_ref, kg_ref, rk, ok_ref))
    for which, (ref, gain, back, out) in enumerate(streams):
        grads = [back[j].reshape(TOK, HD) for j in range(2)]
        for b in range(3):
            column = slice(3 * which + b, 3 * which + b + 1)
            unit = ref[chunk(b), :].astype(F32) * inverse[:, column]
            normed_grad = jnp.concatenate([g[chunk(b)] for g in grads], axis=1).astype(F32)
            centred = normed_grad * gain[...] - unit * mean[:, column]
            out[chunk(b), :] = (inverse[:, column] * centred).astype(BF16)
    for j in range(2):
        ov_ref[:, chunk(j)] = rv[j].reshape(TOK, HD)
    ogq_ref[...] = gain_ref[0:1, :]
    ogk_ref[...] = gain_ref[1:2, :]


VM = pl.BlockSpec(memory_space=pltpu.VMEM)
DMA = pltpu.SemaphoreType.DMA
LIMIT = 60000 * 1024


def shape(dims, kind):
    return jax.ShapeDtypeStruct(dims, kind)


def vmem(kind, *dims):
    return pltpu.VMEM(dims, kind)


def per_device(query_proj, key_proj, value_proj, query_gain, key_gain, stripe_of, grad_out):
    query_gain = query_gain[None, :]
    key_gain = key_gain[None, :]
    back = shape((2, 2, STRIPE, HD), BF16)
    small = shape((8, 128), F32)
    rq, rk, rv, total, mean, gains = pl.pallas_call(
        main_kernel,
        out_shape=(back, back, back, small, small, shape((8, 256), F32)),
        in_specs=[pl.BlockSpec(memory_space=pltpu.SMEM)] + [VM] * 6,
        out_specs=(VM,) * 6,
        scratch_shapes=[vmem(BF16, 2, STRIPE, 256)] * 2
        + [vmem(BF16, 16, STRIPE, HD)] * 4
        + [vmem(BF16, 8, STRIPE, HD)] * 2
        + [vmem(BF16, 4, QUAD, HD)] * 4
        + [
            vmem(F32, 8, 128),
            vmem(F32, 16, 8, 128),
            vmem(F32, 4, STEPS, STRIPE, QUAD),
            vmem(F32, 4, STEPS, STRIPE, QUAD),
            vmem(F32, STEPS, STRIPE, 128),
            vmem(F32, 4, 2, STRIPE, 128),
            vmem(F32, STEPS, STRIPE, 128),
            vmem(F32, STEPS, STRIPE, 128),
            vmem(F32, 8, STRIPE, 128),
            vmem(F32, 8, STRIPE, 128),
            vmem(F32, STEPS, STRIPE, HD),
            vmem(F32, STEPS, STRIPE, HD),
            vmem(F32, 256, HD),
            vmem(F32, 4, 24, 256),
            vmem(F32, 2, 8, 256),
            vmem(F32, 2, 8, 256),
            vmem(F32, 4, 1, QUAD),
            vmem(F32, 4, 1, QUAD),
            vmem(jnp.int32, 4, 1, QUAD),
            vmem(jnp.int32, 4, 1, QUAD),
        ]
        + [vmem(F32, 8, STRIPE, HD)] * 3
        + [vmem(BF16, 8, STRIPE, HD)] * 3
        + [vmem(BF16, 4, STRIPE, HD)] * 6
        + [
            vmem(F32, 8, 128),
            vmem(F32, 16, 8, 128),
            vmem(F32, 8, 256),
            vmem(F32, 4, 8, 256),
            DMA((4, 2)),
            DMA((4, 2)),
            DMA((4, 2)),
            DMA((4, 2)),
            DMA((4, 2)),
            DMA((4, 2)),
            DMA((16,)),
            DMA((16,)),
            DMA((4,)),
            DMA((4,)),
            DMA((3, 2)),
            DMA((3, 2)),
            DMA((3, 2)),
            DMA((3, 2)),
            DMA((16,)),
            DMA((16,)),
            DMA((4,)),
            DMA((4,)),
            DMA((4,)),
            DMA((4,)),
            vmem(F32, 8, 256),
            vmem(F32, 4, 8, 256),
            pltpu.SMEM((104,), jnp.int32),
        ],
        compiler_params=pltpu.CompilerParams(
            collective_id=1, has_side_effects=True, vmem_limit_bytes=LIMIT
        ),
        name="main",
    )(
        stripe_of,
        *(a.reshape(2, STRIPE, 256) for a in (query_proj, key_proj, value_proj, grad_out)),
        query_gain,
        key_gain,
    )

    out = shape((TOK, 256), BF16)
    gain_out = shape((1, 256), F32)
    grad_query, grad_key, grad_value, gain_q, gain_k = pl.pallas_call(
        finish_kernel,
        out_shape=(out, out, out, gain_out, gain_out),
        in_specs=[VM] * 10,
        out_specs=(VM,) * 5,
        name="finish",
    )(rq, rk, rv, total, mean, gains, query_proj, key_proj, query_gain, key_gain)
    return (grad_query, grad_key, grad_value, gain_q[0], gain_k[0])


def solution(mesh):
    torus = Mesh(mesh.devices.reshape(4, 4, 8, 2), AXES)
    wide = P(("y", "x"), ("z", "core"))
    thin = P(("z", "core"))
    return jax.shard_map(
        per_device,
        mesh=torus,
        in_specs=(wide, wide, wide, thin, thin, P(), wide),
        out_specs=(wide, wide, wide, thin, thin),
        check_vma=False,
    )
```

```python
import jax
import jax.numpy as jnp
from jax import lax
from jax.experimental import pallas as pl
from jax.experimental.pallas import tpu as pltpu
from jax.sharding import Mesh
from jax.sharding import PartitionSpec as P

HD = 128
D = 4096
SEQ = 6144
TOK = 384
STRIPE = 192
QUAD = 768
OWN = 768
STEPS = 5
FAR = (8, 7, 9, 6, 10, 5, 11, 4, 12, 3, 13, 2, 14, 1, 15)
QS, QIDX, QST, KS, KIDX, KST, QCOUNT, KCOUNT = 0, 16, 32, 48, 64, 80, 96, 100
EPSILON = 1e-06
AXES = ("y", "x", "z", "core")
MESH = pl.DeviceIdType.MESH
ROOT = HD**-0.5
LOG2E = 1.4426950408889634
SCALE = ROOT * LOG2E
NEG = -1e30
F32 = jnp.float32
BF16 = jnp.bfloat16


def place():
    return tuple(lax.axis_index(a) for a in AXES)


def tp_peer(y, x, z, c, d):
    t = lax.rem(z * 2 + c + d, 16)
    return (y, x, t // 2, lax.rem(t, 2))


def dot_t(a, b):
    return lax.dot_general(a, b, (((1,), (1,)), ((), ())), preferred_element_type=F32)


def dot_n(a, b):
    return lax.dot_general(a, b, (((1,), (0,)), ((), ())), preferred_element_type=F32)


def rows_of(block):
    folded = block[:, :128] + block[:, 128:]
    return [
        jnp.sum(folded[b * 128 : (b + 1) * 128].T, axis=0, keepdims=True) for b in range(3)
    ]


def signal(device):
    pl.semaphore_signal(
        pltpu.get_barrier_semaphore(), inc=1, device_id=device, device_id_type=MESH
    )


def remote(src, dst, send_sem, recv_sem, device):
    return pltpu.make_async_remote_copy(
        src_ref=src,
        dst_ref=dst,
        send_sem=send_sem,
        recv_sem=recv_sem,
        device_id=device,
        device_id_type=MESH,
    )


def sort_keys(keys):
    keys = list(keys)
    n, p = len(keys), 1
    while p < n:
        k = p
        while k >= 1:
            for j in range(k % p, n - k, 2 * k):
                for i in range(min(k, n - j - k)):
                    if (i + j) // (2 * p) == (i + j + k) // (2 * p):
                        a, b = keys[i + j], keys[i + j + k]
                        keys[i + j], keys[i + j + k] = jnp.minimum(a, b), jnp.maximum(a, b)
            k //= 2
        p *= 2
    return keys


def chunk(i):
    return slice(i * 128, (i + 1) * 128)


def main_kernel(
    stripes, q_ref, k_ref, v_ref, g_ref, qg_ref, kg_ref,
    rq, rk, rv, tot_ref, mean_ref, gain_ref,
    qn, kn, all_v, all_k, all_g, all_q, mine_g, mine_q, vp, kp, gp, qp,
    sq, sqr, ss, dps, ms, mm, ls, ws, lz, dl, acc, acc2, tile, st_all, fin_l, fin_d,
    lse, dlt, kpos, qpos, dq_all, dk_all, dv_all, dq_send, dk_send, dv_send,
    dq_got, dk_got, dv_got, dq_ret, dk_ret, dv_ret, mt, mtr, gs, gsr,
    row_s, row_r, y_s, y_r, sib_s, sib_r, tp_s, tp_r, st_s, st_r, red_s, red_r,
    ret_s, ret_r, mt_s, mt_r, cx_s, cx_r, cy_s, cy_r, gy, gyr, table,
):
    y, x, z, c = place()
    half = x // 2
    parity = lax.rem(x, 2)
    tp = z * 2 + c
    sibling = (y, x, z, 1 - c)
    y_query = y + 1 - 2 * lax.rem(y, 2)
    y_key = 3 - y

    def x_peer(d):
        return (y, lax.rem(x + d, 4), z, c)

    def y_peer(d):
        return (lax.rem(y + d, 4), x, z, c)

    for d in FAR:
        signal(tp_peer(y, x, z, c, d))
    for j in range(2):
        @pl.when(2 * c + j != x)
        def _():
            signal((y, 2 * c + j, z, half))
    for d in range(1, 4):
        signal(x_peer(d))
        signal(y_peer(d))
    signal((y_query, x, z, 1 - c))

    ordered = []
    for at, other in ((QS, y_query), (KS, y_key)):
        members = [stripes[y * 8 + i] for i in range(8)]
        members += [stripes[other * 8 + i] for i in range(8)]
        keys = sort_keys([m * 16 + i for i, m in enumerate(members)])
        for i in range(16):
            table[at + i] = members[i]
            table[at + 16 + i] = keys[i] & 15
            table[at + 32 + i] = keys[i] >> 4
        ordered.append([k >> 4 for k in keys[:8]])
    for at, count_at, across in ((QS, QCOUNT, ordered[1]), (KS, KCOUNT, ordered[0])):
        for p in range(4):
            first = table[at + c * 4 + 2 * (p % 2) + 8 * (1 - p // 2)]
            low = jnp.minimum(first, 31 - first)
            seen = 3
            for other in across:
                seen = seen + jnp.where(other >= low, 1, 0)
            table[count_at + p] = 2 + (seen >> 2)

    rows = []
    for ref in (q_ref, k_ref):
        wide = ref[...].astype(F32).reshape(TOK, 256)
        rows += rows_of(wide * wide)
    for i, row in enumerate(rows):
        sq[i : i + 1, :] = row
    sq[6:8, :] = jnp.zeros((2, 128), F32)
    sqr[pl.ds(tp, 1)] = sq[...][None]
    lane = lax.broadcasted_iota(jnp.int32, (1, QUAD), 1)
    for sorted_at, out in ((KST, kpos), (QST, qpos)):
        for quad in range(4):
            base = [(table[sorted_at + quad * 4 + i] - i) * STRIPE for i in range(4)]
            shift = jnp.where(
                lane < 2 * STRIPE,
                jnp.where(lane < STRIPE, base[0], base[1]),
                jnp.where(lane < 3 * STRIPE, base[2], base[3]),
            )
            out[quad] = lane + shift
    tile[STRIPE:256, :] = jnp.zeros((256 - STRIPE, HD), F32)
    for p in range(4):
        for side in range(2):
            mm[p, side] = jnp.zeros((STRIPE, 128), F32)
    mine = jnp.where(half == c, 1, 0)
    pl.semaphore_wait(pltpu.get_barrier_semaphore(), 24 - mine)

    V, K, G, Q = range(4)
    sources = (v_ref, kn, g_ref, qn)
    alls = (all_v, all_k, all_g, all_q)
    held = (all_v, all_k, mine_g, mine_q)
    partners = ((y_key, x, z, c), (y_key, x, z, c), (y_query, x, z, c), (y_query, x, z, c))

    def seat(a, block, core, start, size):
        if a < 2:
            return held[a].at[pl.ds(block * 8 + core * 4 + start, size)]
        return held[a].at[pl.ds(block * 4 + start, size)]

    def row_copy(a, j):
        return remote(
            sources[a].at[:, :, chunk(j)],
            seat(a, 0, half, parity * 2, 2),
            row_s.at[a, j],
            row_r.at[a, parity],
            (y, 2 * c + j, z, half),
        )

    def row_start(a):
        for j in range(2):
            @pl.when(2 * c + j != x)
            def _():
                row_copy(a, j).start()

            @pl.when(2 * c + j == x)
            def _():
                pltpu.make_async_copy(
                    sources[a].at[:, :, chunk(j)],
                    seat(a, 0, half, parity * 2, 2),
                    row_r.at[a, parity],
                ).start()

    def y_copy(a, j):
        return remote(
            seat(a, 0, c, j * 2, 2),
            seat(a, 1, c, j * 2, 2),
            y_s.at[a, j],
            y_r.at[a, j],
            partners[a],
        )

    def sib_copy(a, which, core):
        part = alls[a].at[pl.ds(which * 8 + core * 4, 4)]
        return remote(seat(a, which, core, 0, 4), part, sib_s.at[a, which], sib_r.at[a, which], sibling)

    def spread(a):
        for j in range(2):
            part = seat(a, 0, c, j * 2, 2)
            remote(part, part, row_s.at[a, j], row_r.at[a, j], sibling).wait_recv()
            y_copy(a, j).start()
        sib_copy(a, 0, c).start()

    def arrive(a):
        for j in range(2):
            part = seat(a, 1, c, j * 2, 2)
            remote(part, part, y_s.at[a, j], y_r.at[a, j], sibling).wait_recv()
        sib_copy(a, 1, c).start()

    def settle(a, order, target):
        for which in range(2):
            sib_copy(a, which, 1 - c).wait_recv()
            if a >= 2:
                alls[a][pl.ds(which * 8 + c * 4, 4)] = held[a][which * 4 : which * 4 + 4]
        for s in range(16):
            target[s // 4, s % 4 * STRIPE : (s % 4 + 1) * STRIPE, :] = alls[a][table[order + s]]

    row_start(V)

    def tp_copy(src, dst, send, recv, d, slot):
        return remote(src, dst.at[slot], send.at[d], recv.at[slot], tp_peer(y, x, z, c, d))

    for d in FAR:
        tp_copy(sq, sqr, tp_s, tp_r, d, tp).start()
    row_start(G)
    spread(V)
    for d in range(1, 16):
        tp_copy(sq, sqr, tp_s, tp_r, d, lax.rem(tp + d, 16)).wait_recv()
    total = sqr[0]
    for i in range(1, 16):
        total = total + sqr[i]
    tot_ref[...] = total
    inverse = lax.rsqrt(total / D + EPSILON).T
    for ref, gain, out, base, a in ((k_ref, kg_ref, kn, 3, K), (q_ref, qg_ref, qn, 0, Q)):
        wide = ref[...].astype(F32).reshape(TOK, 256)
        parts = []
        for b in range(3):
            unit = wide[chunk(b)] * inverse[:, base + b : base + b + 1]
            parts.append(unit * gain[...])
        out[...] = jnp.concatenate(parts, axis=0).reshape(2, STRIPE, 256).astype(BF16)
        row_start(a)

    def pair_of(set_at, count_at, p):
        base = c * 4 + 2 * lax.rem(p, 2) + 8 * (1 - p // 2)
        first = table[set_at + base]
        first_high = first >= 16
        high = jnp.where(first_high, first, 31 - first)
        high_at = jnp.where(first_high, 0, 1)
        return base, first_high, high, high_at, table[count_at + p]

    def row_step(p, t):
        base, first_high, high, high_at, count = pair_of(QS, QCOUNT, p)
        is_high = t < count
        side = jnp.where(is_high, high_at, 1 - high_at)
        stripe = jnp.where(is_high, high, 31 - high)
        quad = jnp.where(is_high, t, t - count)
        local = 2 * lax.rem(p, 2) + 4 * (1 - p // 2)
        return local + side, side, stripe, jnp.clip(quad, 0, 3)

    def column_step(p, t):
        base, first_high, high, high_at, count = pair_of(KS, KCOUNT, p)
        is_low = t < count
        side = jnp.where(is_low, 1 - high_at, high_at)
        stripe = jnp.where(is_low, 31 - high, high)
        quad = jnp.where(is_low, 4 - count + t, t - 1)
        return base + side, stripe, jnp.clip(quad, 0, 3)

    def split(ref, count, start, join):
        two, three = 2 < count, 3 < count
        first = join(ref[0], ref[1])
        first = join(first, jnp.where(two, ref[2], start))
        first = join(first, jnp.where(three, ref[3], start))
        second = join(ref[4], jnp.where(two, start, ref[2]))
        second = join(second, jnp.where(three, start, ref[3]))
        return first, second

    def loop(lower, upper, body):
        def one(p, carry):
            body(p)
            return carry

        lax.fori_loop(lower, upper, one, 0)

    def grad_probs(p):
        for t in range(STEPS):
            slot, side, stripe, quad = row_step(p, t)
            dps[p, t] = dot_t(mine_g[slot], vp[quad])

    def score(p):
        base, first_high, high, high_at, count = pair_of(QS, QCOUNT, p)
        row = lax.broadcasted_iota(jnp.int32, (STRIPE, QUAD), 0)
        for t in range(STEPS):
            slot, side, stripe, quad = row_step(p, t)
            s = dot_t(mine_q[slot], kp[quad]) * SCALE
            s = jnp.where(kpos[quad] - stripe * STRIPE <= row, s, NEG)
            ss[p, t] = s
            most = s[:, chunk(0)]
            for i in range(1, 6):
                most = jnp.maximum(most, s[:, chunk(i)])
            ms[t] = most
        for side, most in enumerate(split(ms, count, NEG, jnp.maximum)):
            at = high_at if side == 0 else 1 - high_at
            wide = jnp.broadcast_to(jnp.max(most, axis=1, keepdims=True), (STRIPE, 128))
            mm[p, 0] = jnp.where(at == 0, wide, mm[p, 0])
            mm[p, 1] = jnp.where(at == 1, wide, mm[p, 1])

    def sums(p):
        base, first_high, high, high_at, count = pair_of(QS, QCOUNT, p)
        for t in range(STEPS):
            slot, side, stripe, quad = row_step(p, t)
            most = mm[p, side]
            l = jnp.zeros((STRIPE, 128), F32)
            w = jnp.zeros((STRIPE, 128), F32)
            for i in range(6):
                e = jnp.exp2(ss[p, t, :, chunk(i)] - most)
                l = l + e
                w = w + e * dps[p, t, :, chunk(i)]
            ls[t] = l
            ws[t] = w
        l_ends = [jnp.sum(v, axis=1, keepdims=True) for v in split(ls, count, 0.0, jnp.add)]
        w_ends = [jnp.sum(v, axis=1, keepdims=True) for v in split(ws, count, 0.0, jnp.add)]
        lane = lax.broadcasted_iota(jnp.int32, (STRIPE, HD), 1)
        for side in range(2):
            take_first = first_high if side == 0 else jnp.logical_not(first_high)
            l = jnp.where(take_first, l_ends[0], l_ends[1])
            w = jnp.where(take_first, w_ends[0], w_ends[1])
            tile[0:STRIPE, :] = jnp.where(
                lane == 0, mm[p, side], jnp.where(lane == 1, l, w)
            )
            turned = tile[...].T
            for i in range(3):
                st_all[0, pl.ds(i * 8 + p * 2 + side, 1), :] = turned[i : i + 1, :]

    def query_grad(p):
        base, first_high, high, high_at, count = pair_of(QS, QCOUNT, p)
        for t in range(STEPS):
            slot, side, stripe, quad = row_step(p, t)
            log_total = lz[p * 2 + side]
            delta = dl[p * 2 + side]
            parts = []
            for i in range(6):
                probs = jnp.exp2(ss[p, t, :, chunk(i)] - log_total)
                parts.append((probs * (dps[p, t, :, chunk(i)] - delta)).astype(BF16))
            acc[t] = dot_n(jnp.concatenate(parts, axis=1), kp[quad])
        ends = split(acc, count, 0.0, jnp.add)
        for side in range(2):
            take_first = first_high if side == 0 else jnp.logical_not(first_high)
            value = jnp.where(take_first, ends[0], ends[1]) * ROOT
            dq_all[p * 2 + side] = value
            dq_send[p * 2 + side] = value.astype(BF16)

    def key_grads(p):
        base, first_high, high, high_at, count = pair_of(KS, KCOUNT, p)
        row = lax.broadcasted_iota(jnp.int32, (STRIPE, QUAD), 0)
        for t in range(STEPS):
            slot, stripe, quad = column_step(p, t)
            qv = qp[quad]
            gv = gp[quad]
            s = dot_t(all_k[slot], qv) * SCALE - lse[quad]
            probs = jnp.where(row <= qpos[quad] - stripe * STRIPE, jnp.exp2(s), 0.0)
            dp = dot_t(all_v[slot], gv)
            ds = (probs * (dp - dlt[quad])).astype(BF16)
            acc[t] = dot_n(probs.astype(BF16), gv)
            acc2[t] = dot_n(ds, qv)
        for source, scale, out, send in ((acc, None, dv_all, dv_send), (acc2, ROOT, dk_all, dk_send)):
            ends = split(source, count, 0.0, jnp.add)
            for side in range(2):
                take_low = jnp.logical_not(first_high) if side == 0 else first_high
                value = jnp.where(take_low, ends[0], ends[1])
                value = value if scale is None else value * scale
                out[p * 2 + side] = value
                send[p * 2 + side] = value.astype(BF16)

    spread(G)
    arrive(V)
    arrive(G)
    spread(K)
    settle(V, KIDX, vp)
    loop(0, 2, grad_probs)
    spread(Q)
    loop(2, 4, grad_probs)
    arrive(K)
    arrive(Q)
    settle(K, KIDX, kp)
    score(0)
    for p in range(1, 4):
        score(p)
        sums(p - 1)
    sums(3)

    stat_peers = (None, (y_query, x, z, c), sibling, (y_query, x, z, 1 - c))

    def stat_copy(i):
        return remote(st_all.at[0], st_all.at[i], st_s.at[i], st_r.at[i], stat_peers[i])

    for i in range(1, 4):
        stat_copy(i).start()
    settle(G, QIDX, gp)
    settle(Q, QIDX, qp)
    for i in range(1, 4):
        stat_copy(i).wait_recv()
    for which in range(2):
        mine, other = st_all[2 * which], st_all[2 * which + 1]
        other = jnp.concatenate(
            [other[i * 8 + r : i * 8 + r + 4] for i in range(3) for r in (4, 0)], axis=0
        )
        most = jnp.maximum(mine[0:8], other[0:8])
        left, right = jnp.exp2(mine[0:8] - most), jnp.exp2(other[0:8] - most)
        l = mine[8:16] * left + other[8:16] * right
        w = mine[16:24] * left + other[16:24] * right
        log_total = most + jnp.log2(l)
        delta = w / l
        core = c if which == 0 else 1 - c
        fin_l[core] = log_total
        fin_d[core] = delta
        if which == 0:
            turned_l, turned_d = log_total.T, delta.T
            for i in range(8):
                lz[i] = jnp.broadcast_to(turned_l[0:STRIPE, i : i + 1], (STRIPE, 128))
                dl[i] = jnp.broadcast_to(turned_d[0:STRIPE, i : i + 1], (STRIPE, 128))

    reduces = (
        (dq_send, dq_got, (y_query, x, z, c)),
        (dk_send, dk_got, (y_key, x, z, c)),
        (dv_send, dv_got, (y_key, x, z, c)),
    )

    def reduce_copy(a, p):
        send, got, device = reduces[a]
        part = pl.ds(2 * p, 2)
        return remote(send.at[part], got.at[part], red_s.at[a, p], red_r.at[a, p], device)

    returns = ((dq_ret, rq), (dk_ret, rk), (dv_ret, rv))

    def return_copy(a, j):
        out, back = returns[a]
        return remote(
            out.at[pl.ds(j * 2, 2)],
            back.at[parity],
            ret_s.at[a, j],
            ret_r.at[a, parity],
            (y, 2 * c + j, z, half),
        )

    def return_start(a, j):
        out, back = returns[a]

        @pl.when(2 * c + j != x)
        def _():
            return_copy(a, j).start()

        @pl.when(2 * c + j == x)
        def _():
            pltpu.make_async_copy(
                out.at[pl.ds(j * 2, 2)], back.at[parity], ret_r.at[a, parity]
            ).start()

    def return_wait(a):
        back = returns[a][1]
        for j in range(2):
            remote(
                back.at[j], back.at[j], ret_s.at[a, j], ret_r.at[a, j], sibling
            ).wait_recv()

    def join(a, mine, p):
        reduce_copy(a, p).wait_recv()
        for i in (2 * p, 2 * p + 1):
            returns[a][0][i] = (mine[4 + i] + reduces[a][1][i].astype(F32)).astype(BF16)
        return_start(a, p)

    for quad in range(4):
        parts = [[], []]
        for i in range(4):
            at = table[QIDX + quad * 4 + i]
            core = lax.rem(at // 4, 2)
            row = lax.rem(at, 4) + 4 * (1 - at // 8)
            parts[0].append(fin_l[core, pl.ds(row, 1), 0:STRIPE])
            parts[1].append(fin_d[core, pl.ds(row, 1), 0:STRIPE])
        lse[quad] = jnp.concatenate(parts[0], axis=1)
        dlt[quad] = jnp.concatenate(parts[1], axis=1)
    for p in range(2):
        key_grads(p)
        reduce_copy(1, p).start()
        reduce_copy(2, p).start()
        if p == 0:
            loop(0, 2, query_grad)
            for other in range(2):
                reduce_copy(0, other).start()
    loop(2, 4, query_grad)
    for p in range(2):
        join(0, dq_all, p)
    for p in range(2):
        key_grads(2 + p)
        join(1, dk_all, p)
        join(2, dv_all, p)

    streams = ((q_ref, qg_ref, rq), (k_ref, kg_ref, rk))
    gs[...] = jnp.zeros((8, 256), F32)
    mt[...] = jnp.zeros((8, 128), F32)
    for which, (ref, gain, back) in enumerate(streams):
        return_wait(which)
        gain_sum = jnp.zeros((1, 256), F32)
        wide = ref[...].astype(F32).reshape(TOK, 256)
        grads = [back[j].reshape(TOK, HD) for j in range(2)]
        for b in range(3):
            scale = inverse[:, 3 * which + b : 3 * which + b + 1]
            unit = wide[chunk(b)] * scale
            normed_grad = jnp.concatenate([g[chunk(b)] for g in grads], axis=1).astype(F32)
            product = normed_grad * unit
            gain_sum = gain_sum + jnp.sum(product, axis=0, keepdims=True)
            weighted = product * gain[...]
            folded = weighted[:, :128] + weighted[:, 128:]
            mt[3 * which + b : 3 * which + b + 1, :] = jnp.sum(folded.T, axis=0, keepdims=True)
        gs[which : which + 1, :] = gain_sum

    def x_copy(d, slot):
        return remote(gs, gsr.at[slot], cx_s.at[d], cx_r.at[slot], x_peer(d))

    def gain_copy(d, slot):
        return remote(gy, gyr.at[slot], cy_s.at[d], cy_r.at[slot], y_peer(d))

    for d in FAR:
        tp_copy(mt, mtr, mt_s, mt_r, d, tp).start()
    for d in range(1, 4):
        x_copy(d, x).start()
    mtr[pl.ds(tp, 1)] = mt[...][None]
    gsr[pl.ds(x, 1)] = gs[...][None]
    for d in range(1, 4):
        x_copy(d, lax.rem(x + d, 4)).wait_recv()
    gains = (gsr[0] + gsr[1]) + (gsr[2] + gsr[3])
    gy[...] = gains
    gyr[pl.ds(y, 1)] = gains[None]
    for d in range(1, 4):
        gain_copy(d, y).start()
    return_wait(2)
    for a in range(4):
        for j in range(2):
            @pl.when(2 * c + j != x)
            def _():
                row_copy(a, j).wait_send()
            y_copy(a, j).wait_send()
            sib_copy(a, j, c).wait_send()
    for i in range(1, 4):
        stat_copy(i).wait_send()
    for a in range(3):
        for j in range(2):
            reduce_copy(a, j).wait_send()

            @pl.when(2 * c + j != x)
            def _():
                return_copy(a, j).wait_send()
    for d in range(1, 16):
        tp_copy(sq, sqr, tp_s, tp_r, d, tp).wait_send()
    for d in range(1, 16):
        tp_copy(mt, mtr, mt_s, mt_r, d, lax.rem(tp + d, 16)).wait_recv()
    total = mtr[0]
    for i in range(1, 16):
        total = total + mtr[i]
    mean_ref[...] = total
    for d in range(1, 4):
        gain_copy(d, lax.rem(y + d, 4)).wait_recv()
    gain_ref[...] = (gyr[0] + gyr[1]) + (gyr[2] + gyr[3])
    for d in range(1, 16):
        tp_copy(mt, mtr, mt_s, mt_r, d, tp).wait_send()
    for d in range(1, 4):
        x_copy(d, x).wait_send()
        gain_copy(d, y).wait_send()


def finish_kernel(
    rq, rk, rv, tot_ref, mean_ref, gain_ref, q_ref, k_ref, qg_ref, kg_ref,
    oq_ref, ok_ref, ov_ref, ogq_ref, ogk_ref,
):
    inverse = lax.rsqrt(tot_ref[...] / D + EPSILON).T
    mean = (mean_ref[...] / D).T
    streams = ((q_ref, qg_ref, rq, oq_ref), (k_ref, kg_ref, rk, ok_ref))
    for which, (ref, gain, back, out) in enumerate(streams):
        grads = [back[j].reshape(TOK, HD) for j in range(2)]
        for b in range(3):
            column = slice(3 * which + b, 3 * which + b + 1)
            unit = ref[chunk(b), :].astype(F32) * inverse[:, column]
            normed_grad = jnp.concatenate([g[chunk(b)] for g in grads], axis=1).astype(F32)
            centred = normed_grad * gain[...] - unit * mean[:, column]
            out[chunk(b), :] = (inverse[:, column] * centred).astype(BF16)
    for j in range(2):
        ov_ref[:, chunk(j)] = rv[j].reshape(TOK, HD)
    ogq_ref[...] = gain_ref[0:1, :]
    ogk_ref[...] = gain_ref[1:2, :]


VM = pl.BlockSpec(memory_space=pltpu.VMEM)
DMA = pltpu.SemaphoreType.DMA
LIMIT = 60000 * 1024


def shape(dims, kind):
    return jax.ShapeDtypeStruct(dims, kind)


def vmem(kind, *dims):
    return pltpu.VMEM(dims, kind)


def per_device(query_proj, key_proj, value_proj, query_gain, key_gain, stripe_of, grad_out):
    query_gain = query_gain[None, :]
    key_gain = key_gain[None, :]
    back = shape((2, 2, STRIPE, HD), BF16)
    small = shape((8, 128), F32)
    rq, rk, rv, total, mean, gains = pl.pallas_call(
        main_kernel,
        out_shape=(back, back, back, small, small, shape((8, 256), F32)),
        in_specs=[pl.BlockSpec(memory_space=pltpu.SMEM)] + [VM] * 6,
        out_specs=(VM,) * 6,
        scratch_shapes=[vmem(BF16, 2, STRIPE, 256)] * 2
        + [vmem(BF16, 16, STRIPE, HD)] * 4
        + [vmem(BF16, 8, STRIPE, HD)] * 2
        + [vmem(BF16, 4, QUAD, HD)] * 4
        + [
            vmem(F32, 8, 128),
            vmem(F32, 16, 8, 128),
            vmem(F32, 4, STEPS, STRIPE, QUAD),
            vmem(F32, 4, STEPS, STRIPE, QUAD),
            vmem(F32, STEPS, STRIPE, 128),
            vmem(F32, 4, 2, STRIPE, 128),
            vmem(F32, STEPS, STRIPE, 128),
            vmem(F32, STEPS, STRIPE, 128),
            vmem(F32, 8, STRIPE, 128),
            vmem(F32, 8, STRIPE, 128),
            vmem(F32, STEPS, STRIPE, HD),
            vmem(F32, STEPS, STRIPE, HD),
            vmem(F32, 256, HD),
            vmem(F32, 4, 24, 256),
            vmem(F32, 2, 8, 256),
            vmem(F32, 2, 8, 256),
            vmem(F32, 4, 1, QUAD),
            vmem(F32, 4, 1, QUAD),
            vmem(jnp.int32, 4, 1, QUAD),
            vmem(jnp.int32, 4, 1, QUAD),
        ]
        + [vmem(F32, 8, STRIPE, HD)] * 3
        + [vmem(BF16, 8, STRIPE, HD)] * 3
        + [vmem(BF16, 4, STRIPE, HD)] * 6
        + [
            vmem(F32, 8, 128),
            vmem(F32, 16, 8, 128),
            vmem(F32, 8, 256),
            vmem(F32, 4, 8, 256),
            DMA((4, 2)),
            DMA((4, 2)),
            DMA((4, 2)),
            DMA((4, 2)),
            DMA((4, 2)),
            DMA((4, 2)),
            DMA((16,)),
            DMA((16,)),
            DMA((4,)),
            DMA((4,)),
            DMA((3, 2)),
            DMA((3, 2)),
            DMA((3, 2)),
            DMA((3, 2)),
            DMA((16,)),
            DMA((16,)),
            DMA((4,)),
            DMA((4,)),
            DMA((4,)),
            DMA((4,)),
            vmem(F32, 8, 256),
            vmem(F32, 4, 8, 256),
            pltpu.SMEM((104,), jnp.int32),
        ],
        compiler_params=pltpu.CompilerParams(
            collective_id=1, has_side_effects=True, vmem_limit_bytes=LIMIT
        ),
        name="main",
    )(
        stripe_of,
        *(a.reshape(2, STRIPE, 256) for a in (query_proj, key_proj, value_proj, grad_out)),
        query_gain,
        key_gain,
    )

    out = shape((TOK, 256), BF16)
    gain_out = shape((1, 256), F32)
    grad_query, grad_key, grad_value, gain_q, gain_k = pl.pallas_call(
        finish_kernel,
        out_shape=(out, out, out, gain_out, gain_out),
        in_specs=[VM] * 10,
        out_specs=(VM,) * 5,
        name="finish",
    )(rq, rk, rv, total, mean, gains, query_proj, key_proj, query_gain, key_gain)
    return (grad_query, grad_key, grad_value, gain_q[0], gain_k[0])


def solution(mesh):
    torus = Mesh(mesh.devices.reshape(4, 4, 8, 2), AXES)
    wide = P(("y", "x"), ("z", "core"))
    thin = P(("z", "core"))
    return jax.shard_map(
        per_device,
        mesh=torus,
        in_specs=(wide, wide, wide, thin, thin, P(), wide),
        out_specs=(wide, wide, wide, thin, thin),
        check_vma=False,
    )
```
